32 devices in a mesh: data: 32 (over z, y, x, core).
Axes of the slice: x: 2, y: 2, z: 4, core: 2. Of those that a mesh axis runs over, the one named last changes fastest.
Arguments:
- tokens: bfloat16 [32768, 384], P('data')
- w_in: bfloat16 [384, 1536], replicated
- w_out: bfloat16 [1536, 384], replicated
- task_heads: bfloat16 [2, 384, 10], replicated
- labels: int32 [2, 32768], P(None, 'data')
- label_mask: int32 [2, 32768], P(None, 'data')
Outputs:
- output 1: float32 [2], replicated
- output 2: float32 [589824], P('data')
- output 3: float32 [589824], P('data')
All inputs are finite; a program needn't handle non-finite values.
Results may differ from the reference program's by a relative error of at most 0.0034077.
Values are sent between devices in bfloat16 or wider.
A program may use at most 1 GiB of HBM per device.

```python
import jax
import jax.numpy as jnp
from jax import lax

MODEL_DIM = 384
HIDDEN_DIM = 1536
NUM_TASKS = 2
NUM_CLASSES = 10
TOK_DEV = 1024
GROUP_SIZE = 32
SOLVER_STEPS = 20


def draw_labels(rng_key):
    sub_keys = jax.random.split(rng_key, 7)
    tokens_total = TOK_DEV * GROUP_SIZE
    dev_class = jax.random.randint(sub_keys[0], (GROUP_SIZE, 1), 0, NUM_CLASSES)
    keep_draw = jax.random.randint(sub_keys[1], (GROUP_SIZE, TOK_DEV), 0, 4)
    free_class = jax.random.randint(sub_keys[2], (GROUP_SIZE, TOK_DEV), 0, NUM_CLASSES)
    common_class = jnp.where(keep_draw < 3, dev_class, free_class).reshape(tokens_total)
    noise_draw = jax.random.randint(sub_keys[3], (NUM_TASKS, tokens_total), 0, 4)
    task_class = jax.random.randint(sub_keys[4], (NUM_TASKS, tokens_total), 0, NUM_CLASSES)
    labels = jnp.where(noise_draw == 0, task_class, common_class[None, :]).astype(jnp.int32)
    mask_level = jax.random.randint(sub_keys[5], (NUM_TASKS, GROUP_SIZE, 1), 5, 100)
    mask_draw = jax.random.randint(sub_keys[6], (NUM_TASKS, GROUP_SIZE, TOK_DEV), 0, 100)
    label_mask = (mask_draw < mask_level).astype(jnp.int32).reshape(NUM_TASKS, tokens_total)
    return labels, label_mask


def setup_inputs(seed: int = 0) -> dict:
    rng_keys = jax.random.split(jax.random.key(seed), 6)
    tokens_total = TOK_DEV * GROUP_SIZE
    tokens = jax.random.normal(rng_keys[0], (tokens_total, MODEL_DIM), jnp.float32)
    w_in = jax.random.normal(rng_keys[1], (MODEL_DIM, HIDDEN_DIM), jnp.float32) * MODEL_DIM ** -0.5
    w_out = jax.random.normal(rng_keys[2], (HIDDEN_DIM, MODEL_DIM), jnp.float32) * HIDDEN_DIM ** -0.5
    shared_head = jax.random.normal(rng_keys[3], (MODEL_DIM, NUM_CLASSES), jnp.float32)
    own_head = jax.random.normal(rng_keys[4], (NUM_TASKS, MODEL_DIM, NUM_CLASSES), jnp.float32)
    head_sign = (1 - 2 * (jnp.arange(NUM_TASKS) % 2)).astype(jnp.float32)
    task_heads = (head_sign[:, None, None] * shared_head[None] + 0.6 * own_head) * (1.5 * MODEL_DIM ** -0.5)
    labels, label_mask = draw_labels(rng_keys[5])
    return {"tokens": tokens.astype(jnp.bfloat16), "w_in": w_in.astype(jnp.bfloat16), "w_out": w_out.astype(jnp.bfloat16), "task_heads": task_heads.astype(jnp.bfloat16), "labels": labels, "label_mask": label_mask}


def device_grads(x_loc, w_in, w_out, task_heads, lab_loc, mask_loc):
    pre_act = jnp.dot(x_loc, w_in, preferred_element_type=jnp.float32)
    act_out, gelu_slope = jax.jvp(jax.nn.gelu, (pre_act,), (jnp.ones_like(pre_act),))
    act_bf = act_out.astype(jnp.bfloat16)
    residual = x_loc.astype(jnp.float32) + jnp.dot(act_bf, w_out, preferred_element_type=jnp.float32)
    z_bf = residual.astype(jnp.bfloat16)
    heads_wide = task_heads.astype(jnp.float32)
    logits = jnp.einsum("bd,tdc->tbc", z_bf.astype(jnp.float32), heads_wide)
    soft_prob = jax.nn.softmax(logits, axis=-1)
    onehot = (lab_loc[:, :, None] == jnp.arange(NUM_CLASSES)[None, None, :]).astype(jnp.float32)
    d_logit = (mask_loc[:, :, None].astype(jnp.float32) * (soft_prob - onehot)).astype(jnp.bfloat16)
    d_resid = jnp.einsum("tbc,tdc->tbd", d_logit.astype(jnp.float32), heads_wide).astype(jnp.bfloat16)
    d_wide = d_resid.astype(jnp.float32)
    grad_w_out = jnp.einsum("bf,tbd->tfd", act_bf.astype(jnp.float32), d_wide)
    d_act = jnp.einsum("tbd,fd->tbf", d_wide, w_out.astype(jnp.float32))
    d_pre = (d_act * gelu_slope[None]).astype(jnp.bfloat16)
    grad_w_in = jnp.einsum("bd,tbf->tdf", x_loc.astype(jnp.float32), d_pre.astype(jnp.float32))
    return grad_w_in, grad_w_out


def solve_weights(gram_mat):
    step_scale = jnp.trace(gram_mat) / NUM_TASKS

    def solver_step(step_idx, weights):
        pull_vec = (gram_mat * weights[None, :]).sum(axis=1)
        raised = weights * jnp.exp(-pull_vec / step_scale)
        return raised / raised.sum()

    init_weights = jnp.full((NUM_TASKS,), 1.0 / NUM_TASKS, jnp.float32)
    return lax.fori_loop(0, SOLVER_STEPS, solver_step, init_weights)


def reference(tokens, w_in, w_out, task_heads, labels, label_mask):
    inv_count = 1.0 / jnp.maximum(label_mask.sum(axis=1), 1).astype(jnp.float32)
    tok_blocks = tokens.reshape(GROUP_SIZE, TOK_DEV, MODEL_DIM)
    lab_blocks = labels.reshape(NUM_TASKS, GROUP_SIZE, TOK_DEV).transpose(1, 0, 2)
    mask_blocks = label_mask.reshape(NUM_TASKS, GROUP_SIZE, TOK_DEV).transpose(1, 0, 2)
    flat_len = MODEL_DIM * HIDDEN_DIM

    def add_device(grad_sum, block_in):
        x_loc, lab_loc, mask_loc = block_in
        grad_w_in, grad_w_out = device_grads(x_loc, w_in, w_out, task_heads, lab_loc, mask_loc)
        flat_grad = jnp.concatenate([grad_w_in.reshape(NUM_TASKS, flat_len), grad_w_out.reshape(NUM_TASKS, flat_len)], axis=1)
        part_grad = (flat_grad * inv_count[:, None]).astype(jnp.bfloat16).astype(jnp.float32)
        return grad_sum + part_grad, None

    grad_sum, _ = lax.scan(add_device, jnp.zeros((NUM_TASKS, 2 * flat_len), jnp.float32), (tok_blocks, lab_blocks, mask_blocks))
    gram_mat = jnp.dot(grad_sum, grad_sum.T, preferred_element_type=jnp.float32)
    weights = solve_weights(gram_mat)
    combined = (weights[:, None] * grad_sum).sum(axis=0)
    return weights, combined[:flat_len], combined[flat_len:]
```

```python
import functools

import jax
import jax.numpy as jnp
import numpy as np
from jax import lax
from jax.experimental import pallas as pl
from jax.experimental.pallas import tpu as pltpu
from jax.sharding import PartitionSpec as P

SOLVER_STEPS = 20
DEVICES = 32
DIM, HID, TOK, CLS = 384, 1536, 1024, 10
CHUNKS, TASKS = 3, 2
F32, BF16 = jnp.float32, jnp.bfloat16
GELU_C = 0.7978845608028654
GELU_A = 0.044715
PAIRS = ((0, 1), (1, 0), (1, 1))


def row_order():
    order = []
    for x in range(2):
        for c in range(2):
            for y in range(2):
                own = [8 * z + 4 * y + 2 * x + c for z in range(4)]
                for o in own:
                    order += [12 * o + i for i in range(8)]
                for o in own:
                    order += [12 * o + i for i in range(8, 12)]
    return np.array(order)


def select_matrix():
    mat = np.zeros((DIM, DIM), np.float32)
    mat[np.arange(DIM), row_order()] = 1.0
    return mat


def dot(a, b, dims):
    return lax.dot_general(a, b, (dims, ((), ())), preferred_element_type=F32)


def kernel(x_ref, w1_ref, w2_ref, heads_ref, lab_ref, mask_ref, sel_ref,
           weights_ref, gin_ref, gout_ref,
           act_ref, slope_ref, xsel_ref, dzt_ref, dz_ref, zt_ref,
           a1_send, b1_send, a1_recv, b1_recv,
           a2_own, b2_own, a2_send, b2_send, a2_recv, b2_recv,
           a3_send, b3_send, a3_recv, b3_recv, ga_ref, gb_ref,
           cnt_ref, gram_ref,
           s1_ssem, s1_rsem, s2_ssem, s2_rsem, s3_ssem, s3_rsem,
           cnt_ssem, cnt_rsem, gram_ssem, gram_rsem):
    me = lax.axis_index("data")
    core = lax.rem(me, 2)
    px = lax.rem(me // 2, 2)
    py = lax.rem(me // 4, 2)
    pz = me // 8

    def device(z, y, x, c):
        return (z * 8 + y * 4 + x * 2 + c,)

    def flip(v, d):
        return lax.rem(v + d, 2)

    def remote(src, dst, ssem, rsem, dev):
        return pltpu.make_async_remote_copy(src_ref=src, dst_ref=dst, send_sem=ssem, recv_sem=rsem,
                                            device_id=dev, device_id_type=pl.DeviceIdType.MESH)

    barrier = pltpu.get_barrier_semaphore()

    @pl.loop(1, DEVICES)
    def _(d):
        pl.semaphore_signal(barrier, inc=1, device_id=(lax.rem(me + d, DEVICES),),
                            device_id_type=pl.DeviceIdType.MESH)

    def row_copy(buf, ssem, rsem, d, slot):
        return remote(buf.at[slot], buf.at[slot], ssem.at[d], rsem.at[d], (lax.rem(me + d, DEVICES),))

    def row_start(buf, ssem, rsem):
        @pl.loop(1, DEVICES)
        def _(d):
            row_copy(buf, ssem, rsem, d, me).start()

    def row_wait(buf, ssem, rsem):
        @pl.loop(1, DEVICES)
        def _(d):
            row_copy(buf, ssem, rsem, d, lax.rem(me + (DEVICES - d), DEVICES)).wait_recv()

    def row_drain(buf, ssem, rsem):
        @pl.loop(1, DEVICES)
        def _(d):
            row_copy(buf, ssem, rsem, d, me).wait_send()

    lane = lax.broadcasted_iota(jnp.int32, (1, 128), 1)

    def lane_pick(row, k):
        return jnp.sum(jnp.where(lane == k, row, 0.0), axis=1, keepdims=True)

    counts = jnp.sum(mask_ref[...].astype(F32), axis=1, keepdims=True)
    cnt_ref[me] = jnp.where(lane == 0, counts[0:1], jnp.where(lane == 1, counts[1:2], 0.0))

    xt = jnp.transpose(x_ref[...])
    xsel_ref[...] = dot(sel_ref[...], xt, ((1,), (0,))).astype(BF16)
    zt_ref[...] = xt.astype(F32)

    @pl.loop(0, HID // 384)
    def _(i):
        cols = pl.ds(pl.multiple_of(i * 384, 384), 384)
        pre = dot(w1_ref[:, cols], x_ref[...], ((0,), (1,)))
        sq = pre * pre
        th = jnp.tanh(pre * (GELU_C + (GELU_C * GELU_A) * sq))
        cdf = 0.5 * (1.0 + th)
        act = (pre * cdf).astype(BF16)
        act_ref[pl.ds(pl.multiple_of(i * 8, 8), 8)] = act.reshape(8, CHUNKS, 16, TOK)
        slope_ref[cols, :] = cdf + 0.5 * pre * (1.0 - th * th) * (GELU_C + (3.0 * GELU_C * GELU_A) * sq)
        zt_ref[...] += dot(w2_ref[cols, :], act, ((0,), (0,)))

    pl.semaphore_wait(barrier, DEVICES - 1)
    row_start(cnt_ref, cnt_ssem, cnt_rsem)

    zt = zt_ref[...].astype(BF16)
    cls = lax.broadcasted_iota(jnp.int32, (CLS, TOK), 0)
    for t in range(TASKS):
        head = heads_ref[t]
        logits = dot(head, zt, ((0,), (0,)))
        ex = jnp.exp(logits - jnp.max(logits, axis=0, keepdims=True))
        prob = ex / jnp.sum(ex, axis=0, keepdims=True)
        onehot = jnp.where(lab_ref[t:t + 1, :] == cls, 1.0, 0.0)
        err = (mask_ref[t:t + 1, :].astype(F32) * (prob - onehot)).astype(BF16)
        dzt = dot(head, err, ((1,), (0,))).astype(BF16)
        dzt_ref[t] = dzt
        dz_ref[:, t * DIM:(t + 1) * DIM] = jnp.transpose(dzt)

    row_wait(cnt_ref, cnt_ssem, cnt_rsem)
    total = jnp.sum(cnt_ref[...], axis=0)
    inv = [1.0 / jnp.maximum(lane_pick(total, t), 1.0) for t in range(TASKS)]

    def compute_b(k):
        rows = [act_ref[8 * z + 4 * y + 2 * x + c, k]
                for y in range(2) for c in range(2) for z in range(4) for x in range(2)]
        part = dot(jnp.concatenate(rows, axis=0), dz_ref[...], ((1,), (0,)))
        for t in range(TASKS):
            b1_send[k, t] = (part[:, t * DIM:(t + 1) * DIM] * inv[t]).astype(BF16).reshape(4, 128, DIM)

    def compute_a(k, t):
        rows = slice(512 * k, 512 * (k + 1))
        back = dot(w2_ref[rows, :], dzt_ref[t], ((1,), (0,)))
        dpre = (back * slope_ref[rows, :]).astype(BF16)
        part = dot(xsel_ref[...], dpre, ((1,), (1,)))
        a1_send[k, t] = (part * inv[t]).astype(BF16).reshape(4, 96, 512)

    def s1_copy(color, k, t, p):
        dn, dc = PAIRS[p]
        c = flip(core, dc)
        if color == 0:
            x = flip(px, dn)
            return remote(a1_send.at[k, t, x * 2 + c], a1_recv.at[k, t, p],
                          s1_ssem.at[color, k, t, p], s1_rsem.at[color, k, t, p], device(pz, py, x, c))
        y = flip(py, dn)
        return remote(b1_send.at[k, t, y * 2 + c], b1_recv.at[k, t, p],
                      s1_ssem.at[color, k, t, p], s1_rsem.at[color, k, t, p], device(pz, y, px, c))

    def s2_copy(color, k, t):
        if color == 0:
            return remote(a2_send.at[k, t], a2_recv.at[k, t], s2_ssem.at[color, k, t], s2_rsem.at[color, k, t],
                          device(pz, flip(py, 1), px, core))
        return remote(b2_send.at[k, t], b2_recv.at[k, t], s2_ssem.at[color, k, t], s2_rsem.at[color, k, t],
                      device(pz, py, flip(px, 1), core))

    def s3_copy(color, k, t, d):
        z = lax.rem(pz + d, 4)
        send, recv = (a3_send, a3_recv) if color == 0 else (b3_send, b3_recv)
        return remote(send.at[k, t, z], recv.at[k, t, d - 1], s3_ssem.at[color, k, t, d - 1],
                      s3_rsem.at[color, k, t, d - 1], device(z, py, px, core))

    def s1_start(color, k, t):
        for p in (2, 1, 0):
            s1_copy(color, k, t, p).start()

    def s1_finish(color, k, t):
        for p in range(3):
            s1_copy(color, k, t, p).wait_recv()
        if color == 0:
            tot = a1_send[k, t, px * 2 + core].astype(F32)
            for p in range(3):
                tot = tot + a1_recv[k, t, p].astype(F32)
            first, second = tot[0:48], tot[48:96]
            keep = py == 0
            a2_own[k, t] = jnp.where(keep, first, second)
            a2_send[k, t] = jnp.where(keep, second, first)
        else:
            tot = b1_send[k, t, py * 2 + core].astype(F32)
            for p in range(3):
                tot = tot + b1_recv[k, t, p].astype(F32)
            tot = tot.reshape(4, 2, 16, DIM)
            keep = px == 0
            b2_own[k, t] = jnp.where(keep, tot[:, 0], tot[:, 1])
            b2_send[k, t] = jnp.where(keep, tot[:, 1], tot[:, 0])
        s2_copy(color, k, t).start()

    def s2_finish(color, k, t):
        s2_copy(color, k, t).wait_recv()
        if color == 0:
            tot = (a2_own[k, t] + a2_recv[k, t]).reshape(6, 8, 512)
            for z in range(4):
                a3_send[k, t, z, 0] = tot[z]
                a3_send[k, t, z, 1] = tot[4 + z // 2]
        else:
            b3_send[k, t] = b2_own[k, t] + b2_recv[k, t]
        for d in (2, 1, 3):
            s3_copy(color, k, t, d).start()

    def s3_finish(color, k, t):
        for d in range(1, 4):
            s3_copy(color, k, t, d).wait_recv()
        if color == 0:
            ga_ref[k, t] = (a3_send[k, t, pz] + a3_recv[k, t, 0]) + (a3_recv[k, t, 1] + a3_recv[k, t, 2])
        else:
            gb_ref[k, t] = (b3_send[k, t, pz] + b3_recv[k, t, 0]) + (b3_recv[k, t, 1] + b3_recv[k, t, 2])

    subs = [(k, t) for k in range(CHUNKS) for t in range(TASKS)]

    compute_b(0)
    s1_start(1, 0, 0)
    compute_a(0, 0)
    s1_start(0, 0, 0)
    s1_start(1, 0, 1)
    compute_a(0, 1)
    s1_start(0, 0, 1)
    compute_b(1)
    compute_a(1, 0)
    for n, (k, t) in enumerate(subs):
        for color in (1, 0):
            s1_finish(color, k, t)
        if n + 2 < len(subs):
            for color in (1, 0):
                s1_start(color, *subs[n + 2])
        if n >= 1:
            for color in (1, 0):
                s2_finish(color, *subs[n - 1])
        if n + 3 < len(subs):
            nk, nt = subs[n + 3]
            if nt == 0:
                compute_b(nk)
            compute_a(nk, nt)
        if n >= 3:
            for color in (1, 0):
                s3_finish(color, *subs[n - 3])
    for color in (1, 0):
        s2_finish(color, *subs[5])
    for n in (3, 4, 5):
        for color in (1, 0):
            s3_finish(color, *subs[n])

    half = lax.broadcasted_iota(jnp.int32, (8, 512), 0) // 4 == lax.rem(pz, 2)

    def own_rows(k, t):
        return ga_ref[k, t, 0], jnp.where(half, ga_ref[k, t, 1], 0.0)

    sums = [jnp.zeros((8, 128), F32)] * 3
    for k in range(CHUNKS):
        tops = [own_rows(k, t) for t in range(TASKS)]
        lows = [gb_ref[k, t] for t in range(TASKS)]
        for q, (s, t) in enumerate(((0, 0), (0, 1), (1, 1))):
            prod = tops[s][0] * tops[t][0] + tops[s][1] * tops[t][1]
            for j in range(4):
                sums[q] = sums[q] + prod[:, 128 * j:128 * (j + 1)]
            prod = lows[s] * lows[t]
            prod = prod[0:8] + prod[8:16]
            for j in range(3):
                sums[q] = sums[q] + prod[:, 128 * j:128 * (j + 1)]
    row = jnp.zeros((1, 128), F32)
    for q in range(3):
        one = jnp.sum(jnp.sum(sums[q], axis=0, keepdims=True), axis=1, keepdims=True)
        row = jnp.where(lane == q, one, row)
    gram_ref[me] = row
    row_start(gram_ref, gram_ssem, gram_rsem)
    row_wait(gram_ref, gram_ssem, gram_rsem)
    total = jnp.sum(gram_ref[...], axis=0)
    m00, m01, m11 = [jnp.broadcast_to(lane_pick(total, q), (1, 128)) for q in range(3)]
    scale = (m00 + m11) / 2.0
    w0 = jnp.full((1, 128), 0.5, F32)
    w1 = w0
    for _ in range(SOLVER_STEPS):
        r0 = w0 * jnp.exp(-(m00 * w0 + m01 * w1) / scale)
        r1 = w1 * jnp.exp(-(m01 * w0 + m11 * w1) / scale)
        norm = r0 + r1
        w0 = r0 / norm
        w1 = r1 / norm
    weights_ref[...] = jnp.where(lane == 0, w0, w1)

    for k in range(CHUNKS):
        mix = w0[:, 0:1] * gb_ref[k, 0] + w1[:, 0:1] * gb_ref[k, 1]
        for j in range(3):
            gout_ref[pl.ds(48 * k + j, 16, stride=3), :] = mix[:, 128 * j:128 * (j + 1)]
        top = w0[:, 0:1] * ga_ref[k, 0, 0] + w1[:, 0:1] * ga_ref[k, 1, 0]
        low = w0[:, 0:1] * ga_ref[k, 0, 1] + w1[:, 0:1] * ga_ref[k, 1, 1]
        low = jnp.where(lax.rem(pz, 2) == 0, low[0:4], low[4:8])
        for j in range(4):
            gin_ref[pl.ds(4 * k + j, 8, stride=12), :] = top[:, 128 * j:128 * (j + 1)]
            gin_ref[pl.ds(96 + 4 * k + j, 4, stride=12), :] = low[:, 128 * j:128 * (j + 1)]

    row_drain(cnt_ref, cnt_ssem, cnt_rsem)
    row_drain(gram_ref, gram_ssem, gram_rsem)
    for k, t in subs:
        for color in (0, 1):
            for p in range(3):
                s1_copy(color, k, t, p).wait_send()
                s3_copy(color, k, t, p + 1).wait_send()
            s2_copy(color, k, t).wait_send()


def solution(mesh):
    sel = select_matrix()

    def local_step(x_loc, w_in, w_out, task_heads, lab_loc, mask_loc):
        vmem = pl.BlockSpec(memory_space=pltpu.VMEM)
        sub = (CHUNKS, TASKS)
        dma = pltpu.SemaphoreType.DMA
        scratch = [
            pltpu.VMEM((32, CHUNKS, 16, TOK), BF16),
            pltpu.VMEM((HID, TOK), F32),
            pltpu.VMEM((DIM, TOK), BF16),
            pltpu.VMEM((TASKS, DIM, TOK), BF16),
            pltpu.VMEM((TOK, TASKS * DIM), BF16),
            pltpu.VMEM((DIM, TOK), F32),
            pltpu.VMEM(sub + (4, 96, 512), BF16),
            pltpu.VMEM(sub + (4, 128, DIM), BF16),
            pltpu.VMEM(sub + (3, 96, 512), BF16),
            pltpu.VMEM(sub + (3, 128, DIM), BF16),
            pltpu.VMEM(sub + (48, 512), F32),
            pltpu.VMEM(sub + (4, 16, DIM), F32),
            pltpu.VMEM(sub + (48, 512), F32),
            pltpu.VMEM(sub + (4, 16, DIM), F32),
            pltpu.VMEM(sub + (48, 512), F32),
            pltpu.VMEM(sub + (4, 16, DIM), F32),
            pltpu.VMEM(sub + (4, 2, 8, 512), F32),
            pltpu.VMEM(sub + (4, 16, DIM), F32),
            pltpu.VMEM(sub + (3, 2, 8, 512), F32),
            pltpu.VMEM(sub + (3, 16, DIM), F32),
            pltpu.VMEM(sub + (2, 8, 512), F32),
            pltpu.VMEM(sub + (16, DIM), F32),
            pltpu.VMEM((DEVICES, 1, 128), F32),
            pltpu.VMEM((DEVICES, 1, 128), F32),
            dma((2,) + sub + (3,)), dma((2,) + sub + (3,)),
            dma((2,) + sub), dma((2,) + sub),
            dma((2,) + sub + (3,)), dma((2,) + sub + (3,)),
            dma((DEVICES,)), dma((DEVICES,)), dma((DEVICES,)), dma((DEVICES,)),
        ]
        weights, grad_in, grad_out = pl.pallas_call(
            kernel,
            out_shape=[jax.ShapeDtypeStruct((1, 128), F32),
                       jax.ShapeDtypeStruct((144, 128), F32),
                       jax.ShapeDtypeStruct((144, 128), F32)],
            in_specs=[vmem] * 7,
            out_specs=[vmem] * 3,
            scratch_shapes=scratch,
            compiler_params=pltpu.CompilerParams(collective_id=0, has_side_effects=True,
                                                 vmem_limit_bytes=60 * 2 ** 20),
            name="step",
        )(x_loc, w_in, w_out, task_heads, lab_loc, mask_loc, jnp.asarray(sel, BF16))
        return weights[0, :2], grad_in.reshape(-1), grad_out.reshape(-1)

    return jax.shard_map(local_step, mesh=mesh,
                         in_specs=(P("data", None), P(), P(), P(), P(None, "data"), P(None, "data")),
                         out_specs=(P(), P("data"), P("data")), check_vma=False)
```

```python
import contextlib

import jax
import jax.numpy as jnp
import numpy as np
from jax import lax
from jax.experimental import pallas as pl
from jax.experimental.pallas import tpu as pltpu
from jax.sharding import PartitionSpec as P

SOLVER_STEPS = 20
DEVICES = 32
DIM, HID, TOK, CLS = 384, 1536, 1024, 10
CHUNKS, TASKS = 3, 2
F32, BF16 = jnp.float32, jnp.bfloat16
GELU_C = 0.7978845608028654
GELU_A = 0.044715
PAIRS = ((0, 1), (1, 0), (1, 1))

PIECES = (((0, 0, 0), (0, 0, 1), (0, 1, 0), (0, 2, 0)),
          ((1, 0, 0), (1, 1, 0), (1, 2, 0), (1, 2, 1)),
          ((1, 0, 1), (1, 1, 1), (0, 1, 1), (0, 2, 1)))
ROUTE = {piece: (r, n) for r, pieces in enumerate(PIECES) for n, piece in enumerate(pieces)}
COLS = (512, DIM)
PLANE = (96, 128)
TILE = ((2, 8), (16,))


def no_scope(name):
    return contextlib.nullcontext()


scope = no_scope


def owner(z, y, x, c):
    return 8 * z + 4 * y + 2 * x + c


def tiles(owners):
    return [12 * o + i for o in owners for i in range(8)] + [12 * o + i for o in owners for i in range(8, 12)]


def row_orders():
    two = range(2)
    first = [r for x in two for c in two for y in two for r in tiles([owner(z, y, x, c) for z in range(4)])]
    third = [r for zl in two for c in two for y in two for x in two
             for r in tiles([owner(2 * zh + zl, y, x, c) for zh in two])]
    return first, third


def block_orders():
    two = range(2)
    second = [owner(z, y, x, c) for y in two for c in two for x in two for z in range(4)]
    third = [owner(2 * zh + zl, y, x, c) for zl in two for c in two for y in two for x in two for zh in two]
    return second, third


def select_matrices():
    mat = np.zeros((2, DIM, DIM), np.float32)
    for m, order in zip(mat, row_orders()):
        m[np.arange(DIM), np.array(order)] = 1.0
    return mat


def scoped(f):
    def call(*args):
        with scope("_".join([f.__name__, *map(str, args)])):
            return f(*args)
    return call


def dot(a, b, dims):
    return lax.dot_general(a, b, (dims, ((), ())), preferred_element_type=F32)


def kernel(x_hbm, w1_hbm, w2_hbm, heads_hbm, lab_hbm, mask_hbm, sel_hbm,
           gin_hbm, gout_hbm, gram_hbm,
           x_ref, w1_ref, w2_ref, heads_ref, lab_ref, mask_ref, sel_ref,
           gin_ref, gout_ref, gram_out,
           xt_ref, act_ref, slope_ref, xsel_ref, dzt_ref, dz_ref,
           a1_send, b1_send, a1_recv, b1_recv,
           a2_send, b2_send, a2_recv, b2_recv,
           a3_send, b3_send, a3_recv, b3_recv,
           ca2_send, cb2_send, ca2_recv, cb2_recv,
           ca3_send, cb3_send, ca3_recv, cb3_recv,
           cnt_ref, gram_ref,
           in_sem, out_sem, s1_rsem, s2_rsem, s3_rsem, ssem,
           cnt_ssem, cnt_rsem, gram_ssem, gram_rsem):
    me = lax.axis_index("data")
    core = lax.rem(me, 2)
    px = lax.rem(me // 2, 2)
    py = lax.rem(me // 4, 2)
    pz = me // 8
    zl, zh = lax.rem(pz, 2), pz // 2

    def device(z, y, x, c):
        return (owner(z, y, x, c),)

    def flip(v, d):
        return lax.rem(v + d, 2)

    def remote(src, dst, ssem, rsem, dev):
        return pltpu.make_async_remote_copy(src_ref=src, dst_ref=dst, send_sem=ssem, recv_sem=rsem,
                                            device_id=dev, device_id_type=pl.DeviceIdType.MESH)

    loads = {name: pltpu.make_async_copy(src, dst, in_sem.at[i]) for i, (name, src, dst) in enumerate((
        ("mask", mask_hbm, mask_ref), ("x", x_hbm, x_ref), ("w1", w1_hbm, w1_ref), ("w2", w2_hbm, w2_ref),
        ("heads", heads_hbm, heads_ref), ("lab", lab_hbm, lab_ref), ("sel", sel_hbm, sel_ref)))}
    for load in loads.values():
        load.start()

    barrier = pltpu.get_barrier_semaphore()

    @pl.loop(1, DEVICES)
    def _(d):
        pl.semaphore_signal(barrier, inc=1, device_id=(lax.rem(me + d, DEVICES),),
                            device_id_type=pl.DeviceIdType.MESH)

    def row_copy(buf, ssem, rsem, d):
        return remote(buf.at[me], buf.at[me], ssem, rsem, (lax.rem(me + d, DEVICES),))

    def row_start(buf, ssem, rsem):
        @pl.loop(1, DEVICES)
        def _(d):
            row_copy(buf, ssem, rsem, d).start()

    def row_all(buf, ssem, rsem):
        rows = buf.at[pl.ds(0, DEVICES - 1)]
        return remote(rows, rows, ssem, rsem, (lax.rem(me + 1, DEVICES),))

    lane = lax.broadcasted_iota(jnp.int32, (1, 128), 1)

    def lane_pick(row, k):
        return jnp.sum(jnp.where(lane == k, row, 0.0), axis=1, keepdims=True)

    loads["mask"].wait()
    counts = jnp.sum(mask_ref[...].astype(F32), axis=1, keepdims=True)
    cnt_ref[me] = jnp.where(lane == 0, counts[0:1], jnp.where(lane == 1, counts[1:2], 0.0))

    def forward(i):
        cols = slice(i * 384, (i + 1) * 384)
        pre = dot(w1_ref[:, cols], xt_ref[...], ((0,), (0,)))
        sq = pre * pre
        cdf = 0.5 + 0.5 * jnp.tanh(pre * (GELU_C + (GELU_C * GELU_A) * sq))
        act = pre * cdf
        act_ref[8 * i:8 * (i + 1)] = act.astype(BF16).reshape(8, CHUNKS, 16, TOK)
        slope_ref[cols, :] = cdf + act * (1.0 - cdf) * (2.0 * GELU_C + (6.0 * GELU_C * GELU_A) * sq)

    with scope("xt"):
        loads["x"].wait()
        xt_ref[...] = jnp.transpose(x_ref[...])
    with scope("fwd"):
        loads["w1"].wait()
        forward(0)
        forward(1)
    with scope("barrier"):
        pl.semaphore_wait(barrier, DEVICES - 1)
        row_start(cnt_ref, cnt_ssem, cnt_rsem)
    with scope("fwd2"):
        forward(2)
        forward(3)
    with scope("zt"):
        loads["w2"].wait()
        zt = dot(w2_ref[...], act_ref[...].reshape(HID, TOK), ((0,), (0,)))
        zt = (xt_ref[...].astype(F32) + zt).astype(BF16)

    with scope("cls"):
        loads["heads"].wait()
        loads["lab"].wait()
        cls = lax.broadcasted_iota(jnp.int32, (CLS, TOK), 0)
        for t in range(TASKS):
            head = heads_ref[:, t, :]
            logits = dot(head, zt, ((1,), (0,)))
            ex = jnp.exp(logits - jnp.max(logits, axis=0, keepdims=True))
            prob = ex / jnp.sum(ex, axis=0, keepdims=True)
            onehot = jnp.where(lab_ref[t:t + 1, :] == cls, 1.0, 0.0)
            err = (mask_ref[t:t + 1, :].astype(F32) * (prob - onehot)).astype(BF16)
            dzt = dot(head, err, ((0,), (0,))).astype(BF16)
            dzt_ref[t] = dzt
            dz_ref[:, t * DIM:(t + 1) * DIM] = jnp.transpose(dzt)

    with scope("cntwait"):
        row_all(cnt_ref, cnt_ssem, cnt_rsem).wait_recv()
        total = jnp.sum(cnt_ref[...], axis=0)
        inv = [1.0 / jnp.maximum(lane_pick(total, t), 1.0) for t in range(TASKS)]

    orders = block_orders()

    @scoped
    def compute_b(k):
        part = dot(act_ref[:, k].reshape(512, TOK), dz_ref[...], ((1,), (0,)))
        for t in range(TASKS):
            scaled = (part[:, t * DIM:(t + 1) * DIM] * inv[t]).astype(BF16)
            order = orders[ROUTE[1, k, t][0] - 1]
            for n, j in enumerate(order):
                b1_send[2 * k + t, n // 8, 16 * (n % 8):16 * (n % 8 + 1)] = scaled[16 * j:16 * (j + 1)]

    @scoped
    def compute_a(k, t):
        rows = slice(512 * k, 512 * (k + 1))
        back = dot(w2_ref[rows, :], dzt_ref[t], ((1,), (0,)))
        dpre = (back * slope_ref[rows, :]).astype(BF16)
        part = dot(xsel_ref[ROUTE[0, k, t][0] // 2], dpre, ((1,), (1,)))
        a1_send[2 * k + t] = (part * inv[t]).astype(BF16).reshape(4, 96, 512)

    def s1_bufs(part):
        return ((a1_send, a1_recv), (b1_send, b1_recv))[part]

    def s1_copies(route, n):
        part, k, t = PIECES[route][n]
        send, recv = s1_bufs(part)
        for p, (d, dc) in reversed(list(enumerate(PAIRS))):
            c = flip(core, dc)
            if route == 0:
                g = flip(px, d)
                dev = device(pz, py, g, c)
            elif route == 1:
                g = flip(py, d)
                dev = device(pz, g, px, c)
            else:
                g = flip(zl, d)
                dev = device(2 * zh + g, py, px, c)
            yield remote(send.at[2 * k + t, g * 2 + c], recv.at[2 * k + t, p], ssem.at[part],
                         s1_rsem.at[route, n], dev)

    def s2_copies(route, n):
        part = PIECES[route][n][0]
        if route == 0:
            yield remote(a2_send.at[n, flip(py, 1)], a2_recv.at[n], ssem.at[2], s2_rsem.at[route, n],
                         device(pz, flip(py, 1), px, core))
        elif route == 1:
            yield remote(b2_send.at[n, flip(px, 1)], b2_recv.at[n], ssem.at[3], s2_rsem.at[route, n],
                         device(pz, py, flip(px, 1), core))
        else:
            send, recv = ((ca2_send, ca2_recv), (cb2_send, cb2_recv))[part]
            for p, (dy, dx) in reversed(list(enumerate(PAIRS))):
                y, x = flip(py, dy), flip(px, dx)
                yield remote(send.at[n % 2, 2 * y + x], recv.at[n % 2, p], ssem.at[4 + part],
                             s2_rsem.at[route, n], device(pz, y, x, core))

    def s3_copies(route, n):
        part = PIECES[route][n][0]
        if route == 2:
            send, recv = ((ca3_send, ca3_recv), (cb3_send, cb3_recv))[part]
            yield remote(send.at[n % 2, flip(zh, 1)], recv.at[n % 2], ssem.at[8 + part], s3_rsem.at[route, n],
                         device(lax.rem(pz + 2, 4), py, px, core))
            return
        send, recv = ((a3_send, a3_recv), (b3_send, b3_recv))[part]
        for d in (2, 1, 3):
            z = lax.rem(pz + d, 4)
            yield remote(send.at[n, z], recv.at[n, d - 1], ssem.at[6 + part], s3_rsem.at[route, n],
                         device(z, py, px, core))

    def whole(ref, rsem):
        return remote(ref, ref, rsem, rsem, device(lax.rem(pz + 1, 4), py, px, core))

    @scoped
    def s1_start(route, n):
        for copy in s1_copies(route, n):
            copy.start()

    @scoped
    def s1_finish(route, n):
        part, k, t = PIECES[route][n]
        i = 2 * k + t
        send, recv = s1_bufs(part)
        whole(recv.at[i], s1_rsem.at[route, n]).wait_recv()
        slot = (px, py, zl)[route] * 2 + core
        tot = (send[i, slot].astype(F32) + recv[i, 0].astype(F32)) + (recv[i, 1].astype(F32) + recv[i, 2].astype(F32))
        if route < 2:
            (a2_send, b2_send)[route][n] = tot.reshape(2, PLANE[part] // 2, COLS[part])
        else:
            (ca2_send, cb2_send)[part][n % 2] = tot.reshape(4, PLANE[part] // 4, COLS[part])
        for copy in s2_copies(route, n):
            copy.start()

    @scoped
    def s2_finish(route, n):
        part = PIECES[route][n][0]
        if route < 2:
            send, recv = ((a2_send, a2_recv), (b2_send, b2_recv))[route]
            whole(recv.at[n], s2_rsem.at[route, n]).wait_recv()
            tot = send[n, (py, px)[route]] + recv[n]
            out, count = (a3_send, b3_send)[route].at[n], 4
        else:
            send, recv = ((ca2_send, ca2_recv), (cb2_send, cb2_recv))[part]
            whole(recv.at[n % 2], s2_rsem.at[route, n]).wait_recv()
            tot = (send[n % 2, 2 * py + px] + recv[n % 2, 0]) + (recv[n % 2, 1] + recv[n % 2, 2])
            out, count = (ca3_send, cb3_send)[part].at[n % 2], 2
        if part == 0:
            for z in range(count):
                out[z, 0] = tot[8 * z:8 * (z + 1)]
                shared = 8 * (count + z // 2)
                out[z, 1] = tot[shared:shared + 8]
        else:
            out[...] = tot.reshape(count, 16, DIM)
        for copy in s3_copies(route, n):
            copy.start()

    @scoped
    def s3_finish(route, n):
        part, k, t = PIECES[route][n]
        if route == 2:
            send, recv = ((ca3_send, ca3_recv), (cb3_send, cb3_recv))[part]
            whole(recv.at[n % 2], s3_rsem.at[route, n]).wait_recv()
            tot = send[n % 2, zh] + recv[n % 2]
            odd = zh
        else:
            send, recv = ((a3_send, a3_recv), (b3_send, b3_recv))[part]
            whole(recv.at[n], s3_rsem.at[route, n]).wait_recv()
            tot = (send[n, pz] + recv[n, 0]) + (recv[n, 1] + recv[n, 2])
            odd = zl
        if part == 0:
            low = jnp.where(odd == 0, tot[1, 0:4], tot[1, 4:8])
            for j in range(4):
                gin_ref[t, pl.ds(4 * k + j, 8, stride=12), :] = tot[0, :, 128 * j:128 * (j + 1)]
                gin_ref[t, pl.ds(96 + 4 * k + j, 4, stride=12), :] = low[:, 128 * j:128 * (j + 1)]
        else:
            for j in range(3):
                gout_ref[t, pl.ds(48 * k + j, 16, stride=3), :] = tot[:, 128 * j:128 * (j + 1)]

    compute_b(0)
    s1_start(1, 0)
    s1_start(2, 0)
    loads["sel"].wait()
    for r in range(2):
        xsel_ref[r] = dot(sel_ref[r], xt_ref[...], ((1,), (0,))).astype(BF16)
    compute_a(0, 0)
    s1_start(0, 0)
    compute_a(0, 1)
    s1_start(0, 1)
    compute_b(1)
    s1_start(1, 1)
    s1_start(2, 1)
    compute_a(1, 0)
    compute_a(1, 1)
    for r in (1, 2, 0):
        s1_finish(r, 0)
    s1_start(0, 2)
    s1_start(2, 2)
    compute_b(2)
    s1_start(1, 2)
    compute_a(2, 0)
    for r in (1, 2, 0):
        s1_finish(r, 1)
    s1_start(0, 3)
    s1_start(1, 3)
    for r in (1, 0, 2):
        s2_finish(r, 0)
    compute_a(2, 1)
    s1_start(2, 3)
    for r in (1, 0):
        s1_finish(r, 2)
    for r in (1, 0, 2):
        s2_finish(r, 1)
    for r in (1, 0, 2):
        s3_finish(r, 0)
    for r in (1, 0):
        s1_finish(r, 3)
    s1_finish(2, 2)
    s1_finish(2, 3)
    for r in (1, 0):
        s2_finish(r, 2)
    for r in (1, 0, 2):
        s3_finish(r, 1)
    for r in (1, 0):
        s2_finish(r, 3)
    s2_finish(2, 2)
    s2_finish(2, 3)
    for n in (2, 3):
        for r in (1, 0, 2):
            s3_finish(r, n)

    stores = [pltpu.make_async_copy(src, dst, out_sem.at[i])
              for i, (src, dst) in enumerate(((gin_ref, gin_hbm), (gout_ref, gout_hbm), (gram_out, gram_hbm)))]
    with scope("gram"):
        row = jnp.zeros((1, 128), F32)
        for q, (s, t) in enumerate(((0, 0), (0, 1), (1, 1))):
            prod = gin_ref[s] * gin_ref[t] + gout_ref[s] * gout_ref[t]
            one = jnp.sum(jnp.sum(prod, axis=0, keepdims=True), axis=1, keepdims=True)
            row = jnp.where(lane == q, one, row)
        gram_ref[me] = row
    with scope("gramx"):
        row_start(gram_ref, gram_ssem, gram_rsem)
        stores[0].start()
        stores[1].start()
        for i, ref in enumerate((a1_recv, b1_recv, a2_recv, b2_recv, ca2_recv, cb2_recv, a3_recv, b3_recv,
                                 ca3_recv, cb3_recv)):
            whole(ref, ssem.at[i]).wait_send()
        row_all(cnt_ref, cnt_ssem, cnt_rsem).wait_send()
        stores[0].wait()
        stores[1].wait()
        row_all(gram_ref, gram_ssem, gram_rsem).wait_recv()
    with scope("drain"):
        gram_out[...] = jnp.sum(gram_ref[...], axis=0)
        stores[2].start()
        row_all(gram_ref, gram_ssem, gram_rsem).wait_send()
        stores[2].wait()


def combine(gram_hbm, gin_hbm, gout_hbm, weights_ref, sum_in, sum_out, gram_ref, gin_ref, gout_ref, sem):
    loads = [pltpu.make_async_copy(src, dst, sem.at[i])
             for i, (src, dst) in enumerate(((gram_hbm, gram_ref), (gin_hbm, gin_ref), (gout_hbm, gout_ref)))]
    for load in loads:
        load.start()
    loads[0].wait()
    lane = lax.broadcasted_iota(jnp.int32, (1, 128), 1)
    m00, m01, m11 = [jnp.broadcast_to(jnp.sum(jnp.where(lane == q, gram_ref[...], 0.0), axis=1, keepdims=True), (1, 128))
                     for q in range(3)]
    scale = (m00 + m11) / 2.0
    w0 = jnp.full((1, 128), 0.5, F32)
    w1 = w0
    for _ in range(SOLVER_STEPS):
        r0 = w0 * jnp.exp(-(m00 * w0 + m01 * w1) / scale)
        r1 = w1 * jnp.exp(-(m01 * w0 + m11 * w1) / scale)
        norm = r0 + r1
        w0 = r0 / norm
        w1 = r1 / norm
    weights_ref[0] = w0[0, 0]
    weights_ref[1] = w1[0, 0]
    loads[1].wait()
    loads[2].wait()
    sum_in[...] = w0 * gin_ref[0] + w1 * gin_ref[1]
    sum_out[...] = w0 * gout_ref[0] + w1 * gout_ref[1]


def solution(mesh):
    sel = select_matrices()

    def local_step(x_loc, w_in, w_out, task_heads, lab_loc, mask_loc):
        vmem = pl.BlockSpec(memory_space=pltpu.VMEM)
        hbm = pl.BlockSpec(memory_space=pl.ANY)
        dma = pltpu.SemaphoreType.DMA
        heads_t = jnp.transpose(task_heads, (2, 0, 1))
        args = (x_loc, w_in, w_out, heads_t, lab_loc, mask_loc, jnp.asarray(sel, BF16))
        piece = jax.ShapeDtypeStruct((144, 128), F32)
        outs = [jax.ShapeDtypeStruct((TASKS, 144, 128), F32)] * 2 + [jax.ShapeDtypeStruct((1, 128), F32)]
        scratch = [pltpu.VMEM(a.shape, a.dtype) for a in args] + [pltpu.VMEM(a.shape, a.dtype) for a in outs] + [
            pltpu.VMEM((DIM, TOK), BF16),
            pltpu.VMEM((32, CHUNKS, 16, TOK), BF16),
            pltpu.VMEM((HID, TOK), F32),
            pltpu.VMEM((2, DIM, TOK), BF16),
            pltpu.VMEM((TASKS, DIM, TOK), BF16),
            pltpu.VMEM((TOK, TASKS * DIM), BF16)]
        shapes = [[(BF16, (6, 4), 1), (BF16, (6, 3), 1)], [(F32, (4, 2), 2), (F32, (4,), 2)],
                  [(F32, (4, 4), 0), (F32, (4, 3), 0)], [(F32, (2, 4), 4), (F32, (2, 3), 4)],
                  [(F32, (2, 2), 0), (F32, (2,), 0)]]
        for stage in shapes:
            for dtype, lead, div in stage:
                for part in range(2):
                    rows = (PLANE[part] // div,) if div else TILE[part]
                    scratch.append(pltpu.VMEM(lead + rows + (COLS[part],), dtype))
        scratch += [pltpu.VMEM((DEVICES, 1, 128), F32), pltpu.VMEM((DEVICES, 1, 128), F32),
                    dma((len(args),)), dma((3,)), dma((3, 4)), dma((3, 4)), dma((3, 4)), dma((10,)),
                    dma, dma, dma, dma]
        gin, gout, gram = pl.pallas_call(
            kernel,
            out_shape=outs,
            in_specs=[hbm] * len(args),
            out_specs=[hbm] * 3,
            scratch_shapes=scratch,
            compiler_params=pltpu.CompilerParams(collective_id=0, has_side_effects=True,
                                                 vmem_limit_bytes=66_900_000),
            name="step",
        )(*args)
        weights, grad_in, grad_out = pl.pallas_call(
            combine,
            out_shape=[jax.ShapeDtypeStruct((TASKS,), F32), piece, piece],
            in_specs=[hbm] * 3,
            out_specs=[pl.BlockSpec(memory_space=pltpu.SMEM), vmem, vmem],
            scratch_shapes=[pltpu.VMEM(outs[2].shape, F32), pltpu.VMEM(outs[0].shape, F32),
                            pltpu.VMEM(outs[1].shape, F32), dma((3,))],
            compiler_params=pltpu.CompilerParams(vmem_limit_bytes=66_900_000),
            name="combine",
        )(gram, gin, gout)
        return weights, grad_in.reshape(-1), grad_out.reshape(-1)

    return jax.shard_map(local_step, mesh=mesh,
                         in_specs=(P("data", None), P(), P(), P(), P(None, "data"), P(None, "data")),
                         out_specs=(P(), P("data"), P("data")), check_vma=False)
```

```python
import contextlib
import math

import jax
import jax.numpy as jnp
import numpy as np
from jax import lax
from jax.experimental import pallas as pl
from jax.experimental.pallas import tpu as pltpu
from jax.sharding import PartitionSpec as P

SOLVER_STEPS = 20
DEVICES = 32
DIM, HID, TOK, CLS = 384, 1536, 1024, 10
CHUNKS, TASKS = 3, 2
F32, BF16 = jnp.float32, jnp.bfloat16
GELU_C = 0.7978845608028654
GELU_A = 0.044715
PAIRS = ((0, 1), (1, 0), (1, 1))

PIECES = (((1, 0, 1), (0, 0, 1), (0, 1, 0), (0, 2, 0)),
          ((1, 0, 0), (1, 1, 0), (1, 2, 0), (1, 2, 1)),
          ((0, 0, 0), (1, 1, 1), (0, 1, 1), (0, 2, 1)))
ROUTE = {piece: (r, n) for r, pieces in enumerate(PIECES) for n, piece in enumerate(pieces)}
COLS = (512, DIM)
PLANE = (96, 128)
TILE = ((3, 8, 256), (16, DIM))


def no_scope(name):
    return contextlib.nullcontext()


scope = no_scope


def owner(z, y, x, c):
    return 8 * z + 4 * y + 2 * x + c


def tiles(owners):
    return [12 * o + i for o in owners for i in range(8)] + [12 * o + i for o in owners for i in range(8, 12)]


def owners(route):
    two = range(2)
    if route == 0:
        return [[[owner(z, y, x, c) for z in range(4)] for y in two] for x in two for c in two]
    if route == 1:
        return [[[owner(z, y, x, c) for z in range(4)] for x in two] for y in two for c in two]
    return [[[owner(2 * zh + zl, y, x, c) for zh in two] for y in two for x in two] for zl in two for c in two]


def select_matrices():
    mat = np.zeros((2, DIM, DIM), np.float32)
    for m, route in zip(mat, (0, 2)):
        order = [r for first in owners(route) for second in first for r in tiles(second)]
        m[np.arange(DIM), np.array(order)] = 1.0
    return mat


def scoped(f):
    def call(*args):
        with scope("_".join([f.__name__, *map(str, args)])):
            return f(*args)
    return call


def dot(a, b, dims):
    return lax.dot_general(a, b, (dims, ((), ())), preferred_element_type=F32)


def kernel(x_hbm, w1_hbm, w2_hbm, heads_hbm, lab_hbm, mask_hbm, sel_hbm,
           gin_hbm, gout_hbm, gram_hbm,
           x_ref, w1_ref, w2_ref, heads_ref, lab_ref, mask_ref, sel_ref,
           gin_ref, gout_ref, gram_out,
           xt_ref, act_ref, pre_ref, cdf_ref, xsel_ref, dzt_ref, dz_ref, cnt_ref, gram_ref, *rest):
    bufs = {piece: rest[6 * i:6 * (i + 1)] for i, piece in enumerate(ROUTE)}
    in_sem, out_sem, s1_rsem, s2_rsem, s3_rsem, ssem, cnt_ssem, cnt_rsem, gram_ssem, gram_rsem = rest[6 * len(bufs):]
    me = lax.axis_index("data")
    core = lax.rem(me, 2)
    px = lax.rem(me // 2, 2)
    py = lax.rem(me // 4, 2)
    pz = me // 8
    zl, zh = lax.rem(pz, 2), pz // 2

    def device(z, y, x, c):
        return (owner(z, y, x, c),)

    def flip(v, d):
        return lax.rem(v + d, 2)

    def remote(src, dst, ssem, rsem, dev):
        return pltpu.make_async_remote_copy(src_ref=src, dst_ref=dst, send_sem=ssem, recv_sem=rsem,
                                            device_id=dev, device_id_type=pl.DeviceIdType.MESH)

    loads = {name: pltpu.make_async_copy(src, dst, in_sem.at[i]) for i, (name, src, dst) in enumerate((
        ("mask", mask_hbm, mask_ref), ("x", x_hbm, x_ref), ("w1", w1_hbm, w1_ref), ("w2", w2_hbm, w2_ref),
        ("heads", heads_hbm, heads_ref), ("lab", lab_hbm, lab_ref), ("sel", sel_hbm, sel_ref)))}
    for load in loads.values():
        load.start()

    barrier = pltpu.get_barrier_semaphore()

    @pl.loop(1, DEVICES)
    def _(d):
        pl.semaphore_signal(barrier, inc=1, device_id=(lax.rem(me + d, DEVICES),),
                            device_id_type=pl.DeviceIdType.MESH)

    def row_copy(buf, ssem, rsem, d):
        return remote(buf.at[me], buf.at[me], ssem, rsem, (lax.rem(me + d, DEVICES),))

    def row_start(buf, ssem, rsem):
        @pl.loop(1, DEVICES)
        def _(d):
            row_copy(buf, ssem, rsem, d).start()

    def row_all(buf, ssem, rsem):
        rows = buf.at[pl.ds(0, DEVICES - 1)]
        return remote(rows, rows, ssem, rsem, (lax.rem(me + 1, DEVICES),))

    lane = lax.broadcasted_iota(jnp.int32, (1, 128), 1)

    def lane_pick(row, k):
        return jnp.sum(jnp.where(lane == k, row, 0.0), axis=1, keepdims=True)

    loads["mask"].wait()
    counts = jnp.sum(mask_ref[...].astype(F32), axis=1, keepdims=True)
    cnt_ref[me] = jnp.where(lane == 0, counts[0:1], jnp.where(lane == 1, counts[1:2], 0.0))

    def forward(i):
        cols = slice(i * 384, (i + 1) * 384)
        pre = dot(w1_ref[:, cols], xt_ref[...], ((0,), (0,)))
        cdf = 0.5 + 0.5 * jnp.tanh(pre * (GELU_C + (GELU_C * GELU_A) * (pre * pre)))
        act_ref[8 * i:8 * (i + 1)] = (pre * cdf).astype(BF16).reshape(8, CHUNKS, 16, TOK)
        pre_ref[cols, :] = pre
        cdf_ref[cols, :] = cdf

    with scope("xt"):
        loads["x"].wait()
        xt_ref[...] = jnp.transpose(x_ref[...])
    with scope("fwd"):
        loads["w1"].wait()
        forward(0)
        forward(1)
    with scope("barrier"):
        pl.semaphore_wait(barrier, DEVICES - 1)
        row_start(cnt_ref, cnt_ssem, cnt_rsem)
    with scope("fwd2"):
        forward(2)
        forward(3)
    with scope("zt"):
        loads["w2"].wait()
        zt = dot(w2_ref[...], act_ref[...].reshape(HID, TOK), ((0,), (0,)))
        zt = (xt_ref[...].astype(F32) + zt).astype(BF16)

    with scope("cls"):
        loads["heads"].wait()
        loads["lab"].wait()
        cls = lax.broadcasted_iota(jnp.int32, (CLS, TOK), 0)
        for t in range(TASKS):
            head = heads_ref[:, t, :]
            logits = dot(head, zt, ((1,), (0,)))
            ex = jnp.exp(logits - jnp.max(logits, axis=0, keepdims=True))
            prob = ex / jnp.sum(ex, axis=0, keepdims=True)
            onehot = jnp.where(lab_ref[t:t + 1, :] == cls, 1.0, 0.0)
            err = (mask_ref[t:t + 1, :].astype(F32) * (prob - onehot)).astype(BF16)
            dzt = dot(head, err, ((0,), (0,))).astype(BF16)
            dzt_ref[t] = dzt
            dz_ref[:, t * DIM:(t + 1) * DIM] = jnp.transpose(dzt)

    inv = []

    def wait_counts():
        with scope("cntwait"):
            row_all(cnt_ref, cnt_ssem, cnt_rsem).wait_recv()
            total = jnp.sum(cnt_ref[...], axis=0)
            inv.extend(1.0 / jnp.maximum(lane_pick(total, t), 1.0) for t in range(TASKS))

    @scoped
    def compute_b(k, *tasks):
        part = dot(act_ref[:, k].reshape(512, TOK), dz_ref[:, tasks[0] * DIM:(tasks[-1] + 1) * DIM], ((1,), (0,)))
        if not inv:
            wait_counts()
        for i, t in enumerate(tasks):
            scaled = (part[:, i * DIM:(i + 1) * DIM] * inv[t]).astype(BF16)
            send = bufs[1, k, t][0]
            for slot, first in enumerate(owners(ROUTE[1, k, t][0])):
                for n, j in enumerate(o for second in first for o in second):
                    send[slot, 16 * n:16 * (n + 1)] = scaled[16 * j:16 * (j + 1)]

    @scoped
    def compute_a(k, t):
        rows = slice(512 * k, 512 * (k + 1))
        back = dot(w2_ref[rows, :], dzt_ref[t], ((1,), (0,)))
        pre, cdf = pre_ref[rows, :], cdf_ref[rows, :]
        slope = cdf + (pre * cdf) * (1.0 - cdf) * (2.0 * GELU_C + (6.0 * GELU_C * GELU_A) * (pre * pre))
        dpre = (back * slope).astype(BF16)
        part = dot(xsel_ref[ROUTE[0, k, t][0] // 2], dpre, ((1,), (1,)))
        bufs[0, k, t][0][...] = (part * inv[t]).astype(BF16).reshape(4, 96, 512)

    def select_rows(r):
        xsel_ref[r] = dot(sel_ref[r], xt_ref[...], ((1,), (0,))).astype(BF16)

    def s1_copies(route, n):
        send, recv = bufs[PIECES[route][n]][:2]
        for p, (d, dc) in reversed(list(enumerate(PAIRS))):
            c = flip(core, dc)
            g = flip((px, py, zl)[route], d)
            dev = (device(pz, py, g, c), device(pz, g, px, c), device(2 * zh + g, py, px, c))[route]
            yield remote(send.at[g * 2 + c], recv.at[p], ssem.at[0], s1_rsem.at[route, n], dev)

    def s2_copies(route, n):
        send, recv = bufs[PIECES[route][n]][2:4]
        if route == 2:
            for p, (dy, dx) in reversed(list(enumerate(PAIRS))):
                y, x = flip(py, dy), flip(px, dx)
                yield remote(send.at[2 * y + x], recv.at[p], ssem.at[1], s2_rsem.at[route, n],
                             device(pz, y, x, core))
            return
        g = flip((py, px)[route], 1)
        dev = (device(pz, g, px, core), device(pz, py, g, core))[route]
        yield remote(send.at[g], recv.at[0], ssem.at[1], s2_rsem.at[route, n], dev)

    def s3_copies(route, n):
        send, recv = bufs[PIECES[route][n]][4:6]
        if route == 2:
            yield remote(send.at[flip(zh, 1)], recv.at[0], ssem.at[2], s3_rsem.at[route, n],
                         device(lax.rem(pz + 2, 4), py, px, core))
            return
        for d in (2, 1, 3):
            z = lax.rem(pz + d, 4)
            yield remote(send.at[z], recv.at[d - 1], ssem.at[2], s3_rsem.at[route, n], device(z, py, px, core))

    def whole(ref, sem):
        return remote(ref, ref, sem, sem, device(lax.rem(pz + 1, 4), py, px, core))

    def total_of(own, recv, sem):
        whole(recv, sem).wait_recv()
        terms = [own.astype(F32)] + [recv[i].astype(F32) for i in range(recv.shape[0])]
        while len(terms) > 1:
            terms = [a + b for a, b in zip(terms[::2], terms[1::2])]
        return terms[0]

    @scoped
    def s1_start(route, n):
        for copy in s1_copies(route, n):
            copy.start()

    @scoped
    def s1_finish(route, n):
        send, recv, out = bufs[PIECES[route][n]][:3]
        tot = total_of(send[(px, py, zl)[route] * 2 + core], recv, s1_rsem.at[route, n])
        out[...] = tot.reshape(out.shape)
        for copy in s2_copies(route, n):
            copy.start()

    @scoped
    def s2_finish(route, n):
        part = PIECES[route][n][0]
        send, recv, out = bufs[PIECES[route][n]][2:5]
        tot = total_of(send[(py, px, 2 * py + px)[route]], recv, s2_rsem.at[route, n])
        count = out.shape[0]
        if part == 0:
            for z in range(count):
                top = tot[8 * z:8 * (z + 1)]
                low = tot[8 * count + 4 * z:8 * count + 4 * (z + 1)]
                out[z, 0] = top[:, :256]
                out[z, 1] = top[:, 256:]
                out[z, 2] = jnp.concatenate([low[:, :256], low[:, 256:]], axis=0)
        else:
            out[...] = tot.reshape(out.shape)
        for copy in s3_copies(route, n):
            copy.start()

    @scoped
    def s3_finish(route, n):
        part, k, t = PIECES[route][n]
        send, recv = bufs[PIECES[route][n]][4:6]
        tot = total_of(send[zh if route == 2 else pz], recv, s3_rsem.at[route, n])
        if part == 0:
            for j in range(4):
                cols = slice(128 * (j % 2), 128 * (j % 2 + 1))
                gin_ref[t, pl.ds(4 * k + j, 8, stride=12), :] = tot[j // 2, :, cols]
                gin_ref[t, pl.ds(96 + 4 * k + j, 4, stride=12), :] = tot[2, 4 * (j // 2):4 * (j // 2 + 1), cols]
        else:
            for j in range(3):
                gout_ref[t, pl.ds(48 * k + j, 16, stride=3), :] = tot[:, 128 * j:128 * (j + 1)]

    x, y, z = range(3)

    def each(f, n, *routes):
        for r in routes:
            f(r, n)

    compute_b(0, 0)
    s1_start(y, 0)
    compute_b(0, 1)
    s1_start(x, 0)
    loads["sel"].wait()
    select_rows(1)
    compute_a(0, 0)
    s1_start(z, 0)
    select_rows(0)
    compute_a(0, 1)
    s1_start(x, 1)
    compute_b(1, 0, 1)
    each(s1_start, 1, y, z)
    compute_a(1, 0)
    each(s1_finish, 0, y, x)
    s1_start(x, 2)
    compute_b(2, 0, 1)
    s1_start(y, 2)
    compute_a(1, 1)
    s1_start(z, 2)
    each(s1_finish, 1, y, x)
    s1_start(y, 3)
    compute_a(2, 0)
    s1_start(x, 3)
    compute_a(2, 1)
    s1_start(z, 3)
    each(s2_finish, 0, y, x)
    each(s1_finish, 2, y, x)
    each(s2_finish, 1, y, x)
    each(s1_finish, 3, y, x)
    for n in range(4):
        s1_finish(z, n)
    for n in (2, 3):
        each(s3_finish, n - 2, y, x)
        each(s2_finish, n, y, x)
    for n in range(4):
        s2_finish(z, n)
    for n in (2, 3):
        each(s3_finish, n, y, x)
    for n in range(4):
        s3_finish(z, n)

    stores = [pltpu.make_async_copy(src, dst, out_sem.at[i])
              for i, (src, dst) in enumerate(((gin_ref, gin_hbm), (gout_ref, gout_hbm), (gram_out, gram_hbm)))]
    with scope("gram"):
        row = jnp.zeros((1, 128), F32)
        for q, (s, t) in enumerate(((0, 0), (0, 1), (1, 1))):
            prod = gin_ref[s] * gin_ref[t] + gout_ref[s] * gout_ref[t]
            one = jnp.sum(jnp.sum(prod, axis=0, keepdims=True), axis=1, keepdims=True)
            row = jnp.where(lane == q, one, row)
        gram_ref[me] = row
    with scope("gramx"):
        row_start(gram_ref, gram_ssem, gram_rsem)
        stores[0].start()
        stores[1].start()
        for stage in range(3):
            sent = sum(math.prod(b[2 * stage + 1].shape) * (2 if stage == 0 else 4) for b in bufs.values())
            whole(pre_ref.at[pl.ds(0, sent // (4 * TOK))], ssem.at[stage]).wait_send()
        row_all(cnt_ref, cnt_ssem, cnt_rsem).wait_send()
        stores[0].wait()
        stores[1].wait()
        row_all(gram_ref, gram_ssem, gram_rsem).wait_recv()
    with scope("drain"):
        gram_out[...] = jnp.sum(gram_ref[...], axis=0)
        stores[2].start()
        row_all(gram_ref, gram_ssem, gram_rsem).wait_send()
        stores[2].wait()


def combine(gram_hbm, gin_hbm, gout_hbm, weights_ref, sum_in, sum_out, gram_ref, gin_ref, gout_ref, sem):
    loads = [pltpu.make_async_copy(src, dst, sem.at[i])
             for i, (src, dst) in enumerate(((gram_hbm, gram_ref), (gin_hbm, gin_ref), (gout_hbm, gout_ref)))]
    for load in loads:
        load.start()
    loads[0].wait()
    lane = lax.broadcasted_iota(jnp.int32, (1, 128), 1)
    m00, m01, m11 = [jnp.broadcast_to(jnp.sum(jnp.where(lane == q, gram_ref[...], 0.0), axis=1, keepdims=True), (1, 128))
                     for q in range(3)]
    scale = (m00 + m11) / 2.0
    w0 = jnp.full((1, 128), 0.5, F32)
    w1 = w0
    for _ in range(SOLVER_STEPS):
        r0 = w0 * jnp.exp(-(m00 * w0 + m01 * w1) / scale)
        r1 = w1 * jnp.exp(-(m01 * w0 + m11 * w1) / scale)
        norm = r0 + r1
        w0 = r0 / norm
        w1 = r1 / norm
    weights_ref[0] = w0[0, 0]
    weights_ref[1] = w1[0, 0]
    loads[1].wait()
    loads[2].wait()
    sum_in[...] = w0 * gin_ref[0] + w1 * gin_ref[1]
    sum_out[...] = w0 * gout_ref[0] + w1 * gout_ref[1]


def solution(mesh):
    sel = select_matrices()

    def local_step(x_loc, w_in, w_out, task_heads, lab_loc, mask_loc):
        vmem = pl.BlockSpec(memory_space=pltpu.VMEM)
        hbm = pl.BlockSpec(memory_space=pl.ANY)
        dma = pltpu.SemaphoreType.DMA
        heads_t = jnp.transpose(task_heads, (2, 0, 1))
        args = (x_loc, w_in, w_out, heads_t, lab_loc, mask_loc, jnp.asarray(sel, BF16))
        piece = jax.ShapeDtypeStruct((144, 128), F32)
        outs = [jax.ShapeDtypeStruct((TASKS, 144, 128), F32)] * 2 + [jax.ShapeDtypeStruct((1, 128), F32)]
        scratch = [pltpu.VMEM(a.shape, a.dtype) for a in args] + [pltpu.VMEM(a.shape, a.dtype) for a in outs] + [
            pltpu.VMEM((DIM, TOK), BF16),
            pltpu.VMEM((32, CHUNKS, 16, TOK), BF16),
            pltpu.VMEM((HID, TOK), F32),
            pltpu.VMEM((HID, TOK), F32),
            pltpu.VMEM((2, DIM, TOK), BF16),
            pltpu.VMEM((TASKS, DIM, TOK), BF16),
            pltpu.VMEM((TOK, TASKS * DIM), BF16),
            pltpu.VMEM((DEVICES, 1, 128), F32),
            pltpu.VMEM((DEVICES, 1, 128), F32)]
        for (part, k, t), (route, n) in ROUTE.items():
            fan = 4 if route == 2 else 2
            rows, cols = PLANE[part], COLS[part]
            scratch += [pltpu.VMEM((4, rows, cols), BF16), pltpu.VMEM((3, rows, cols), BF16),
                        pltpu.VMEM((fan, rows // fan, cols), F32), pltpu.VMEM((fan - 1, rows // fan, cols), F32),
                        pltpu.VMEM((8 // fan,) + TILE[part], F32), pltpu.VMEM((8 // fan - 1,) + TILE[part], F32)]
        scratch += [dma((len(args),)), dma((3,)), dma((3, 4)), dma((3, 4)), dma((3, 4)), dma((3,)),
                    dma, dma, dma, dma]
        gin, gout, gram = pl.pallas_call(
            kernel,
            out_shape=outs,
            in_specs=[hbm] * len(args),
            out_specs=[hbm] * 3,
            scratch_shapes=scratch,
            compiler_params=pltpu.CompilerParams(collective_id=0, has_side_effects=True,
                                                 vmem_limit_bytes=66_900_000),
            name="step",
        )(*args)
        weights, grad_in, grad_out = pl.pallas_call(
            combine,
            out_shape=[jax.ShapeDtypeStruct((TASKS,), F32), piece, piece],
            in_specs=[hbm] * 3,
            out_specs=[pl.BlockSpec(memory_space=pltpu.SMEM), vmem, vmem],
            scratch_shapes=[pltpu.VMEM(outs[2].shape, F32), pltpu.VMEM(outs[0].shape, F32),
                            pltpu.VMEM(outs[1].shape, F32), dma((3,))],
            compiler_params=pltpu.CompilerParams(vmem_limit_bytes=66_900_000),
            name="combine",
        )(gram, gin, gout)
        return weights, grad_in.reshape(-1), grad_out.reshape(-1)

    return jax.shard_map(local_step, mesh=mesh,
                         in_specs=(P("data", None), P(), P(), P(), P(None, "data"), P(None, "data")),
                         out_specs=(P(), P("data"), P("data")), check_vma=False)
```

```python
import contextlib
import itertools
import math

import jax
import jax.numpy as jnp
import numpy as np
from jax import lax
from jax.experimental import pallas as pl
from jax.experimental.pallas import tpu as pltpu
from jax.sharding import PartitionSpec as P

SOLVER_STEPS = 20
DEVICES = 32
DIM, HID, TOK, CLS = 384, 1536, 1024, 10
CHUNKS, TASKS = 3, 2
F32, BF16 = jnp.float32, jnp.bfloat16
GELU_C = 0.7978845608028654
GELU_A = 0.044715

ROUTES = {"x": ("x", "y", "zl", "zh"), "y": ("y", "x", "zl", "zh"), "z": ("zl", "xy", "zh"),
          "zyx": ("zl", "y", "x", "zh"), "zxy": ("zl", "x", "y", "zh")}
X = ((1, 0, 1), (0, 0, 1), (0, 1, 0), (0, 2, 0))
Y = ((1, 0, 0), (1, 1, 0), (1, 2, 0), (1, 2, 1))
Z = ((0, 0, 0), (1, 1, 1), (0, 1, 1), (0, 2, 1))
PATH = dict.fromkeys(X, ROUTES["x"]) | dict.fromkeys(Y, ROUTES["y"]) | {
    Z[0]: ROUTES["zyx"], Z[1]: ROUTES["zxy"], Z[2]: ROUTES["z"], Z[3]: ROUTES["z"]}
NUMBER = {piece: i for i, piece in enumerate(PATH)}
COLS = (512, DIM)
PLANE = (96, 128)
TILE = ((3, 8, 256), (16, DIM))


def no_scope(name):
    return contextlib.nullcontext()


scope = no_scope


def owner(z, y, x, c):
    return 8 * z + 4 * y + 2 * x + c


def tiles(owners):
    return [12 * o + i for o in owners for i in range(8)] + [12 * o + i for o in owners for i in range(8, 12)]


def axes_of(stage):
    return ("y", "x") if stage == "xy" else (stage,)


def owners(path):
    def points(axes):
        return [dict(zip(axes, bits)) for bits in itertools.product(range(2), repeat=len(axes))]

    def number(at):
        return owner(2 * at["zh"] + at["zl"], at["y"], at["x"], at["c"])

    rest = [axis for stage in path[2:] for axis in axes_of(stage)]
    return [[[number(p | q | r) for r in points(rest)] for q in points(axes_of(path[1]))] for p in points((path[0], "c"))]


def orders_of_rows():
    paths = list(dict.fromkeys(path for piece, path in PATH.items() if piece[0] == 0))
    orders = [tuple(r for first in owners(path) for second in first for r in tiles(second)) for path in paths]
    kinds = list(dict.fromkeys(orders))
    return kinds, {path: kinds.index(order) for path, order in zip(paths, orders)}


ORDERS, ORDER_OF = orders_of_rows()


def select_matrices():
    mat = np.zeros((len(ORDERS), DIM, DIM), np.float32)
    for m, order in zip(mat, ORDERS):
        m[np.arange(DIM), np.array(order)] = 1.0
    return mat


def buffers(part, path):
    rows, cols, fan = PLANE[part], COLS[part], 2 ** len(axes_of(path[1]))
    shapes = [((4, rows, cols), BF16), ((3, rows, cols), BF16),
              ((fan, rows // fan, cols), F32), ((fan - 1, rows // fan, cols), F32)]
    for left in range(len(path) - 3, -1, -1):
        shapes += [((2,) * (left + 1) + TILE[part], F32), ((1,) + (2,) * left + TILE[part], F32)]
    return shapes


def scoped(f):
    def call(*args):
        with scope("_".join([f.__name__, *map(str, args)])):
            return f(*args)
    return call


def dot(a, b, dims):
    return lax.dot_general(a, b, (dims, ((), ())), preferred_element_type=F32)


def kernel(x_hbm, w1_hbm, w2_hbm, heads_hbm, lab_hbm, mask_hbm, sel_hbm,
           gin_hbm, gout_hbm, gram_out,
           x_ref, w1_ref, w2_ref, heads_ref, lab_ref, mask_ref, sel_ref,
           gin_ref, gout_ref, xt_ref, act_ref, pre_ref, cdf_ref, xsel_ref, dzt_ref, dz_ref, cnt_ref, gram_ref, *rest):
    rest = list(rest)
    bufs = {piece: [rest.pop(0) for _ in range(2 * len(path))] for piece, path in PATH.items()}
    in_sem, out_sem, rsem, ssem, cnt_ssem, cnt_rsem, gram_ssem, gram_rsem = rest
    me = lax.axis_index("data")
    core = lax.rem(me, 2)
    px = lax.rem(me // 2, 2)
    py = lax.rem(me // 4, 2)
    pz = me // 8
    zl, zh = lax.rem(pz, 2), pz // 2

    here = {"x": px, "y": py, "c": core, "zl": zl, "zh": zh}

    def peer(at):
        at = here | at
        return (owner(2 * at["zh"] + at["zl"], at["y"], at["x"], at["c"]),)

    def flip(v, d):
        return lax.rem(v + d, 2)

    def remote(src, dst, ssem, rsem, dev):
        return pltpu.make_async_remote_copy(src_ref=src, dst_ref=dst, send_sem=ssem, recv_sem=rsem,
                                            device_id=dev, device_id_type=pl.DeviceIdType.MESH)

    loads = {name: pltpu.make_async_copy(src, dst, in_sem.at[i]) for i, (name, src, dst) in enumerate((
        ("x", x_hbm, x_ref), ("w1", w1_hbm, w1_ref), ("mask", mask_hbm, mask_ref), ("w2", w2_hbm, w2_ref),
        ("heads", heads_hbm, heads_ref), ("lab", lab_hbm, lab_ref), ("sel", sel_hbm, sel_ref)))}
    for load in loads.values():
        load.start()

    others = []
    for z in (3 - pz, lax.rem(pz + 2, 4), pz + 1 - 2 * zl, pz):
        for dy, dx, dc in itertools.product((1, 0), repeat=3):
            others.append((owner(z, flip(py, dy), flip(px, dx), flip(core, dc)),))
    others.pop()

    barrier = pltpu.get_barrier_semaphore()
    for dev in others:
        pl.semaphore_signal(barrier, inc=1, device_id=dev, device_id_type=pl.DeviceIdType.MESH)

    def row_start(buf, ssem, rsem):
        for dev in others:
            remote(buf.at[me], buf.at[me], ssem, rsem, dev).start()

    def row_all(buf, ssem, rsem):
        rows = buf.at[pl.ds(0, DEVICES - 1)]
        return remote(rows, rows, ssem, rsem, others[0])

    lane = lax.broadcasted_iota(jnp.int32, (1, 128), 1)

    def lane_pick(row, k):
        return jnp.sum(jnp.where(lane == k, row, 0.0), axis=1, keepdims=True)

    def forward(i):
        cols = slice(i * 384, (i + 1) * 384)
        pre = dot(w1_ref[:, cols], xt_ref[...], ((0,), (0,)))
        cdf = 0.5 + 0.5 * jnp.tanh(pre * (GELU_C + (GELU_C * GELU_A) * (pre * pre)))
        act_ref[8 * i:8 * (i + 1)] = (pre * cdf).astype(BF16).reshape(8, CHUNKS, 16, TOK)
        pre_ref[cols, :] = pre
        cdf_ref[cols, :] = cdf

    with scope("xt"):
        loads["x"].wait()
        xt_ref[...] = jnp.transpose(x_ref[...])
    with scope("fwd"):
        loads["w1"].wait()
        forward(0)
        forward(1)
        loads["mask"].wait()
        counts = jnp.sum(mask_ref[...].astype(F32), axis=1, keepdims=True)
        cnt_ref[me] = jnp.where(lane == 0, counts[0:1], jnp.where(lane == 1, counts[1:2], 0.0))
    with scope("barrier"):
        pl.semaphore_wait(barrier, DEVICES - 1)
        row_start(cnt_ref, cnt_ssem, cnt_rsem)
    with scope("fwd2"):
        forward(2)
        forward(3)
    with scope("zt"):
        loads["w2"].wait()
        zt = dot(w2_ref[...], act_ref[...].reshape(HID, TOK), ((0,), (0,)))
        zt = (xt_ref[...].astype(F32) + zt).astype(BF16)

    with scope("cls"):
        loads["heads"].wait()
        loads["lab"].wait()
        cls = lax.broadcasted_iota(jnp.int32, (CLS, TOK), 0)
        for t in range(TASKS):
            head = heads_ref[:, t, :]
            logits = dot(head, zt, ((1,), (0,)))
            ex = jnp.exp(logits - jnp.max(logits, axis=0, keepdims=True))
            prob = ex / jnp.sum(ex, axis=0, keepdims=True)
            onehot = jnp.where(lab_ref[t:t + 1, :] == cls, 1.0, 0.0)
            err = (mask_ref[t:t + 1, :].astype(F32) * (prob - onehot)).astype(BF16)
            dzt = dot(head, err, ((0,), (0,))).astype(BF16)
            dzt_ref[t] = dzt
            dz_ref[:, t * DIM:(t + 1) * DIM] = jnp.transpose(dzt)

    inv = []

    def wait_counts():
        with scope("cntwait"):
            row_all(cnt_ref, cnt_ssem, cnt_rsem).wait_recv()
            total = jnp.sum(cnt_ref[...], axis=0)
            inv.extend(1.0 / jnp.maximum(lane_pick(total, t), 1.0) for t in range(TASKS))

    @scoped
    def compute_b(k, *tasks):
        part = dot(act_ref[:, k].reshape(512, TOK), dz_ref[:, tasks[0] * DIM:(tasks[-1] + 1) * DIM], ((1,), (0,)))
        if not inv:
            wait_counts()
        for i, t in enumerate(tasks):
            scaled = (part[:, i * DIM:(i + 1) * DIM] * inv[t]).astype(BF16)
            send = bufs[1, k, t][0]
            for slot, first in enumerate(owners(PATH[1, k, t])):
                for n, j in enumerate(o for second in first for o in second):
                    send[slot, 16 * n:16 * (n + 1)] = scaled[16 * j:16 * (j + 1)]

    @scoped
    def compute_a(k, t):
        rows = slice(512 * k, 512 * (k + 1))
        back = dot(w2_ref[rows, :], dzt_ref[t], ((1,), (0,)))
        pre, cdf = pre_ref[rows, :], cdf_ref[rows, :]
        slope = cdf + (pre * cdf) * (1.0 - cdf) * (2.0 * GELU_C + (6.0 * GELU_C * GELU_A) * (pre * pre))
        dpre = (back * slope).astype(BF16)
        part = dot(xsel_ref[ORDER_OF[PATH[0, k, t]]], dpre, ((1,), (1,)))
        bufs[0, k, t][0][...] = (part * inv[t]).astype(BF16).reshape(4, 96, 512)

    def select_rows(r):
        xsel_ref[r] = dot(sel_ref[r], xt_ref[...], ((1,), (0,))).astype(BF16)

    def axes(piece, i):
        return (PATH[piece][0], "c") if i == 0 else axes_of(PATH[piece][i])

    def sent_on(piece, i):
        return 3 if i + 1 == len(PATH[piece]) else i

    def index_of(at, names):
        return sum(at[name] * 2 ** (len(names) - 1 - i) for i, name in enumerate(names))

    def send_stage(piece, i):
        send, recv = bufs[piece][2 * i:2 * i + 2]
        names = axes(piece, i)
        moves = list(itertools.product(range(2), repeat=len(names)))[1:]
        for p, move in reversed(list(enumerate(moves))):
            at = {name: flip(here[name], d) for name, d in zip(names, move)}
            remote(send.at[index_of(at, names)], recv.at[p], ssem.at[sent_on(piece, i)], rsem.at[NUMBER[piece], i],
                   peer(at)).start()

    def whole(ref, sem):
        return remote(ref, ref, sem, sem, others[0])

    @scoped
    def start(piece):
        send_stage(piece, 0)

    @scoped
    def advance(i, *pieces):
        for piece in pieces:
            advance_one(piece, i)

    def advance_one(piece, i):
        part, k, t = piece
        send, recv = bufs[piece][2 * i:2 * i + 2]
        whole(recv, rsem.at[NUMBER[piece], i]).wait_recv()
        terms = [send[index_of(here, axes(piece, i))].astype(F32)]
        terms += [recv[p].astype(F32) for p in range(recv.shape[0])]
        while len(terms) > 1:
            terms = [a + b for a, b in zip(terms[::2], terms[1::2])]
        tot = terms[0]
        if i + 1 < len(PATH[piece]):
            out = bufs[piece][2 * i + 2]
            if i == 1 and part == 0:
                count = tot.shape[0] // 12
                for q in range(count):
                    at = (q,) if count == 2 else (q // 2, q % 2)
                    top = tot[8 * q:8 * (q + 1)]
                    low = tot[8 * count + 4 * q:8 * count + 4 * (q + 1)]
                    out[at + (0,)] = top[:, :256]
                    out[at + (1,)] = top[:, 256:]
                    out[at + (2,)] = jnp.concatenate([low[:, :256], low[:, 256:]], axis=0)
            else:
                out[...] = tot.reshape(out.shape)
            send_stage(piece, i + 1)
        elif part == 0:
            for j in range(4):
                cols = slice(128 * (j % 2), 128 * (j % 2 + 1))
                gin_ref[t, pl.ds(4 * k + j, 8, stride=12), :] = tot[j // 2, :, cols]
                gin_ref[t, pl.ds(96 + 4 * k + j, 4, stride=12), :] = tot[2, 4 * (j // 2):4 * (j // 2 + 1), cols]
        else:
            for j in range(3):
                gout_ref[t, pl.ds(48 * k + j, 16, stride=3), :] = tot[:, 128 * j:128 * (j + 1)]

    compute_b(0, 0)
    start(Y[0])
    compute_b(0, 1)
    start(X[0])
    loads["sel"].wait()
    select_rows(ORDER_OF[PATH[Z[0]]])
    compute_a(0, 0)
    start(Z[0])
    compute_b(1, 0)
    start(Y[1])
    select_rows(ORDER_OF[PATH[X[1]]])
    compute_a(0, 1)
    start(X[1])
    compute_b(1, 1)
    start(Z[1])
    compute_a(1, 0)
    advance(0, Y[0], X[0])
    start(X[2])
    compute_b(2, 0, 1)
    start(Y[2])
    for r in range(len(ORDERS)):
        if r not in (ORDER_OF[PATH[Z[0]]], ORDER_OF[PATH[X[1]]]):
            select_rows(r)
    compute_a(1, 1)
    start(Z[2])
    advance(0, Y[1], X[1], Z[0])
    start(Y[3])
    compute_a(2, 0)
    advance(0, Z[1])
    start(X[3])
    compute_a(2, 1)
    start(Z[3])
    advance(1, X[0], Y[0])
    advance(0, Y[2], X[2])
    advance(2, X[0], Y[0])
    advance(1, X[1], Y[1])
    advance(1, Z[0], Z[1])
    advance(2, X[1], Y[1])
    advance(0, Y[3], X[3])
    advance(0, Z[2], Z[3])
    advance(1, X[2], Y[2])
    advance(2, Z[0], Z[1])
    advance(3, X[0], Y[0])
    advance(1, X[3], Y[3])
    advance(2, X[2], Y[2])
    advance(1, Z[2])
    advance(2, X[3], Y[3])
    advance(3, X[1], Y[1])
    advance(1, Z[3])
    advance(3, Z[0], Z[1])
    advance(3, X[2], Y[2])
    advance(2, Z[2])
    advance(3, X[3], Y[3])
    advance(2, Z[3])

    stores = [pltpu.make_async_copy(src, dst, out_sem.at[i])
              for i, (src, dst) in enumerate(((gin_ref, gin_hbm), (gout_ref, gout_hbm)))]
    with scope("gram"):
        row = jnp.zeros((1, 128), F32)
        for q, (s, t) in enumerate(((0, 0), (0, 1), (1, 1))):
            prod = gin_ref[s] * gin_ref[t] + gout_ref[s] * gout_ref[t]
            one = jnp.sum(jnp.sum(prod, axis=0, keepdims=True), axis=1, keepdims=True)
            row = jnp.where(lane == q, one, row)
        gram_ref[me] = row
    with scope("gramx"):
        row_start(gram_ref, gram_ssem, gram_rsem)
        stores[0].start()
        stores[1].start()
        for i in range(4):
            sent = [b[2 * j + 1] for piece, b in bufs.items() for j in range(len(PATH[piece])) if sent_on(piece, j) == i]
            nbytes = sum(math.prod(ref.shape) * (2 if i == 0 else 4) for ref in sent)
            whole(pre_ref.at[pl.ds(0, nbytes // (4 * TOK))], ssem.at[i]).wait_send()
        row_all(cnt_ref, cnt_ssem, cnt_rsem).wait_send()
        stores[0].wait()
        stores[1].wait()
        row_all(gram_ref, gram_ssem, gram_rsem).wait_recv()
    with scope("drain"):
        gram_out[...] = jnp.sum(gram_ref[...], axis=0)
        row_all(gram_ref, gram_ssem, gram_rsem).wait_send()


def combine(gram_ref, gin_hbm, gout_hbm, weights_ref, sum_in, sum_out, gin_ref, gout_ref, sem):
    loads = [pltpu.make_async_copy(src, dst, sem.at[i])
             for i, (src, dst) in enumerate(((gin_hbm, gin_ref), (gout_hbm, gout_ref)))]
    for load in loads:
        load.start()
    lane = lax.broadcasted_iota(jnp.int32, (1, 128), 1)
    m00, m01, m11 = [jnp.broadcast_to(jnp.sum(jnp.where(lane == q, gram_ref[...], 0.0), axis=1, keepdims=True), (1, 128))
                     for q in range(3)]
    scale = (m00 + m11) / 2.0
    w0 = jnp.full((1, 128), 0.5, F32)
    w1 = w0
    for _ in range(SOLVER_STEPS):
        r0 = w0 * jnp.exp(-(m00 * w0 + m01 * w1) / scale)
        r1 = w1 * jnp.exp(-(m01 * w0 + m11 * w1) / scale)
        norm = r0 + r1
        w0 = r0 / norm
        w1 = r1 / norm
    weights_ref[0] = w0[0, 0]
    weights_ref[1] = w1[0, 0]
    for load in loads:
        load.wait()
    sum_in[...] = w0 * gin_ref[0] + w1 * gin_ref[1]
    sum_out[...] = w0 * gout_ref[0] + w1 * gout_ref[1]


def solution(mesh):
    sel = select_matrices()

    def local_step(x_loc, w_in, w_out, task_heads, lab_loc, mask_loc):
        vmem = pl.BlockSpec(memory_space=pltpu.VMEM)
        hbm = pl.BlockSpec(memory_space=pl.ANY)
        dma = pltpu.SemaphoreType.DMA
        heads_t = jnp.transpose(task_heads, (2, 0, 1))
        args = (x_loc, w_in, w_out, heads_t, lab_loc, mask_loc, jnp.asarray(sel, BF16))
        piece = jax.ShapeDtypeStruct((144, 128), F32)
        outs = [jax.ShapeDtypeStruct((TASKS, 144, 128), F32)] * 2 + [jax.ShapeDtypeStruct((1, 128), F32)]
        scratch = [pltpu.VMEM(a.shape, a.dtype) for a in args] + [pltpu.VMEM(a.shape, a.dtype) for a in outs[:2]] + [
            pltpu.VMEM((DIM, TOK), BF16),
            pltpu.VMEM((32, CHUNKS, 16, TOK), BF16),
            pltpu.VMEM((HID, TOK), F32),
            pltpu.VMEM((HID, TOK), F32),
            pltpu.VMEM((len(ORDERS), DIM, TOK), BF16),
            pltpu.VMEM((TASKS, DIM, TOK), BF16),
            pltpu.VMEM((TOK, TASKS * DIM), BF16),
            pltpu.VMEM((DEVICES, 1, 128), F32),
            pltpu.VMEM((DEVICES, 1, 128), F32)]
        scratch += [pltpu.VMEM(*shape) for piece, path in PATH.items() for shape in buffers(piece[0], path)]
        scratch += [dma((len(args),)), dma((3,)), dma((len(PATH), 4)), dma((4,)), dma, dma, dma, dma]
        gin, gout, gram = pl.pallas_call(
            kernel,
            out_shape=outs,
            in_specs=[hbm] * len(args),
            out_specs=[hbm, hbm, vmem],
            scratch_shapes=scratch,
            compiler_params=pltpu.CompilerParams(collective_id=0, has_side_effects=True,
                                                 vmem_limit_bytes=66_900_000),
            name="step",
        )(*args)
        weights, grad_in, grad_out = pl.pallas_call(
            combine,
            out_shape=[jax.ShapeDtypeStruct((TASKS,), F32), piece, piece],
            in_specs=[vmem, hbm, hbm],
            out_specs=[pl.BlockSpec(memory_space=pltpu.SMEM), vmem, vmem],
            scratch_shapes=[pltpu.VMEM(outs[0].shape, F32), pltpu.VMEM(outs[1].shape, F32), dma((2,))],
            compiler_params=pltpu.CompilerParams(vmem_limit_bytes=66_900_000),
            name="combine",
        )(gram, gin, gout)
        return weights, grad_in.reshape(-1), grad_out.reshape(-1)

    return jax.shard_map(local_step, mesh=mesh,
                         in_specs=(P("data", None), P(), P(), P(), P(None, "data"), P(None, "data")),
                         out_specs=(P(), P("data"), P("data")), check_vma=False)
```

```python
import contextlib
import itertools
import math

import jax
import jax.numpy as jnp
import numpy as np
from jax import lax
from jax.experimental import pallas as pl
from jax.experimental.pallas import tpu as pltpu
from jax.sharding import PartitionSpec as P

SOLVER_STEPS = 20
DEVICES = 32
DIM, HID, TOK, CLS = 384, 1536, 1024, 10
CHUNKS, TASKS = 3, 2
F32, BF16 = jnp.float32, jnp.bfloat16
GELU_C = 0.7978845608028654
GELU_A = 0.044715

ROUTES = {"x": ("x", "y", "zl", "zh"), "y": ("y", "x", "zl", "zh"), "z": ("zl", "xy", "zh"),
          "x3": ("x", "y", "z"), "y3": ("y", "x", "z"), "zyx": ("zl", "y", "x", "zh"), "zxy": ("zl", "x", "y", "zh")}
AXES = {"xy": ("y", "x"), "z": ("zl", "zh")}
X = ((1, 0, 1), (0, 0, 1), (0, 1, 0), (0, 2, 0))
Y = ((1, 0, 0), (1, 1, 0), (1, 2, 0), (1, 2, 1))
Z = ((0, 0, 0), (1, 1, 1), (0, 1, 1), (0, 2, 1))
CHOSEN = ("x", "x", "x3", "x3", "y", "y", "y3", "y3", "zyx", "zxy", "z", "z")
PATH = {piece: ROUTES[name] for piece, name in zip(X + Y + Z, CHOSEN)}
NUMBER = {piece: i for i, piece in enumerate(PATH)}
COLS = (512, DIM)
PLANE = (96, 128)
TILE = ((3, 8, 256), (16, DIM))


def no_scope(name):
    return contextlib.nullcontext()


scope = no_scope


def owner(z, y, x, c):
    return 8 * z + 4 * y + 2 * x + c


def tiles(owners):
    return [12 * o + i for o in owners for i in range(8)] + [12 * o + i for o in owners for i in range(8, 12)]


def axes_of(stage):
    return AXES.get(stage, (stage,))


def owners(path):
    def points(axes):
        return [dict(zip(axes, bits)) for bits in itertools.product(range(2), repeat=len(axes))]

    def number(at):
        return owner(2 * at["zh"] + at["zl"], at["y"], at["x"], at["c"])

    rest = [axis for stage in path[2:] for axis in axes_of(stage)]
    return [[[number(p | q | r) for r in points(rest)] for q in points(axes_of(path[1]))] for p in points((path[0], "c"))]


def orders_of_rows():
    paths = list(dict.fromkeys(path for piece, path in PATH.items() if piece[0] == 0))
    orders = [tuple(r for first in owners(path) for second in first for r in tiles(second)) for path in paths]
    kinds = list(dict.fromkeys(orders))
    return kinds, {path: kinds.index(order) for path, order in zip(paths, orders)}


ORDERS, ORDER_OF = orders_of_rows()


def select_matrices():
    mat = np.zeros((len(ORDERS), DIM, DIM), np.float32)
    for m, order in zip(mat, ORDERS):
        m[np.arange(DIM), np.array(order)] = 1.0
    return mat


def buffers(part, path):
    rows, cols = PLANE[part], COLS[part]
    fans = [2 ** len(axes_of(stage)) for stage in path]
    shapes = [((4, rows, cols), BF16), ((3, rows, cols), BF16),
              ((fans[1], rows // fans[1], cols), F32), ((fans[1] - 1, rows // fans[1], cols), F32)]
    for i in range(2, len(path)):
        later = tuple(fans[i + 1:])
        shapes += [((fans[i],) + later + TILE[part], F32), ((fans[i] - 1,) + later + TILE[part], F32)]
    return shapes


def scoped(f):
    def call(*args):
        with scope("_".join([f.__name__, *map(str, args)])):
            return f(*args)
    return call


def dot(a, b, dims):
    return lax.dot_general(a, b, (dims, ((), ())), preferred_element_type=F32)


def kernel(x_hbm, w1_hbm, w2_hbm, heads_hbm, lab_hbm, mask_hbm, sel_hbm,
           gin_hbm, gout_hbm, gram_out,
           x_ref, w1_ref, w2_ref, heads_ref, lab_ref, mask_ref, sel_ref,
           gin_ref, gout_ref, xt_ref, act_ref, pre_ref, cdf_ref, xsel_ref, dzt_ref, dz_ref, err_ref, cnt_ref, gram_ref, *rest):
    rest = list(rest)
    bufs = {piece: [rest.pop(0) for _ in range(2 * len(path))] for piece, path in PATH.items()}
    in_sem, out_sem, rsem, ssem, cnt_ssem, cnt_rsem, gram_ssem, gram_rsem = rest
    me = lax.axis_index("data")
    core = lax.rem(me, 2)
    px = lax.rem(me // 2, 2)
    py = lax.rem(me // 4, 2)
    pz = me // 8
    zl, zh = lax.rem(pz, 2), pz // 2

    here = {"x": px, "y": py, "c": core, "zl": zl, "zh": zh}

    def peer(at):
        at = here | at
        return (owner(2 * at["zh"] + at["zl"], at["y"], at["x"], at["c"]),)

    def flip(v, d):
        return lax.rem(v + d, 2)

    def remote(src, dst, ssem, rsem, dev):
        return pltpu.make_async_remote_copy(src_ref=src, dst_ref=dst, send_sem=ssem, recv_sem=rsem,
                                            device_id=dev, device_id_type=pl.DeviceIdType.MESH)

    loads = {name: pltpu.make_async_copy(src, dst, in_sem.at[i]) for i, (name, src, dst) in enumerate((
        ("x", x_hbm, x_ref), ("w1", w1_hbm, w1_ref), ("mask", mask_hbm, mask_ref), ("w2", w2_hbm, w2_ref),
        ("heads", heads_hbm, heads_ref), ("lab", lab_hbm, lab_ref), ("sel", sel_hbm, sel_ref)))}
    for load in loads.values():
        load.start()

    others = []
    for z in (3 - pz, lax.rem(pz + 2, 4), pz + 1 - 2 * zl, pz):
        for dy, dx, dc in itertools.product((1, 0), repeat=3):
            others.append((owner(z, flip(py, dy), flip(px, dx), flip(core, dc)),))
    others.pop()

    barrier = pltpu.get_barrier_semaphore()
    for dev in others:
        pl.semaphore_signal(barrier, inc=1, device_id=dev, device_id_type=pl.DeviceIdType.MESH)

    def row_start(buf, ssem, rsem):
        for dev in others:
            remote(buf.at[me], buf.at[me], ssem, rsem, dev).start()

    def row_all(buf, ssem, rsem):
        rows = buf.at[pl.ds(0, DEVICES - 1)]
        return remote(rows, rows, ssem, rsem, others[0])

    lane = lax.broadcasted_iota(jnp.int32, (1, 128), 1)

    def lane_pick(row, k):
        return jnp.sum(jnp.where(lane == k, row, 0.0), axis=1, keepdims=True)

    def forward(i):
        cols = slice(i * 384, (i + 1) * 384)
        pre = dot(w1_ref[:, cols], xt_ref[...], ((0,), (0,)))
        cdf = 0.5 + 0.5 * jnp.tanh(pre * (GELU_C + (GELU_C * GELU_A) * (pre * pre)))
        act_ref[8 * i:8 * (i + 1)] = (pre * cdf).astype(BF16).reshape(8, CHUNKS, 16, TOK)
        pre_ref[cols, :] = pre
        cdf_ref[cols, :] = cdf

    with scope("xt"):
        loads["x"].wait()
        xt_ref[...] = jnp.transpose(x_ref[...])
    with scope("fwd"):
        loads["w1"].wait()
        forward(0)
        forward(1)
        loads["mask"].wait()
        counts = jnp.sum(mask_ref[...].astype(F32), axis=1, keepdims=True)
        cnt_ref[me] = jnp.where(lane == 0, counts[0:1], jnp.where(lane == 1, counts[1:2], 0.0))
    with scope("barrier"):
        pl.semaphore_wait(barrier, DEVICES - 1)
        row_start(cnt_ref, cnt_ssem, cnt_rsem)
    with scope("fwd2"):
        forward(2)
        forward(3)
    with scope("zt"):
        loads["w2"].wait()
        zt = dot(w2_ref[...], act_ref[...].reshape(HID, TOK), ((0,), (0,)))
        zt = (xt_ref[...].astype(F32) + zt).astype(BF16)

    with scope("cls"):
        loads["heads"].wait()
        loads["lab"].wait()
        pad = jnp.zeros((16 - CLS, DIM), BF16)
        heads = jnp.concatenate([heads_ref[:, 0, :], pad, heads_ref[:, 1, :], pad], axis=0)
        logits = dot(heads, zt, ((1,), (0,)))
        cls = lax.broadcasted_iota(jnp.int32, (16, TOK), 0)
        for t in range(TASKS):
            score = jnp.where(cls < CLS, logits[16 * t:16 * (t + 1)], -jnp.inf)
            ex = jnp.exp(score - jnp.max(score, axis=0, keepdims=True))
            prob = ex / jnp.sum(ex, axis=0, keepdims=True)
            onehot = jnp.where(lab_ref[t:t + 1, :] == cls, 1.0, 0.0)
            err_ref[t] = (mask_ref[t:t + 1, :].astype(F32) * (prob - onehot)).astype(BF16)
            head = heads[16 * t:16 * (t + 1)]
            dz_ref[:, t * DIM:(t + 1) * DIM] = dot(err_ref[t], head, ((0,), (0,))).astype(BF16)

    def compute_dzt():
        for t in range(TASKS):
            dzt_ref[t] = dot(heads[16 * t:16 * (t + 1)], err_ref[t], ((0,), (0,))).astype(BF16)

    inv = []

    def wait_counts():
        with scope("cntwait"):
            row_all(cnt_ref, cnt_ssem, cnt_rsem).wait_recv()
            total = jnp.sum(cnt_ref[...], axis=0)
            inv.extend(1.0 / jnp.maximum(lane_pick(total, t), 1.0) for t in range(TASKS))

    @scoped
    def compute_b(k, *tasks):
        part = dot(act_ref[:, k].reshape(512, TOK), dz_ref[:, tasks[0] * DIM:(tasks[-1] + 1) * DIM], ((1,), (0,)))
        if not inv:
            wait_counts()
        for i, t in enumerate(tasks):
            scaled = (part[:, i * DIM:(i + 1) * DIM] * inv[t]).astype(BF16)
            send = bufs[1, k, t][0]
            for slot, first in enumerate(owners(PATH[1, k, t])):
                for n, j in enumerate(o for second in first for o in second):
                    send[slot, 16 * n:16 * (n + 1)] = scaled[16 * j:16 * (j + 1)]

    @scoped
    def compute_a(k, t):
        rows = slice(512 * k, 512 * (k + 1))
        back = dot(w2_ref[rows, :], dzt_ref[t], ((1,), (0,)))
        pre, cdf = pre_ref[rows, :], cdf_ref[rows, :]
        slope = cdf + (pre * cdf) * (1.0 - cdf) * (2.0 * GELU_C + (6.0 * GELU_C * GELU_A) * (pre * pre))
        dpre = (back * slope).astype(BF16)
        part = dot(xsel_ref[ORDER_OF[PATH[0, k, t]]], dpre, ((1,), (1,)))
        bufs[0, k, t][0][...] = (part * inv[t]).astype(BF16).reshape(4, 96, 512)

    def select_rows(r):
        xsel_ref[r] = dot(sel_ref[r], xt_ref[...], ((1,), (0,))).astype(BF16)

    def axes(piece, i):
        return (PATH[piece][0], "c") if i == 0 else axes_of(PATH[piece][i])

    def sent_on(piece, i):
        return 3 if i + 1 == len(PATH[piece]) else i

    def index_of(at, names):
        return sum(at[name] * 2 ** (len(names) - 1 - i) for i, name in enumerate(names))

    def send_stage(piece, i):
        send, recv = bufs[piece][2 * i:2 * i + 2]
        names = axes(piece, i)
        moves = list(itertools.product(range(2), repeat=len(names)))[1:]
        for p, move in reversed(list(enumerate(moves))):
            at = {name: flip(here[name], d) for name, d in zip(names, move)}
            remote(send.at[index_of(at, names)], recv.at[p], ssem.at[sent_on(piece, i)], rsem.at[NUMBER[piece], i],
                   peer(at)).start()

    def whole(ref, sem):
        return remote(ref, ref, sem, sem, others[0])

    @scoped
    def start(piece):
        send_stage(piece, 0)

    @scoped
    def advance(i, *pieces):
        for piece in pieces:
            advance_one(piece, i)

    def advance_one(piece, i):
        part, k, t = piece
        send, recv = bufs[piece][2 * i:2 * i + 2]
        whole(recv, rsem.at[NUMBER[piece], i]).wait_recv()
        terms = [send[index_of(here, axes(piece, i))].astype(F32)]
        terms += [recv[p].astype(F32) for p in range(recv.shape[0])]
        while len(terms) > 1:
            terms = [a + b for a, b in zip(terms[::2], terms[1::2])]
        tot = terms[0]
        if i + 1 < len(PATH[piece]):
            out = bufs[piece][2 * i + 2]
            if i == 1 and part == 0:
                count = tot.shape[0] // 12
                for q in range(count):
                    at = (q,) if out.shape[0] == count else (q // 2, q % 2)
                    top = tot[8 * q:8 * (q + 1)]
                    low = tot[8 * count + 4 * q:8 * count + 4 * (q + 1)]
                    out[at + (0,)] = top[:, :256]
                    out[at + (1,)] = top[:, 256:]
                    out[at + (2,)] = jnp.concatenate([low[:, :256], low[:, 256:]], axis=0)
            else:
                out[...] = tot.reshape(out.shape)
            send_stage(piece, i + 1)
        elif part == 0:
            for j in range(4):
                cols = slice(128 * (j % 2), 128 * (j % 2 + 1))
                gin_ref[t, pl.ds(4 * k + j, 8, stride=12), :] = tot[j // 2, :, cols]
                gin_ref[t, pl.ds(96 + 4 * k + j, 4, stride=12), :] = tot[2, 4 * (j // 2):4 * (j // 2 + 1), cols]
        else:
            for j in range(3):
                gout_ref[t, pl.ds(48 * k + j, 16, stride=3), :] = tot[:, 128 * j:128 * (j + 1)]

    compute_b(0, 1)
    start(X[0])
    compute_b(0, 0)
    start(Y[0])
    compute_b(1, 1)
    start(Z[1])
    compute_b(2, 0, 1)
    loads["sel"].wait()
    select_rows(0)
    compute_dzt()
    compute_a(1, 0)
    start(Y[2])
    start(X[2])
    select_rows(2)
    compute_a(1, 1)
    select_rows(1)
    start(Z[2])
    compute_a(0, 1)
    advance(0, X[0])
    compute_b(1, 0)
    advance(0, Y[0], Z[1])
    compute_a(0, 0)
    start(Z[0])
    start(Y[3])
    advance(0, Y[2])
    compute_a(2, 1)
    start(Z[3])
    compute_a(2, 0)
    start(X[3])
    advance(0, X[2])
    start(Y[1])
    advance(0, Y[3])
    advance(1, Y[2], X[0], X[2])
    advance(0, X[3], Z[0])
    start(X[1])
    advance(1, Y[0])
    advance(2, X[0])
    advance(1, Y[3], Z[1])
    advance(0, Y[1])
    advance(2, X[2], Y[0])
    advance(0, X[1])
    advance(1, X[3], Z[0])
    advance(0, Z[3])
    advance(1, Y[1])
    advance(2, Z[1], Z[0])
    advance(0, Z[2])
    advance(1, X[1])
    advance(3, X[0])
    advance(2, Y[1])
    advance(1, Z[3])
    advance(3, Z[0])
    advance(2, Y[2], X[1])
    advance(1, Z[2])
    advance(3, Y[0], X[1])
    advance(2, X[3])
    advance(3, Y[1], Z[1])
    advance(2, Z[3], Y[3], Z[2])

    stores = [pltpu.make_async_copy(src, dst, out_sem.at[i])
              for i, (src, dst) in enumerate(((gin_ref, gin_hbm), (gout_ref, gout_hbm)))]
    with scope("gram"):
        row = jnp.zeros((1, 128), F32)
        for q, (s, t) in enumerate(((0, 0), (0, 1), (1, 1))):
            prod = gin_ref[s] * gin_ref[t] + gout_ref[s] * gout_ref[t]
            one = jnp.sum(jnp.sum(prod, axis=0, keepdims=True), axis=1, keepdims=True)
            row = jnp.where(lane == q, one, row)
        gram_ref[me] = row
    with scope("gramx"):
        row_start(gram_ref, gram_ssem, gram_rsem)
        stores[0].start()
        stores[1].start()
        for i in range(4):
            sent = [b[2 * j + 1] for piece, b in bufs.items() for j in range(len(PATH[piece])) if sent_on(piece, j) == i]
            nbytes = sum(math.prod(ref.shape) * (2 if i == 0 else 4) for ref in sent)
            whole(pre_ref.at[pl.ds(0, nbytes // (4 * TOK))], ssem.at[i]).wait_send()
        row_all(cnt_ref, cnt_ssem, cnt_rsem).wait_send()
        stores[0].wait()
        stores[1].wait()
        row_all(gram_ref, gram_ssem, gram_rsem).wait_recv()
    with scope("drain"):
        gram_out[...] = jnp.sum(gram_ref[...], axis=0)
        row_all(gram_ref, gram_ssem, gram_rsem).wait_send()


def combine(gram_ref, gin_hbm, gout_hbm, weights_ref, sum_in, sum_out, gin_ref, gout_ref, sem):
    loads = [pltpu.make_async_copy(src, dst, sem.at[i])
             for i, (src, dst) in enumerate(((gin_hbm, gin_ref), (gout_hbm, gout_ref)))]
    for load in loads:
        load.start()
    lane = lax.broadcasted_iota(jnp.int32, (1, 128), 1)
    m00, m01, m11 = [jnp.broadcast_to(jnp.sum(jnp.where(lane == q, gram_ref[...], 0.0), axis=1, keepdims=True), (1, 128))
                     for q in range(3)]
    scale = (m00 + m11) / 2.0
    w0 = jnp.full((1, 128), 0.5, F32)
    w1 = w0
    for _ in range(SOLVER_STEPS):
        r0 = w0 * jnp.exp(-(m00 * w0 + m01 * w1) / scale)
        r1 = w1 * jnp.exp(-(m01 * w0 + m11 * w1) / scale)
        norm = r0 + r1
        w0 = r0 / norm
        w1 = r1 / norm
    weights_ref[0] = w0[0, 0]
    weights_ref[1] = w1[0, 0]
    for load in loads:
        load.wait()
    sum_in[...] = w0 * gin_ref[0] + w1 * gin_ref[1]
    sum_out[...] = w0 * gout_ref[0] + w1 * gout_ref[1]


def solution(mesh):
    sel = select_matrices()

    def local_step(x_loc, w_in, w_out, task_heads, lab_loc, mask_loc):
        vmem = pl.BlockSpec(memory_space=pltpu.VMEM)
        hbm = pl.BlockSpec(memory_space=pl.ANY)
        dma = pltpu.SemaphoreType.DMA
        heads_t = jnp.transpose(task_heads, (2, 0, 1))
        args = (x_loc, w_in, w_out, heads_t, lab_loc, mask_loc, jnp.asarray(sel, BF16))
        piece = jax.ShapeDtypeStruct((144, 128), F32)
        outs = [jax.ShapeDtypeStruct((TASKS, 144, 128), F32)] * 2 + [jax.ShapeDtypeStruct((1, 128), F32)]
        scratch = [pltpu.VMEM(a.shape, a.dtype) for a in args] + [pltpu.VMEM(a.shape, a.dtype) for a in outs[:2]] + [
            pltpu.VMEM((DIM, TOK), BF16),
            pltpu.VMEM((32, CHUNKS, 16, TOK), BF16),
            pltpu.VMEM((HID, TOK), F32),
            pltpu.VMEM((HID, TOK), F32),
            pltpu.VMEM((len(ORDERS), DIM, TOK), BF16),
            pltpu.VMEM((TASKS, DIM, TOK), BF16),
            pltpu.VMEM((TOK, TASKS * DIM), BF16),
            pltpu.VMEM((TASKS, 16, TOK), BF16),
            pltpu.VMEM((DEVICES, 1, 128), F32),
            pltpu.VMEM((DEVICES, 1, 128), F32)]
        scratch += [pltpu.VMEM(*shape) for piece, path in PATH.items() for shape in buffers(piece[0], path)]
        scratch += [dma((len(args),)), dma((3,)), dma((len(PATH), 4)), dma((4,)), dma, dma, dma, dma]
        gin, gout, gram = pl.pallas_call(
            kernel,
            out_shape=outs,
            in_specs=[hbm] * len(args),
            out_specs=[hbm, hbm, vmem],
            scratch_shapes=scratch,
            compiler_params=pltpu.CompilerParams(collective_id=0, has_side_effects=True,
                                                 vmem_limit_bytes=66_900_000),
            name="step",
        )(*args)
        weights, grad_in, grad_out = pl.pallas_call(
            combine,
            out_shape=[jax.ShapeDtypeStruct((TASKS,), F32), piece, piece],
            in_specs=[vmem, hbm, hbm],
            out_specs=[pl.BlockSpec(memory_space=pltpu.SMEM), vmem, vmem],
            scratch_shapes=[pltpu.VMEM(outs[0].shape, F32), pltpu.VMEM(outs[1].shape, F32), dma((2,))],
            compiler_params=pltpu.CompilerParams(vmem_limit_bytes=66_900_000),
            name="combine",
        )(gram, gin, gout)
        return weights, grad_in.reshape(-1), grad_out.reshape(-1)

    return jax.shard_map(local_step, mesh=mesh,
                         in_specs=(P("data", None), P(), P(), P(), P(None, "data"), P(None, "data")),
                         out_specs=(P(), P("data"), P("data")), check_vma=False)
```

```python
import contextlib
import itertools
import math

import jax
import jax.numpy as jnp
import numpy as np
from jax import lax
from jax.experimental import pallas as pl
from jax.experimental.pallas import tpu as pltpu
from jax.sharding import PartitionSpec as P

SOLVER_STEPS = 20
DEVICES = 32
DIM, HID, TOK, CLS = 384, 1536, 1024, 10
CHUNKS, TASKS = 3, 2
F32, BF16 = jnp.float32, jnp.bfloat16
GELU_C = 0.7978845608028654
GELU_A = 0.044715

ROUTES = {"x": ("x", "y", "zl", "zh"), "y": ("y", "x", "zl", "zh"), "z": ("zl", "xy", "zh"),
          "x3": ("x", "y", "z"), "y3": ("y", "x", "z"), "zh": ("zl", "zh", "xy")}
AXES = {"xy": ("y", "x"), "z": ("zl", "zh")}
X = ((1, 0, 1), (0, 0, 1), (0, 1, 0), (0, 2, 0))
Y = ((1, 0, 0), (1, 1, 0), (1, 2, 0), (1, 2, 1))
Z = ((0, 0, 0), (1, 1, 1), (0, 1, 1), (0, 2, 1))
CHOSEN = ("x3", "x3", "x", "x", "y3", "y3", "y", "y", "z", "zh", "z", "z")
PATH = {piece: ROUTES[name] for piece, name in zip(X + Y + Z, CHOSEN)}
NUMBER = {piece: i for i, piece in enumerate(PATH)}
COLS = (512, DIM)
PLANE = (96, 128)
TILE = ((3, 8, 256), (16, DIM))


def no_scope(name):
    return contextlib.nullcontext()


scope = no_scope


def owner(z, y, x, c):
    return 8 * z + 4 * y + 2 * x + c


def tiles(owners):
    return [12 * o + i for o in owners for i in range(8)] + [12 * o + i for o in owners for i in range(8, 12)]


def axes_of(stage):
    return AXES.get(stage, (stage,))


def owners(path):
    def points(axes):
        return [dict(zip(axes, bits)) for bits in itertools.product(range(2), repeat=len(axes))]

    def number(at):
        return owner(2 * at["zh"] + at["zl"], at["y"], at["x"], at["c"])

    rest = [axis for stage in path[2:] for axis in axes_of(stage)]
    return [[[number(p | q | r) for r in points(rest)] for q in points(axes_of(path[1]))] for p in points((path[0], "c"))]


def orders_of_rows():
    paths = list(dict.fromkeys(path for piece, path in PATH.items() if piece[0] == 0))
    orders = [tuple(r for first in owners(path) for second in first for r in tiles(second)) for path in paths]
    kinds = list(dict.fromkeys(orders))
    return kinds, {path: kinds.index(order) for path, order in zip(paths, orders)}


ORDERS, ORDER_OF = orders_of_rows()


def select_matrices():
    mat = np.zeros((len(ORDERS), DIM, DIM), np.float32)
    for m, order in zip(mat, ORDERS):
        m[np.arange(DIM), np.array(order)] = 1.0
    return mat


def buffers(part, path):
    rows, cols = PLANE[part], COLS[part]
    fans = [2 ** len(axes_of(stage)) for stage in path]
    shapes = [((4, rows, cols), BF16), ((3, rows, cols), BF16),
              ((fans[1], rows // fans[1], cols), F32), ((fans[1] - 1, rows // fans[1], cols), F32)]
    for i in range(2, len(path)):
        later = tuple(fans[i + 1:])
        shapes += [((fans[i],) + later + TILE[part], F32), ((fans[i] - 1,) + later + TILE[part], F32)]
    return shapes


def scoped(f):
    def call(*args):
        with scope("_".join([f.__name__, *map(str, args)])):
            return f(*args)
    return call


def dot(a, b, dims):
    return lax.dot_general(a, b, (dims, ((), ())), preferred_element_type=F32)


def kernel(x_hbm, w1_hbm, w2_hbm, heads_hbm, lab_hbm, mask_hbm, sel_hbm,
           gin_hbm, gout_hbm, gram_out,
           x_ref, w1_ref, w2_ref, heads_ref, lab_ref, mask_ref, sel_ref,
           gin_ref, gout_ref, xt_ref, act_ref, pre_ref, cdf_ref, xsel_ref, dz_ref, err_ref, cnt_ref, gram_ref, *rest):
    rest = list(rest)
    bufs = {piece: [rest.pop(0) for _ in range(2 * len(path))] for piece, path in PATH.items()}
    in_sem, out_sem, rsem, ssem, cnt_ssem, cnt_rsem, gram_ssem, gram_rsem = rest
    me = lax.axis_index("data")
    core = lax.rem(me, 2)
    px = lax.rem(me // 2, 2)
    py = lax.rem(me // 4, 2)
    pz = me // 8
    zl, zh = lax.rem(pz, 2), pz // 2

    here = {"x": px, "y": py, "c": core, "zl": zl, "zh": zh}

    def peer(at):
        at = here | at
        return (owner(2 * at["zh"] + at["zl"], at["y"], at["x"], at["c"]),)

    def flip(v, d):
        return lax.rem(v + d, 2)

    def remote(src, dst, ssem, rsem, dev):
        return pltpu.make_async_remote_copy(src_ref=src, dst_ref=dst, send_sem=ssem, recv_sem=rsem,
                                            device_id=dev, device_id_type=pl.DeviceIdType.MESH)

    loads = {name: pltpu.make_async_copy(src, dst, in_sem.at[i]) for i, (name, src, dst) in enumerate((
        ("x", x_hbm, x_ref), ("w1", w1_hbm, w1_ref), ("mask", mask_hbm, mask_ref), ("w2", w2_hbm, w2_ref),
        ("heads", heads_hbm, heads_ref), ("lab", lab_hbm, lab_ref), ("sel", sel_hbm, sel_ref)))}
    for load in loads.values():
        load.start()

    others = []
    for z in (3 - pz, lax.rem(pz + 2, 4), pz + 1 - 2 * zl, pz):
        for dy, dx, dc in itertools.product((1, 0), repeat=3):
            others.append((owner(z, flip(py, dy), flip(px, dx), flip(core, dc)),))
    others.pop()

    barrier = pltpu.get_barrier_semaphore()
    for dev in others:
        pl.semaphore_signal(barrier, inc=1, device_id=dev, device_id_type=pl.DeviceIdType.MESH)

    def row_start(buf, ssem, rsem):
        for dev in others:
            remote(buf.at[me], buf.at[me], ssem, rsem, dev).start()

    def row_all(buf, ssem, rsem):
        rows = buf.at[pl.ds(0, DEVICES - 1)]
        return remote(rows, rows, ssem, rsem, others[0])

    lane = lax.broadcasted_iota(jnp.int32, (1, 128), 1)

    def lane_pick(row, k):
        return jnp.sum(jnp.where(lane == k, row, 0.0), axis=1, keepdims=True)

    def forward(i):
        cols = slice(i * 384, (i + 1) * 384)
        pre = dot(w1_ref[:, cols], xt_ref[...], ((0,), (0,)))
        cdf = 0.5 + 0.5 * jnp.tanh(pre * (GELU_C + (GELU_C * GELU_A) * (pre * pre)))
        act_ref[8 * i:8 * (i + 1)] = (pre * cdf).astype(BF16).reshape(8, CHUNKS, 16, TOK)
        pre_ref[cols, :] = pre
        cdf_ref[cols, :] = cdf

    with scope("xt"):
        loads["x"].wait()
        xt_ref[...] = jnp.transpose(x_ref[...])
    with scope("fwd"):
        loads["w1"].wait()
        forward(0)
        forward(1)
        loads["mask"].wait()
        counts = jnp.sum(mask_ref[...].astype(F32), axis=1, keepdims=True)
        cnt_ref[me] = jnp.where(lane == 0, counts[0:1], jnp.where(lane == 1, counts[1:2], 0.0))
    with scope("barrier"):
        pl.semaphore_wait(barrier, DEVICES - 1)
        row_start(cnt_ref, cnt_ssem, cnt_rsem)
    with scope("fwd2"):
        forward(2)
        forward(3)
    with scope("zt"):
        loads["w2"].wait()
        zt = dot(w2_ref[...], act_ref[...].reshape(HID, TOK), ((0,), (0,)))
        zt = (xt_ref[...].astype(F32) + zt).astype(BF16)

    with scope("cls"):
        loads["heads"].wait()
        loads["lab"].wait()
        pad = jnp.zeros((16 - CLS, DIM), BF16)
        heads = jnp.concatenate([heads_ref[:, 0, :], pad, heads_ref[:, 1, :], pad], axis=0)
        logits = dot(heads, zt, ((1,), (0,)))
        cls = lax.broadcasted_iota(jnp.int32, (16, TOK), 0)
        for t in range(TASKS):
            score = jnp.where(cls < CLS, logits[16 * t:16 * (t + 1)], -jnp.inf)
            ex = jnp.exp(score - jnp.max(score, axis=0, keepdims=True))
            prob = ex / jnp.sum(ex, axis=0, keepdims=True)
            onehot = jnp.where(lab_ref[t:t + 1, :] == cls, 1.0, 0.0)
            err_ref[t] = (mask_ref[t:t + 1, :].astype(F32) * (prob - onehot)).astype(BF16)
            head = heads[16 * t:16 * (t + 1)]
            dz_ref[:, t * DIM:(t + 1) * DIM] = dot(err_ref[t], head, ((0,), (0,))).astype(BF16)

    inv = []

    def wait_counts():
        with scope("cntwait"):
            row_all(cnt_ref, cnt_ssem, cnt_rsem).wait_recv()
            total = jnp.sum(cnt_ref[...], axis=0)
            inv.extend(1.0 / jnp.maximum(lane_pick(total, t), 1.0) for t in range(TASKS))

    @scoped
    def compute_b(k, *tasks):
        part = dot(act_ref[:, k].reshape(512, TOK), dz_ref[:, tasks[0] * DIM:(tasks[-1] + 1) * DIM], ((1,), (0,)))
        if not inv:
            wait_counts()
        for i, t in enumerate(tasks):
            scaled = (part[:, i * DIM:(i + 1) * DIM] * inv[t]).astype(BF16)
            send = bufs[1, k, t][0]
            for slot, first in enumerate(owners(PATH[1, k, t])):
                for n, j in enumerate(o for second in first for o in second):
                    send[slot, 16 * n:16 * (n + 1)] = scaled[16 * j:16 * (j + 1)]

    @scoped
    def compute_a(k, t):
        rows = slice(512 * k, 512 * (k + 1))
        back = dot(w2_ref[rows, :], dz_ref[:, t * DIM:(t + 1) * DIM], ((1,), (1,)))
        pre, cdf = pre_ref[rows, :], cdf_ref[rows, :]
        slope = cdf + (pre * cdf) * (1.0 - cdf) * (2.0 * GELU_C + (6.0 * GELU_C * GELU_A) * (pre * pre))
        dpre = (back * slope).astype(BF16)
        part = dot(xsel_ref[ORDER_OF[PATH[0, k, t]]], dpre, ((1,), (1,)))
        bufs[0, k, t][0][...] = (part * inv[t]).astype(BF16).reshape(4, 96, 512)

    def select_rows(r):
        xsel_ref[r] = dot(sel_ref[r], xt_ref[...], ((1,), (0,))).astype(BF16)

    def axes(piece, i):
        return (PATH[piece][0], "c") if i == 0 else axes_of(PATH[piece][i])

    def sent_on(piece, i):
        return 3 if i + 1 == len(PATH[piece]) else i

    def index_of(at, names):
        return sum(at[name] * 2 ** (len(names) - 1 - i) for i, name in enumerate(names))

    def send_stage(piece, i):
        send, recv = bufs[piece][2 * i:2 * i + 2]
        names = axes(piece, i)
        moves = list(itertools.product(range(2), repeat=len(names)))[1:]
        for p, move in reversed(list(enumerate(moves))):
            at = {name: flip(here[name], d) for name, d in zip(names, move)}
            remote(send.at[index_of(at, names)], recv.at[p], ssem.at[sent_on(piece, i)], rsem.at[NUMBER[piece], i],
                   peer(at)).start()

    def whole(ref, sem):
        return remote(ref, ref, sem, sem, others[0])

    @scoped
    def start(piece):
        send_stage(piece, 0)

    @scoped
    def advance(i, *pieces):
        for piece in pieces:
            advance_one(piece, i)

    def advance_one(piece, i):
        part, k, t = piece
        send, recv = bufs[piece][2 * i:2 * i + 2]
        whole(recv, rsem.at[NUMBER[piece], i]).wait_recv()
        terms = [send[index_of(here, axes(piece, i))].astype(F32)]
        terms += [recv[p].astype(F32) for p in range(recv.shape[0])]
        while len(terms) > 1:
            terms = [a + b for a, b in zip(terms[::2], terms[1::2])]
        tot = terms[0]
        if i + 1 < len(PATH[piece]):
            out = bufs[piece][2 * i + 2]
            if i == 1 and part == 0:
                count = tot.shape[0] // 12
                for q in range(count):
                    at = (q,) if out.shape[0] == count else (q // 2, q % 2)
                    top = tot[8 * q:8 * (q + 1)]
                    low = tot[8 * count + 4 * q:8 * count + 4 * (q + 1)]
                    out[at + (0,)] = top[:, :256]
                    out[at + (1,)] = top[:, 256:]
                    out[at + (2,)] = jnp.concatenate([low[:, :256], low[:, 256:]], axis=0)
            else:
                out[...] = tot.reshape(out.shape)
            send_stage(piece, i + 1)
        elif part == 0:
            for j in range(4):
                cols = slice(128 * (j % 2), 128 * (j % 2 + 1))
                gin_ref[t, pl.ds(4 * k + j, 8, stride=12), :] = tot[j // 2, :, cols]
                gin_ref[t, pl.ds(96 + 4 * k + j, 4, stride=12), :] = tot[2, 4 * (j // 2):4 * (j // 2 + 1), cols]
        else:
            for j in range(3):
                gout_ref[t, pl.ds(48 * k + j, 16, stride=3), :] = tot[:, 128 * j:128 * (j + 1)]

    compute_b(1, 1)
    start(Z[1])
    compute_b(0, 1)
    start(X[0])
    compute_b(1, 0)
    start(Y[1])
    loads["sel"].wait()
    select_rows(1)
    compute_a(0, 0)
    select_rows(0)
    start(Z[0])
    compute_a(0, 1)
    start(X[1])
    compute_b(0, 0)
    start(Y[0])
    compute_b(2, 0, 1)
    compute_a(2, 1)
    start(Y[2])
    advance(0, Z[1], Y[1])
    compute_a(1, 0)
    start(X[2])
    start(Z[3])
    advance(0, X[0])
    compute_a(2, 0)
    advance(1, Y[1])
    compute_a(1, 1)
    advance(0, Y[0], Y[2])
    start(Z[2])
    start(Y[3])
    start(X[3])
    advance(1, Y[0], X[0])
    advance(0, X[1])
    advance(2, Y[1])
    advance(0, Y[3])
    advance(1, Y[2])
    advance(0, X[2], Z[3])
    advance(1, X[1], X[2])
    advance(0, X[3], Z[2], Z[0])
    advance(2, Y[2], Y[0])
    advance(1, Y[3])
    advance(2, X[2])
    advance(1, Z[3], X[3])
    advance(2, Y[3])
    advance(1, Z[1], Z[2])
    advance(2, X[3])
    advance(3, X[2])
    advance(2, Z[3])
    advance(1, Z[0])
    advance(3, Y[3])
    advance(2, X[1])
    advance(3, X[3])
    advance(2, X[0], Z[1])
    advance(3, Y[2])
    advance(2, Z[2], Z[0])

    stores = [pltpu.make_async_copy(src, dst, out_sem.at[i])
              for i, (src, dst) in enumerate(((gin_ref, gin_hbm), (gout_ref, gout_hbm)))]
    with scope("gram"):
        row = jnp.zeros((1, 128), F32)
        for q, (s, t) in enumerate(((0, 0), (0, 1), (1, 1))):
            prod = gin_ref[s] * gin_ref[t] + gout_ref[s] * gout_ref[t]
            one = jnp.sum(jnp.sum(prod, axis=0, keepdims=True), axis=1, keepdims=True)
            row = jnp.where(lane == q, one, row)
        gram_ref[me] = row
    with scope("gramx"):
        row_start(gram_ref, gram_ssem, gram_rsem)
        stores[0].start()
        stores[1].start()
        for i in range(4):
            sent = [b[2 * j + 1] for piece, b in bufs.items() for j in range(len(PATH[piece])) if sent_on(piece, j) == i]
            nbytes = sum(math.prod(ref.shape) * (2 if i == 0 else 4) for ref in sent)
            width = next(w for w in (1024, 512, 256) if nbytes // (4 * w) % 8 == 0)
            whole(pre_ref.at[pl.ds(0, nbytes // (4 * width)), pl.ds(0, width)], ssem.at[i]).wait_send()
        row_all(cnt_ref, cnt_ssem, cnt_rsem).wait_send()
        stores[0].wait()
        stores[1].wait()
        row_all(gram_ref, gram_ssem, gram_rsem).wait_recv()
    with scope("drain"):
        gram_out[...] = jnp.sum(gram_ref[...], axis=0)
        row_all(gram_ref, gram_ssem, gram_rsem).wait_send()


def combine(gram_ref, gin_hbm, gout_hbm, weights_ref, sum_in, sum_out, gin_ref, gout_ref, sem):
    loads = [pltpu.make_async_copy(src, dst, sem.at[i])
             for i, (src, dst) in enumerate(((gin_hbm, gin_ref), (gout_hbm, gout_ref)))]
    for load in loads:
        load.start()
    lane = lax.broadcasted_iota(jnp.int32, (1, 128), 1)
    m00, m01, m11 = [jnp.broadcast_to(jnp.sum(jnp.where(lane == q, gram_ref[...], 0.0), axis=1, keepdims=True), (1, 128))
                     for q in range(3)]
    scale = (m00 + m11) / 2.0
    w0 = jnp.full((1, 128), 0.5, F32)
    w1 = w0
    for _ in range(SOLVER_STEPS):
        r0 = w0 * jnp.exp(-(m00 * w0 + m01 * w1) / scale)
        r1 = w1 * jnp.exp(-(m01 * w0 + m11 * w1) / scale)
        norm = r0 + r1
        w0 = r0 / norm
        w1 = r1 / norm
    weights_ref[0] = w0[0, 0]
    weights_ref[1] = w1[0, 0]
    for load in loads:
        load.wait()
    sum_in[...] = w0 * gin_ref[0] + w1 * gin_ref[1]
    sum_out[...] = w0 * gout_ref[0] + w1 * gout_ref[1]


def solution(mesh):
    sel = select_matrices()

    def local_step(x_loc, w_in, w_out, task_heads, lab_loc, mask_loc):
        vmem = pl.BlockSpec(memory_space=pltpu.VMEM)
        hbm = pl.BlockSpec(memory_space=pl.ANY)
        dma = pltpu.SemaphoreType.DMA
        heads_t = jnp.transpose(task_heads, (2, 0, 1))
        args = (x_loc, w_in, w_out, heads_t, lab_loc, mask_loc, jnp.asarray(sel, BF16))
        piece = jax.ShapeDtypeStruct((144, 128), F32)
        outs = [jax.ShapeDtypeStruct((TASKS, 144, 128), F32)] * 2 + [jax.ShapeDtypeStruct((1, 128), F32)]
        scratch = [pltpu.VMEM(a.shape, a.dtype) for a in args] + [pltpu.VMEM(a.shape, a.dtype) for a in outs[:2]] + [
            pltpu.VMEM((DIM, TOK), BF16),
            pltpu.VMEM((32, CHUNKS, 16, TOK), BF16),
            pltpu.VMEM((HID, TOK), F32),
            pltpu.VMEM((HID, TOK), F32),
            pltpu.VMEM((len(ORDERS), DIM, TOK), BF16),
            pltpu.VMEM((TOK, TASKS * DIM), BF16),
            pltpu.VMEM((TASKS, 16, TOK), BF16),
            pltpu.VMEM((DEVICES, 1, 128), F32),
            pltpu.VMEM((DEVICES, 1, 128), F32)]
        scratch += [pltpu.VMEM(*shape) for piece, path in PATH.items() for shape in buffers(piece[0], path)]
        scratch += [dma((len(args),)), dma((3,)), dma((len(PATH), 4)), dma((4,)), dma, dma, dma, dma]
        gin, gout, gram = pl.pallas_call(
            kernel,
            out_shape=outs,
            in_specs=[hbm] * len(args),
            out_specs=[hbm, hbm, vmem],
            scratch_shapes=scratch,
            compiler_params=pltpu.CompilerParams(collective_id=0, has_side_effects=True,
                                                 vmem_limit_bytes=66_900_000),
            name="step",
        )(*args)
        weights, grad_in, grad_out = pl.pallas_call(
            combine,
            out_shape=[jax.ShapeDtypeStruct((TASKS,), F32), piece, piece],
            in_specs=[vmem, hbm, hbm],
            out_specs=[pl.BlockSpec(memory_space=pltpu.SMEM), vmem, vmem],
            scratch_shapes=[pltpu.VMEM(outs[0].shape, F32), pltpu.VMEM(outs[1].shape, F32), dma((2,))],
            compiler_params=pltpu.CompilerParams(vmem_limit_bytes=66_900_000),
            name="combine",
        )(gram, gin, gout)
        return weights, grad_in.reshape(-1), grad_out.reshape(-1)

    return jax.shard_map(local_step, mesh=mesh,
                         in_specs=(P("data", None), P(), P(), P(), P(None, "data"), P(None, "data")),
                         out_specs=(P(), P("data"), P("data")), check_vma=False)
```

```python
import contextlib
import itertools
import math

import jax
import jax.numpy as jnp
import numpy as np
from jax import lax
from jax.experimental import pallas as pl
from jax.experimental.pallas import tpu as pltpu
from jax.sharding import PartitionSpec as P

SOLVER_STEPS = 20
DEVICES = 32
DIM, HID, TOK, CLS = 384, 1536, 1024, 10
CHUNKS, TASKS = 3, 2
F32, BF16 = jnp.float32, jnp.bfloat16
GELU_C = 0.7978845608028654
GELU_A = 0.044715

ROUTES = {"x": ("x", "y", "zl", "zh"), "y": ("y", "x", "zl", "zh"), "z": ("zl", "xy", "zh"),
          "x3": ("x", "y", "z"), "y3": ("y", "x", "z"), "zh": ("zl", "zh", "xy"),
          "zyx": ("zl", "y", "x", "zh"), "zxy": ("zl", "x", "y", "zh")}
AXES = {"xy": ("y", "x"), "z": ("zl", "zh")}
X = ((1, 0, 1), (0, 0, 1), (0, 1, 0), (0, 2, 0))
Y = ((1, 0, 0), (1, 1, 0), (1, 2, 0), (1, 2, 1))
Z = ((0, 0, 0), (1, 1, 1), (0, 1, 1), (0, 2, 1))
CHOSEN = ("x3", "x3", "x", "x", "y3", "y3", "y", "y", "z", "zh", "z", "z")
PATH = {piece: ROUTES[name] for piece, name in zip(X + Y + Z, CHOSEN)}
NUMBER = {piece: i for i, piece in enumerate(PATH)}
COLS = (512, DIM)
PLANE = (96, 128)
TILE = ((3, 8, 256), (16, DIM))


def no_scope(name):
    return contextlib.nullcontext()


scope = no_scope


def owner(z, y, x, c):
    return 8 * z + 4 * y + 2 * x + c


def tiles(owners):
    return [12 * o + i for o in owners for i in range(8)] + [12 * o + i for o in owners for i in range(8, 12)]


def axes_of(stage):
    return AXES.get(stage, (stage,))


def owners(path):
    def points(axes):
        return [dict(zip(axes, bits)) for bits in itertools.product(range(2), repeat=len(axes))]

    def number(at):
        return owner(2 * at["zh"] + at["zl"], at["y"], at["x"], at["c"])

    rest = [axis for stage in path[2:] for axis in axes_of(stage)]
    return [[[number(p | q | r) for r in points(rest)] for q in points(axes_of(path[1]))] for p in points((path[0], "c"))]


def orders_of_rows():
    paths = list(dict.fromkeys(path for piece, path in PATH.items() if piece[0] == 0))
    orders = [tuple(r for first in owners(path) for second in first for r in tiles(second)) for path in paths]
    kinds = list(dict.fromkeys(orders))
    return kinds, {path: kinds.index(order) for path, order in zip(paths, orders)}


ORDERS, ORDER_OF = orders_of_rows()


def select_matrices():
    mat = np.zeros((len(ORDERS), DIM, DIM), np.float32)
    for m, order in zip(mat, ORDERS):
        m[np.arange(DIM), np.array(order)] = 1.0
    return mat


def buffers(part, path):
    rows, cols = PLANE[part], COLS[part]
    fans = [2 ** len(axes_of(stage)) for stage in path]
    shapes = [((4, rows, cols), BF16), ((3, rows, cols), BF16),
              ((fans[1], rows // fans[1], cols), F32), ((fans[1] - 1, rows // fans[1], cols), F32)]
    for i in range(2, len(path)):
        later = tuple(fans[i + 1:])
        shapes += [((fans[i],) + later + TILE[part], F32), ((fans[i] - 1,) + later + TILE[part], F32)]
    return shapes


def scoped(f):
    def call(*args):
        with scope("_".join([f.__name__, *map(str, args)])):
            return f(*args)
    return call


def dot(a, b, dims):
    return lax.dot_general(a, b, (dims, ((), ())), preferred_element_type=F32)


def kernel(x_hbm, w1_hbm, w2_hbm, heads_hbm, lab_hbm, mask_hbm, sel_hbm,
           gin_hbm, gout_hbm, gram_out,
           x_ref, w1_ref, w2_ref, heads_ref, lab_ref, mask_ref, sel_ref,
           gin_ref, gout_ref, xt_ref, act_ref, pre_ref, cdf_ref, xsel_ref, dz_ref, err_ref, cnt_ref, gram_ref, *rest):
    rest = list(rest)
    bufs = {piece: [rest.pop(0) for _ in range(2 * len(path))] for piece, path in PATH.items()}
    in_sem, out_sem, rsem, ssem, cnt_ssem, cnt_rsem, gram_ssem, gram_rsem = rest
    me = lax.axis_index("data")
    core = lax.rem(me, 2)
    px = lax.rem(me // 2, 2)
    py = lax.rem(me // 4, 2)
    pz = me // 8
    zl, zh = lax.rem(pz, 2), pz // 2

    here = {"x": px, "y": py, "c": core, "zl": zl, "zh": zh}

    def peer(at):
        at = here | at
        return (owner(2 * at["zh"] + at["zl"], at["y"], at["x"], at["c"]),)

    def flip(v, d):
        return lax.rem(v + d, 2)

    def remote(src, dst, ssem, rsem, dev):
        return pltpu.make_async_remote_copy(src_ref=src, dst_ref=dst, send_sem=ssem, recv_sem=rsem,
                                            device_id=dev, device_id_type=pl.DeviceIdType.MESH)

    loads = {name: pltpu.make_async_copy(src, dst, in_sem.at[i]) for i, (name, src, dst) in enumerate((
        ("x", x_hbm, x_ref), ("w1", w1_hbm, w1_ref), ("mask", mask_hbm, mask_ref), ("w2", w2_hbm, w2_ref),
        ("heads", heads_hbm, heads_ref), ("lab", lab_hbm, lab_ref), ("sel", sel_hbm, sel_ref)))}
    for load in loads.values():
        load.start()

    others = []
    for z in (3 - pz, lax.rem(pz + 2, 4), pz + 1 - 2 * zl, pz):
        for dy, dx, dc in itertools.product((1, 0), repeat=3):
            others.append((owner(z, flip(py, dy), flip(px, dx), flip(core, dc)),))
    others.pop()

    barrier = pltpu.get_barrier_semaphore()
    for dev in others:
        pl.semaphore_signal(barrier, inc=1, device_id=dev, device_id_type=pl.DeviceIdType.MESH)

    def row_start(buf, ssem, rsem):
        for dev in others:
            remote(buf.at[me], buf.at[me], ssem, rsem, dev).start()

    def row_all(buf, ssem, rsem):
        rows = buf.at[pl.ds(0, DEVICES - 1)]
        return remote(rows, rows, ssem, rsem, others[0])

    lane = lax.broadcasted_iota(jnp.int32, (1, 128), 1)

    def lane_pick(row, k):
        return jnp.sum(jnp.where(lane == k, row, 0.0), axis=1, keepdims=True)

    def forward(i):
        cols = slice(i * 384, (i + 1) * 384)
        pre = dot(w1_ref[:, cols], xt_ref[...], ((0,), (0,)))
        cdf = 0.5 + 0.5 * jnp.tanh(pre * (GELU_C + (GELU_C * GELU_A) * (pre * pre)))
        act_ref[8 * i:8 * (i + 1)] = (pre * cdf).astype(BF16).reshape(8, CHUNKS, 16, TOK)
        pre_ref[cols, :] = pre
        cdf_ref[cols, :] = cdf

    with scope("xt"):
        loads["x"].wait()
        xt_ref[...] = jnp.transpose(x_ref[...])
    with scope("fwd"):
        loads["w1"].wait()
        forward(0)
        forward(1)
        loads["mask"].wait()
        counts = jnp.sum(mask_ref[...].astype(F32), axis=1, keepdims=True)
        cnt_ref[me] = jnp.where(lane == 0, counts[0:1], jnp.where(lane == 1, counts[1:2], 0.0))
    with scope("barrier"):
        pl.semaphore_wait(barrier, DEVICES - 1)
        row_start(cnt_ref, cnt_ssem, cnt_rsem)
    with scope("fwd2"):
        forward(2)
        forward(3)
    with scope("zt"):
        loads["w2"].wait()
        zt = dot(w2_ref[...], act_ref[...].reshape(HID, TOK), ((0,), (0,)))
        zt = (xt_ref[...].astype(F32) + zt).astype(BF16)

    with scope("cls"):
        loads["heads"].wait()
        loads["lab"].wait()
        pad = jnp.zeros((16 - CLS, DIM), BF16)
        heads = jnp.concatenate([heads_ref[:, 0, :], pad, heads_ref[:, 1, :], pad], axis=0)
        logits = dot(heads, zt, ((1,), (0,)))
        cls = lax.broadcasted_iota(jnp.int32, (16, TOK), 0)
        for t in range(TASKS):
            score = jnp.where(cls < CLS, logits[16 * t:16 * (t + 1)], -jnp.inf)
            ex = jnp.exp(score - jnp.max(score, axis=0, keepdims=True))
            prob = ex / jnp.sum(ex, axis=0, keepdims=True)
            onehot = jnp.where(lab_ref[t:t + 1, :] == cls, 1.0, 0.0)
            err_ref[t] = (mask_ref[t:t + 1, :].astype(F32) * (prob - onehot)).astype(BF16)
            head = heads[16 * t:16 * (t + 1)]
            dz_ref[:, t * DIM:(t + 1) * DIM] = dot(err_ref[t], head, ((0,), (0,))).astype(BF16)

    inv = []

    def wait_counts():
        with scope("cntwait"):
            row_all(cnt_ref, cnt_ssem, cnt_rsem).wait_recv()
            total = jnp.sum(cnt_ref[...], axis=0)
            inv.extend(1.0 / jnp.maximum(lane_pick(total, t), 1.0) for t in range(TASKS))

    @scoped
    def compute_b(k, *tasks):
        part = dot(act_ref[:, k].reshape(512, TOK), dz_ref[:, tasks[0] * DIM:(tasks[-1] + 1) * DIM], ((1,), (0,)))
        if not inv:
            wait_counts()
        for i, t in enumerate(tasks):
            scaled = (part[:, i * DIM:(i + 1) * DIM] * inv[t]).astype(BF16)
            send = bufs[1, k, t][0]
            for slot, first in enumerate(owners(PATH[1, k, t])):
                for n, j in enumerate(o for second in first for o in second):
                    send[slot, 16 * n:16 * (n + 1)] = scaled[16 * j:16 * (j + 1)]

    @scoped
    def compute_a(k, t):
        rows = slice(512 * k, 512 * (k + 1))
        back = dot(w2_ref[rows, :], dz_ref[:, t * DIM:(t + 1) * DIM], ((1,), (1,)))
        pre, cdf = pre_ref[rows, :], cdf_ref[rows, :]
        slope = cdf + (pre * cdf) * (1.0 - cdf) * (2.0 * GELU_C + (6.0 * GELU_C * GELU_A) * (pre * pre))
        dpre = (back * slope).astype(BF16)
        part = dot(xsel_ref[ORDER_OF[PATH[0, k, t]]], dpre, ((1,), (1,)))
        bufs[0, k, t][0][...] = (part * inv[t]).astype(BF16).reshape(4, 96, 512)

    def select_rows(r):
        xsel_ref[r] = dot(sel_ref[r], xt_ref[...], ((1,), (0,))).astype(BF16)

    def axes(piece, i):
        return (PATH[piece][0], "c") if i == 0 else axes_of(PATH[piece][i])

    def sent_on(piece, i):
        return 3 if i + 1 == len(PATH[piece]) else i

    def index_of(at, names):
        return sum(at[name] * 2 ** (len(names) - 1 - i) for i, name in enumerate(names))

    def send_stage(piece, i):
        send, recv = bufs[piece][2 * i:2 * i + 2]
        names = axes(piece, i)
        moves = list(itertools.product(range(2), repeat=len(names)))[1:]
        for p, move in reversed(list(enumerate(moves))):
            at = {name: flip(here[name], d) for name, d in zip(names, move)}
            remote(send.at[index_of(at, names)], recv.at[p], ssem.at[sent_on(piece, i)], rsem.at[NUMBER[piece], i],
                   peer(at)).start()

    def whole(ref, sem):
        return remote(ref, ref, sem, sem, others[0])

    @scoped
    def start(piece):
        send_stage(piece, 0)

    @scoped
    def advance(i, *pieces):
        for piece in pieces:
            advance_one(piece, i)

    def advance_one(piece, i):
        part, k, t = piece
        send, recv = bufs[piece][2 * i:2 * i + 2]
        whole(recv, rsem.at[NUMBER[piece], i]).wait_recv()
        terms = [send[index_of(here, axes(piece, i))].astype(F32)]
        terms += [recv[p].astype(F32) for p in range(recv.shape[0])]
        while len(terms) > 1:
            terms = [a + b for a, b in zip(terms[::2], terms[1::2])]
        tot = terms[0]
        if i + 1 < len(PATH[piece]):
            out = bufs[piece][2 * i + 2]
            if i == 1 and part == 0:
                count = tot.shape[0] // 12
                for q in range(count):
                    at = (q,) if out.shape[0] == count else (q // 2, q % 2)
                    top = tot[8 * q:8 * (q + 1)]
                    low = tot[8 * count + 4 * q:8 * count + 4 * (q + 1)]
                    out[at + (0,)] = top[:, :256]
                    out[at + (1,)] = top[:, 256:]
                    out[at + (2,)] = jnp.concatenate([low[:, :256], low[:, 256:]], axis=0)
            else:
                out[...] = tot.reshape(out.shape)
            send_stage(piece, i + 1)
        elif part == 0:
            for j in range(4):
                cols = slice(128 * (j % 2), 128 * (j % 2 + 1))
                gin_ref[t, pl.ds(4 * k + j, 8, stride=12), :] = tot[j // 2, :, cols]
                gin_ref[t, pl.ds(96 + 4 * k + j, 4, stride=12), :] = tot[2, 4 * (j // 2):4 * (j // 2 + 1), cols]
        else:
            for j in range(3):
                gout_ref[t, pl.ds(48 * k + j, 16, stride=3), :] = tot[:, 128 * j:128 * (j + 1)]

    compute_b(0, 0)
    start(Y[0])
    compute_b(0, 1)
    start(X[0])
    compute_b(1, 1)
    start(Z[1])
    compute_b(2, 0, 1)
    loads["sel"].wait()
    select_rows(0)
    start(Y[2])
    compute_a(2, 0)
    start(X[3])
    select_rows(1)
    compute_a(1, 1)
    start(Z[2])
    compute_a(2, 1)
    compute_b(1, 0)
    advance(0, Y[0], X[0])
    compute_a(0, 1)
    advance(0, Z[1])
    start(Y[1])
    start(X[1])
    start(Z[3])
    compute_a(0, 0)
    advance(0, Y[2])
    start(Y[3])
    compute_a(1, 0)
    advance(1, Y[0])
    start(X[2])
    start(Z[0])
    advance(0, Y[1], X[1])
    advance(1, X[0])
    advance(0, X[3])
    advance(1, Y[2])
    advance(0, Y[3], Z[3])
    advance(1, X[1])
    advance(0, X[2], Z[0])
    advance(1, X[3])
    advance(0, Z[2])
    advance(1, Y[1])
    advance(2, Y[2])
    advance(1, Y[3])
    advance(2, X[0], X[3])
    advance(1, X[2], Z[3], Z[1], Z[0])
    advance(2, Y[3], X[2], Y[0])
    advance(1, Z[2])
    advance(2, Z[3], Y[1], Z[1])
    advance(3, X[2], X[3])
    advance(2, Z[0])
    advance(3, Y[3])
    advance(2, X[1])
    advance(3, Y[2])
    advance(2, Z[2])

    stores = [pltpu.make_async_copy(src, dst, out_sem.at[i])
              for i, (src, dst) in enumerate(((gin_ref, gin_hbm), (gout_ref, gout_hbm)))]
    with scope("gram"):
        row = jnp.zeros((1, 128), F32)
        for q, (s, t) in enumerate(((0, 0), (0, 1), (1, 1))):
            prod = gin_ref[s] * gin_ref[t] + gout_ref[s] * gout_ref[t]
            one = jnp.sum(jnp.sum(prod, axis=0, keepdims=True), axis=1, keepdims=True)
            row = jnp.where(lane == q, one, row)
        gram_ref[me] = row
    with scope("gramx"):
        row_start(gram_ref, gram_ssem, gram_rsem)
        stores[0].start()
        stores[1].start()
        for i in range(4):
            sent = [b[2 * j + 1] for piece, b in bufs.items() for j in range(len(PATH[piece])) if sent_on(piece, j) == i]
            nbytes = sum(math.prod(ref.shape) * (2 if i == 0 else 4) for ref in sent)
            width = next(w for w in (1024, 512, 256) if nbytes // (4 * w) % 8 == 0)
            whole(pre_ref.at[pl.ds(0, nbytes // (4 * width)), pl.ds(0, width)], ssem.at[i]).wait_send()
        row_all(cnt_ref, cnt_ssem, cnt_rsem).wait_send()
        stores[0].wait()
        stores[1].wait()
        row_all(gram_ref, gram_ssem, gram_rsem).wait_recv()
    with scope("drain"):
        gram_out[...] = jnp.sum(gram_ref[...], axis=0)
        row_all(gram_ref, gram_ssem, gram_rsem).wait_send()


def combine(gram_ref, gin_hbm, gout_hbm, weights_ref, sum_in, sum_out, gin_ref, gout_ref, sem):
    loads = [pltpu.make_async_copy(src, dst, sem.at[i])
             for i, (src, dst) in enumerate(((gin_hbm, gin_ref), (gout_hbm, gout_ref)))]
    for load in loads:
        load.start()
    lane = lax.broadcasted_iota(jnp.int32, (1, 128), 1)
    m00, m01, m11 = [jnp.broadcast_to(jnp.sum(jnp.where(lane == q, gram_ref[...], 0.0), axis=1, keepdims=True), (1, 128))
                     for q in range(3)]
    scale = (m00 + m11) / 2.0
    w0 = jnp.full((1, 128), 0.5, F32)
    w1 = w0
    for _ in range(SOLVER_STEPS):
        r0 = w0 * jnp.exp(-(m00 * w0 + m01 * w1) / scale)
        r1 = w1 * jnp.exp(-(m01 * w0 + m11 * w1) / scale)
        norm = r0 + r1
        w0 = r0 / norm
        w1 = r1 / norm
    weights_ref[0] = w0[0, 0]
    weights_ref[1] = w1[0, 0]
    for load in loads:
        load.wait()
    sum_in[...] = w0 * gin_ref[0] + w1 * gin_ref[1]
    sum_out[...] = w0 * gout_ref[0] + w1 * gout_ref[1]


def solution(mesh):
    sel = select_matrices()

    def local_step(x_loc, w_in, w_out, task_heads, lab_loc, mask_loc):
        vmem = pl.BlockSpec(memory_space=pltpu.VMEM)
        hbm = pl.BlockSpec(memory_space=pl.ANY)
        dma = pltpu.SemaphoreType.DMA
        heads_t = jnp.transpose(task_heads, (2, 0, 1))
        args = (x_loc, w_in, w_out, heads_t, lab_loc, mask_loc, jnp.asarray(sel, BF16))
        piece = jax.ShapeDtypeStruct((144, 128), F32)
        outs = [jax.ShapeDtypeStruct((TASKS, 144, 128), F32)] * 2 + [jax.ShapeDtypeStruct((1, 128), F32)]
        scratch = [pltpu.VMEM(a.shape, a.dtype) for a in args] + [pltpu.VMEM(a.shape, a.dtype) for a in outs[:2]] + [
            pltpu.VMEM((DIM, TOK), BF16),
            pltpu.VMEM((32, CHUNKS, 16, TOK), BF16),
            pltpu.VMEM((HID, TOK), F32),
            pltpu.VMEM((HID, TOK), F32),
            pltpu.VMEM((len(ORDERS), DIM, TOK), BF16),
            pltpu.VMEM((TOK, TASKS * DIM), BF16),
            pltpu.VMEM((TASKS, 16, TOK), BF16),
            pltpu.VMEM((DEVICES, 1, 128), F32),
            pltpu.VMEM((DEVICES, 1, 128), F32)]
        scratch += [pltpu.VMEM(*shape) for piece, path in PATH.items() for shape in buffers(piece[0], path)]
        scratch += [dma((len(args),)), dma((3,)), dma((len(PATH), 4)), dma((4,)), dma, dma, dma, dma]
        gin, gout, gram = pl.pallas_call(
            kernel,
            out_shape=outs,
            in_specs=[hbm] * len(args),
            out_specs=[hbm, hbm, vmem],
            scratch_shapes=scratch,
            compiler_params=pltpu.CompilerParams(collective_id=0, has_side_effects=True,
                                                 vmem_limit_bytes=66_900_000),
            name="step",
        )(*args)
        weights, grad_in, grad_out = pl.pallas_call(
            combine,
            out_shape=[jax.ShapeDtypeStruct((TASKS,), F32), piece, piece],
            in_specs=[vmem, hbm, hbm],
            out_specs=[pl.BlockSpec(memory_space=pltpu.SMEM), vmem, vmem],
            scratch_shapes=[pltpu.VMEM(outs[0].shape, F32), pltpu.VMEM(outs[1].shape, F32), dma((2,))],
            compiler_params=pltpu.CompilerParams(vmem_limit_bytes=66_900_000),
            name="combine",
        )(gram, gin, gout)
        return weights, grad_in.reshape(-1), grad_out.reshape(-1)

    return jax.shard_map(local_step, mesh=mesh,
                         in_specs=(P("data", None), P(), P(), P(), P(None, "data"), P(None, "data")),
                         out_specs=(P(), P("data"), P("data")), check_vma=False)
```

```python
import contextlib
import itertools
import math

import jax
import jax.numpy as jnp
import numpy as np
from jax import lax
from jax.experimental import pallas as pl
from jax.experimental.pallas import tpu as pltpu
from jax.sharding import PartitionSpec as P

SOLVER_STEPS = 20
DEVICES = 32
DIM, HID, TOK, CLS = 384, 1536, 1024, 10
CHUNKS, TASKS = 3, 2
F32, BF16 = jnp.float32, jnp.bfloat16
GELU_C = 0.7978845608028654
GELU_A = 0.044715

ROUTES = {"x": ("x", "y", "zl", "zh"), "y": ("y", "x", "zl", "zh"), "z": ("zl", "xy", "zh"),
          "x3": ("x", "y", "z"), "y3": ("y", "x", "z"), "zh": ("zl", "zh", "xy"),
          "zyx": ("zl", "y", "x", "zh"), "zxy": ("zl", "x", "y", "zh")}
AXES = {"xy": ("y", "x"), "z": ("zl", "zh")}
X = ((1, 0, 1), (0, 0, 1), (0, 1, 0), (0, 2, 0))
Y = ((1, 0, 0), (1, 1, 0), (1, 2, 0), (1, 2, 1))
Z = ((0, 0, 0), (1, 1, 1), (0, 1, 1), (0, 2, 1))
CHOSEN = ("x3", "x3", "x", "x", "y3", "y3", "y", "y", "z", "zh", "z", "z")
PATH = {piece: ROUTES[name] for piece, name in zip(X + Y + Z, CHOSEN)}
NUMBER = {piece: i for i, piece in enumerate(PATH)}
COLS = (512, DIM)
PLANE = (96, 128)
TILE = ((3, 8, 256), (16, DIM))


def no_scope(name):
    return contextlib.nullcontext()


scope = no_scope


def owner(z, y, x, c):
    return 8 * z + 4 * y + 2 * x + c


def tiles(owners):
    return [12 * o + i for o in owners for i in range(8)] + [12 * o + i for o in owners for i in range(8, 12)]


def axes_of(stage):
    return AXES.get(stage, (stage,))


def owners(path):
    def points(axes):
        return [dict(zip(axes, bits)) for bits in itertools.product(range(2), repeat=len(axes))]

    def number(at):
        return owner(2 * at["zh"] + at["zl"], at["y"], at["x"], at["c"])

    rest = [axis for stage in path[2:] for axis in axes_of(stage)]
    return [[[number(p | q | r) for r in points(rest)] for q in points(axes_of(path[1]))] for p in points((path[0], "c"))]


def orders_of_rows():
    paths = list(dict.fromkeys(path for piece, path in PATH.items() if piece[0] == 0))
    orders = [tuple(r for first in owners(path) for second in first for r in tiles(second)) for path in paths]
    kinds = list(dict.fromkeys(orders))
    return kinds, {path: kinds.index(order) for path, order in zip(paths, orders)}


ORDERS, ORDER_OF = orders_of_rows()


def select_matrices():
    mat = np.zeros((len(ORDERS), DIM, DIM), np.float32)
    for m, order in zip(mat, ORDERS):
        m[np.arange(DIM), np.array(order)] = 1.0
    return mat


def buffers(part, path):
    rows, cols = PLANE[part], COLS[part]
    fans = [2 ** len(axes_of(stage)) for stage in path]
    shapes = [((4, rows, cols), BF16), ((3, rows, cols), BF16),
              ((fans[1], rows // fans[1], cols), F32), ((fans[1] - 1, rows // fans[1], cols), F32)]
    for i in range(2, len(path)):
        later = tuple(fans[i + 1:])
        shapes += [((fans[i],) + later + TILE[part], F32), ((fans[i] - 1,) + later + TILE[part], F32)]
    return shapes


def scoped(f):
    def call(*args):
        with scope("_".join([f.__name__, *map(str, args)])):
            return f(*args)
    return call


def dot(a, b, dims):
    return lax.dot_general(a, b, (dims, ((), ())), preferred_element_type=F32)


def kernel(x_hbm, w1_hbm, w2_hbm, heads_hbm, lab_hbm, mask_hbm, sel_hbm,
           gin_hbm, gout_hbm, gram_hbm,
           x_ref, w1_ref, w2_ref, heads_ref, lab_ref, mask_ref, sel_ref,
           gin_ref, gout_ref, gram_out, xt_ref, act_ref, pre_ref, cdf_ref, xsel_ref, dz_ref, err_ref, cnt_ref, gram_ref, *rest):
    rest = list(rest)
    bufs = {piece: [rest.pop(0) for _ in range(2 * len(path))] for piece, path in PATH.items()}
    in_sem, out_sem, rsem, ssem, cnt_ssem, cnt_rsem, gram_ssem, gram_rsem = rest
    me = lax.axis_index("data")
    core = lax.rem(me, 2)
    px = lax.rem(me // 2, 2)
    py = lax.rem(me // 4, 2)
    pz = me // 8
    zl, zh = lax.rem(pz, 2), pz // 2

    here = {"x": px, "y": py, "c": core, "zl": zl, "zh": zh}

    def peer(at):
        at = here | at
        return (owner(2 * at["zh"] + at["zl"], at["y"], at["x"], at["c"]),)

    def flip(v, d):
        return lax.rem(v + d, 2)

    def remote(src, dst, ssem, rsem, dev):
        return pltpu.make_async_remote_copy(src_ref=src, dst_ref=dst, send_sem=ssem, recv_sem=rsem,
                                            device_id=dev, device_id_type=pl.DeviceIdType.MESH)

    loads = {name: pltpu.make_async_copy(src, dst, in_sem.at[i]) for i, (name, src, dst) in enumerate((
        ("x", x_hbm, x_ref), ("w1", w1_hbm, w1_ref), ("mask", mask_hbm, mask_ref), ("w2", w2_hbm, w2_ref),
        ("heads", heads_hbm, heads_ref), ("lab", lab_hbm, lab_ref), ("sel", sel_hbm, sel_ref)))}
    for load in loads.values():
        load.start()

    others = []
    for z in (3 - pz, lax.rem(pz + 2, 4), pz + 1 - 2 * zl, pz):
        for dy, dx, dc in itertools.product((1, 0), repeat=3):
            others.append((owner(z, flip(py, dy), flip(px, dx), flip(core, dc)),))
    others.pop()

    barrier = pltpu.get_barrier_semaphore()
    for dev in others:
        pl.semaphore_signal(barrier, inc=1, device_id=dev, device_id_type=pl.DeviceIdType.MESH)

    def row_start(buf, ssem, rsem):
        for dev in others:
            remote(buf.at[me], buf.at[me], ssem, rsem, dev).start()

    def row_all(buf, ssem, rsem):
        rows = buf.at[pl.ds(0, DEVICES - 1)]
        return remote(rows, rows, ssem, rsem, others[0])

    lane = lax.broadcasted_iota(jnp.int32, (1, 128), 1)

    def lane_pick(row, k):
        return jnp.sum(jnp.where(lane == k, row, 0.0), axis=1, keepdims=True)

    def forward(i):
        cols = slice(i * 384, (i + 1) * 384)
        pre = dot(w1_ref[:, cols], xt_ref[...], ((0,), (0,)))
        cdf = 0.5 + 0.5 * jnp.tanh(pre * (GELU_C + (GELU_C * GELU_A) * (pre * pre)))
        act_ref[8 * i:8 * (i + 1)] = (pre * cdf).astype(BF16).reshape(8, CHUNKS, 16, TOK)
        pre_ref[cols, :] = pre
        cdf_ref[cols, :] = cdf

    with scope("xt"):
        loads["x"].wait()
        xt_ref[...] = jnp.transpose(x_ref[...])
    with scope("fwd"):
        loads["w1"].wait()
        forward(0)
        forward(1)
        loads["mask"].wait()
        counts = jnp.sum(mask_ref[...].astype(F32), axis=1, keepdims=True)
        cnt_ref[me] = jnp.where(lane == 0, counts[0:1], jnp.where(lane == 1, counts[1:2], 0.0))
    with scope("barrier"):
        pl.semaphore_wait(barrier, DEVICES - 1)
        row_start(cnt_ref, cnt_ssem, cnt_rsem)
    with scope("fwd2"):
        forward(2)
        forward(3)
    with scope("zt"):
        loads["w2"].wait()
        zt = dot(w2_ref[...], act_ref[...].reshape(HID, TOK), ((0,), (0,)))
        zt = (xt_ref[...].astype(F32) + zt).astype(BF16)

    with scope("cls"):
        loads["heads"].wait()
        loads["lab"].wait()
        pad = jnp.zeros((16 - CLS, DIM), BF16)
        heads = jnp.concatenate([heads_ref[:, 0, :], pad, heads_ref[:, 1, :], pad], axis=0)
        logits = dot(heads, zt, ((1,), (0,)))
        cls = lax.broadcasted_iota(jnp.int32, (16, TOK), 0)
        for t in range(TASKS):
            score = jnp.where(cls < CLS, logits[16 * t:16 * (t + 1)], -jnp.inf)
            ex = jnp.exp(score - jnp.max(score, axis=0, keepdims=True))
            prob = ex / jnp.sum(ex, axis=0, keepdims=True)
            onehot = jnp.where(lab_ref[t:t + 1, :] == cls, 1.0, 0.0)
            err_ref[t] = (mask_ref[t:t + 1, :].astype(F32) * (prob - onehot)).astype(BF16)
            head = heads[16 * t:16 * (t + 1)]
            dz_ref[:, t * DIM:(t + 1) * DIM] = dot(err_ref[t], head, ((0,), (0,))).astype(BF16)

    inv = []

    def wait_counts():
        with scope("cntwait"):
            row_all(cnt_ref, cnt_ssem, cnt_rsem).wait_recv()
            total = jnp.sum(cnt_ref[...], axis=0)
            inv.extend(1.0 / jnp.maximum(lane_pick(total, t), 1.0) for t in range(TASKS))

    @scoped
    def compute_b(k, *tasks):
        part = dot(act_ref[:, k].reshape(512, TOK), dz_ref[:, tasks[0] * DIM:(tasks[-1] + 1) * DIM], ((1,), (0,)))
        if not inv:
            wait_counts()
        for i, t in enumerate(tasks):
            scaled = (part[:, i * DIM:(i + 1) * DIM] * inv[t]).astype(BF16)
            send = bufs[1, k, t][0]
            for slot, first in enumerate(owners(PATH[1, k, t])):
                for n, j in enumerate(o for second in first for o in second):
                    send[slot, 16 * n:16 * (n + 1)] = scaled[16 * j:16 * (j + 1)]

    @scoped
    def compute_a(k, t):
        rows = slice(512 * k, 512 * (k + 1))
        back = dot(w2_ref[rows, :], dz_ref[:, t * DIM:(t + 1) * DIM], ((1,), (1,)))
        pre, cdf = pre_ref[rows, :], cdf_ref[rows, :]
        slope = cdf + (pre * cdf) * (1.0 - cdf) * (2.0 * GELU_C + (6.0 * GELU_C * GELU_A) * (pre * pre))
        dpre = (back * slope).astype(BF16)
        part = dot(xsel_ref[ORDER_OF[PATH[0, k, t]]], dpre, ((1,), (1,)))
        bufs[0, k, t][0][...] = (part * inv[t]).astype(BF16).reshape(4, 96, 512)

    def select_rows(r):
        xsel_ref[r] = dot(sel_ref[r], xt_ref[...], ((1,), (0,))).astype(BF16)

    def axes(piece, i):
        return (PATH[piece][0], "c") if i == 0 else axes_of(PATH[piece][i])

    def sent_on(piece, i):
        return 3 if i + 1 == len(PATH[piece]) else i

    def index_of(at, names):
        return sum(at[name] * 2 ** (len(names) - 1 - i) for i, name in enumerate(names))

    def send_stage(piece, i):
        send, recv = bufs[piece][2 * i:2 * i + 2]
        names = axes(piece, i)
        moves = list(itertools.product(range(2), repeat=len(names)))[1:]
        for p, move in reversed(list(enumerate(moves))):
            at = {name: flip(here[name], d) for name, d in zip(names, move)}
            remote(send.at[index_of(at, names)], recv.at[p], ssem.at[sent_on(piece, i)], rsem.at[NUMBER[piece], i],
                   peer(at)).start()

    def whole(ref, sem):
        return remote(ref, ref, sem, sem, others[0])

    @scoped
    def start(piece):
        send_stage(piece, 0)

    @scoped
    def advance(i, *pieces):
        for piece in pieces:
            advance_one(piece, i)

    def advance_one(piece, i):
        part, k, t = piece
        send, recv = bufs[piece][2 * i:2 * i + 2]
        whole(recv, rsem.at[NUMBER[piece], i]).wait_recv()
        terms = [send[index_of(here, axes(piece, i))].astype(F32)]
        terms += [recv[p].astype(F32) for p in range(recv.shape[0])]
        while len(terms) > 1:
            terms = [a + b for a, b in zip(terms[::2], terms[1::2])]
        tot = terms[0]
        if i + 1 < len(PATH[piece]):
            out = bufs[piece][2 * i + 2]
            if i == 1 and part == 0:
                count = tot.shape[0] // 12
                for q in range(count):
                    at = (q,) if out.shape[0] == count else (q // 2, q % 2)
                    top = tot[8 * q:8 * (q + 1)]
                    low = tot[8 * count + 4 * q:8 * count + 4 * (q + 1)]
                    out[at + (0,)] = top[:, :256]
                    out[at + (1,)] = top[:, 256:]
                    out[at + (2,)] = jnp.concatenate([low[:, :256], low[:, 256:]], axis=0)
            else:
                out[...] = tot.reshape(out.shape)
            send_stage(piece, i + 1)
        elif part == 0:
            for j in range(4):
                cols = slice(128 * (j % 2), 128 * (j % 2 + 1))
                gin_ref[t, pl.ds(4 * k + j, 8, stride=12), :] = tot[j // 2, :, cols]
                gin_ref[t, pl.ds(96 + 4 * k + j, 4, stride=12), :] = tot[2, 4 * (j // 2):4 * (j // 2 + 1), cols]
        else:
            for j in range(3):
                gout_ref[t, pl.ds(48 * k + j, 16, stride=3), :] = tot[:, 128 * j:128 * (j + 1)]

    compute_b(0, 0)
    start(Y[0])
    compute_b(0, 1)
    start(X[0])
    compute_b(1, 1)
    start(Z[1])
    compute_b(2, 0, 1)
    loads["sel"].wait()
    select_rows(0)
    start(Y[2])
    compute_a(2, 0)
    start(X[3])
    select_rows(1)
    compute_a(1, 1)
    start(Z[2])
    compute_a(2, 1)
    compute_b(1, 0)
    advance(0, Y[0], X[0])
    compute_a(0, 1)
    advance(0, Z[1])
    start(Y[1])
    start(X[1])
    start(Z[3])
    compute_a(0, 0)
    advance(0, Y[2])
    start(Y[3])
    compute_a(1, 0)
    advance(1, Y[0])
    start(X[2])
    start(Z[0])
    advance(0, Y[1], X[1])
    advance(1, X[0])
    advance(0, X[3])
    advance(1, Y[2])
    advance(0, Y[3], Z[3])
    advance(1, X[1])
    advance(0, X[2], Z[0])
    advance(1, X[3])
    advance(0, Z[2])
    advance(1, Y[1])
    advance(2, Y[2])
    advance(1, Y[3])
    advance(2, X[0], X[3])
    advance(1, X[2], Z[3], Z[1], Z[0])
    advance(2, Y[3], X[2], Y[0])
    advance(1, Z[2])
    advance(2, Z[3], Y[1], Z[1])
    advance(3, X[2], X[3])
    advance(2, Z[0])
    advance(3, Y[3])
    advance(2, X[1])
    advance(3, Y[2])
    advance(2, Z[2])

    stores = [pltpu.make_async_copy(src, dst, out_sem.at[i])
              for i, (src, dst) in enumerate(((gin_ref, gin_hbm), (gout_ref, gout_hbm), (gram_out, gram_hbm)))]
    with scope("gram"):
        row = jnp.zeros((1, 128), F32)
        for q, (s, t) in enumerate(((0, 0), (0, 1), (1, 1))):
            prod = gin_ref[s] * gin_ref[t] + gout_ref[s] * gout_ref[t]
            one = jnp.sum(jnp.sum(prod, axis=0, keepdims=True), axis=1, keepdims=True)
            row = jnp.where(lane == q, one, row)
        gram_ref[me] = row
    with scope("gramx"):
        row_start(gram_ref, gram_ssem, gram_rsem)
        stores[0].start()
        stores[1].start()
        for i in range(4):
            sent = [b[2 * j + 1] for piece, b in bufs.items() for j in range(len(PATH[piece])) if sent_on(piece, j) == i]
            nbytes = sum(math.prod(ref.shape) * (2 if i == 0 else 4) for ref in sent)
            width = next(w for w in (1024, 512, 256) if nbytes // (4 * w) % 8 == 0)
            whole(pre_ref.at[pl.ds(0, nbytes // (4 * width)), pl.ds(0, width)], ssem.at[i]).wait_send()
        row_all(cnt_ref, cnt_ssem, cnt_rsem).wait_send()
        stores[0].wait()
        stores[1].wait()
        row_all(gram_ref, gram_ssem, gram_rsem).wait_recv()
    with scope("drain"):
        gram_out[...] = jnp.sum(gram_ref[...], axis=0)
        stores[2].start()
        row_all(gram_ref, gram_ssem, gram_rsem).wait_send()
        stores[2].wait()


def combine(gram_hbm, gin_hbm, gout_hbm, weights_ref, sum_in, sum_out, gram_ref, gin_ref, gout_ref, sem):
    loads = [pltpu.make_async_copy(src, dst, sem.at[i])
             for i, (src, dst) in enumerate(((gram_hbm, gram_ref), (gin_hbm, gin_ref), (gout_hbm, gout_ref)))]
    for load in loads:
        load.start()
    loads[0].wait()
    lane = lax.broadcasted_iota(jnp.int32, (1, 128), 1)
    m00, m01, m11 = [jnp.broadcast_to(jnp.sum(jnp.where(lane == q, gram_ref[...], 0.0), axis=1, keepdims=True), (1, 128))
                     for q in range(3)]
    scale = (m00 + m11) / 2.0
    w0 = jnp.full((1, 128), 0.5, F32)
    w1 = w0
    for _ in range(SOLVER_STEPS):
        r0 = w0 * jnp.exp(-(m00 * w0 + m01 * w1) / scale)
        r1 = w1 * jnp.exp(-(m01 * w0 + m11 * w1) / scale)
        norm = r0 + r1
        w0 = r0 / norm
        w1 = r1 / norm
    weights_ref[0] = w0[0, 0]
    weights_ref[1] = w1[0, 0]
    loads[1].wait()
    loads[2].wait()
    sum_in[...] = w0 * gin_ref[0] + w1 * gin_ref[1]
    sum_out[...] = w0 * gout_ref[0] + w1 * gout_ref[1]


def solution(mesh):
    sel = select_matrices()

    def local_step(x_loc, w_in, w_out, task_heads, lab_loc, mask_loc):
        vmem = pl.BlockSpec(memory_space=pltpu.VMEM)
        hbm = pl.BlockSpec(memory_space=pl.ANY)
        dma = pltpu.SemaphoreType.DMA
        heads_t = jnp.transpose(task_heads, (2, 0, 1))
        args = (x_loc, w_in, w_out, heads_t, lab_loc, mask_loc, jnp.asarray(sel, BF16))
        piece = jax.ShapeDtypeStruct((144, 128), F32)
        outs = [jax.ShapeDtypeStruct((TASKS, 144, 128), F32)] * 2 + [jax.ShapeDtypeStruct((1, 128), F32)]
        scratch = [pltpu.VMEM(a.shape, a.dtype) for a in args] + [pltpu.VMEM(a.shape, a.dtype) for a in outs] + [
            pltpu.VMEM((DIM, TOK), BF16),
            pltpu.VMEM((32, CHUNKS, 16, TOK), BF16),
            pltpu.VMEM((HID, TOK), F32),
            pltpu.VMEM((HID, TOK), F32),
            pltpu.VMEM((len(ORDERS), DIM, TOK), BF16),
            pltpu.VMEM((TOK, TASKS * DIM), BF16),
            pltpu.VMEM((TASKS, 16, TOK), BF16),
            pltpu.VMEM((DEVICES, 1, 128), F32),
            pltpu.VMEM((DEVICES, 1, 128), F32)]
        scratch += [pltpu.VMEM(*shape) for piece, path in PATH.items() for shape in buffers(piece[0], path)]
        scratch += [dma((len(args),)), dma((3,)), dma((len(PATH), 4)), dma((4,)), dma, dma, dma, dma]
        gin, gout, gram = pl.pallas_call(
            kernel,
            out_shape=outs,
            in_specs=[hbm] * len(args),
            out_specs=[hbm] * 3,
            scratch_shapes=scratch,
            compiler_params=pltpu.CompilerParams(collective_id=0, has_side_effects=True,
                                                 vmem_limit_bytes=66_900_000),
            name="step",
        )(*args)
        weights, grad_in, grad_out = pl.pallas_call(
            combine,
            out_shape=[jax.ShapeDtypeStruct((TASKS,), F32), piece, piece],
            in_specs=[hbm] * 3,
            out_specs=[pl.BlockSpec(memory_space=pltpu.SMEM), vmem, vmem],
            scratch_shapes=[pltpu.VMEM(outs[2].shape, F32), pltpu.VMEM(outs[0].shape, F32),
                            pltpu.VMEM(outs[1].shape, F32), dma((3,))],
            compiler_params=pltpu.CompilerParams(vmem_limit_bytes=66_900_000),
            name="combine",
        )(gram, gin, gout)
        return weights, grad_in.reshape(-1), grad_out.reshape(-1)

    return jax.shard_map(local_step, mesh=mesh,
                         in_specs=(P("data", None), P(), P(), P(), P(None, "data"), P(None, "data")),
                         out_specs=(P(), P("data"), P("data")), check_vma=False)
```

```python
import contextlib
import itertools
import math

import jax
import jax.numpy as jnp
import numpy as np
from jax import lax
from jax.experimental import pallas as pl
from jax.experimental.pallas import tpu as pltpu
from jax.sharding import PartitionSpec as P

SOLVER_STEPS = 20
DEVICES = 32
DIM, HID, TOK, CLS = 384, 1536, 1024, 10
CHUNKS, TASKS = 3, 2
F32, BF16 = jnp.float32, jnp.bfloat16
GELU_C = 0.7978845608028654
GELU_A = 0.044715

ROUTES = {"x": ("x", "y", "zl", "zh"), "y": ("y", "x", "zl", "zh"), "z": ("zl", "xy", "zh"),
          "x3": ("x", "y", "z"), "y3": ("y", "x", "z"), "zh": ("zl", "zh", "xy"),
          "zyx": ("zl", "y", "x", "zh"), "zxy": ("zl", "x", "y", "zh")}
AXES = {"xy": ("y", "x"), "z": ("zl", "zh")}
X = ((1, 0, 1), (0, 0, 1), (0, 1, 0), (0, 2, 0))
Y = ((1, 0, 0), (1, 1, 0), (1, 2, 0), (1, 2, 1))
Z = ((0, 0, 0), (1, 1, 1), (0, 1, 1), (0, 2, 1))
CHOSEN = ("x3", "x3", "x", "x", "y3", "y3", "y", "y", "z", "zh", "z", "z")
PATH = {piece: ROUTES[name] for piece, name in zip(X + Y + Z, CHOSEN)}
NUMBER = {piece: i for i, piece in enumerate(PATH)}
COLS = (512, DIM)
PLANE = (96, 128)
TILE = ((3, 8, 256), (16, DIM))


def no_scope(name):
    return contextlib.nullcontext()


scope = no_scope


def owner(z, y, x, c):
    return 8 * z + 4 * y + 2 * x + c


def tiles(owners):
    return [12 * o + i for o in owners for i in range(8)] + [12 * o + i for o in owners for i in range(8, 12)]


def axes_of(stage):
    return AXES.get(stage, (stage,))


def owners(path):
    def points(axes):
        return [dict(zip(axes, bits)) for bits in itertools.product(range(2), repeat=len(axes))]

    def number(at):
        return owner(2 * at["zh"] + at["zl"], at["y"], at["x"], at["c"])

    rest = [axis for stage in path[2:] for axis in axes_of(stage)]
    return [[[number(p | q | r) for r in points(rest)] for q in points(axes_of(path[1]))] for p in points((path[0], "c"))]


def orders_of_rows():
    paths = list(dict.fromkeys(path for piece, path in PATH.items() if piece[0] == 0))
    orders = [tuple(r for first in owners(path) for second in first for r in tiles(second)) for path in paths]
    kinds = list(dict.fromkeys(orders))
    return kinds, {path: kinds.index(order) for path, order in zip(paths, orders)}


ORDERS, ORDER_OF = orders_of_rows()


def select_matrices():
    mat = np.zeros((len(ORDERS), DIM, DIM), np.float32)
    for m, order in zip(mat, ORDERS):
        m[np.arange(DIM), np.array(order)] = 1.0
    return mat


def buffers(part, path):
    rows, cols = PLANE[part], COLS[part]
    fans = [2 ** len(axes_of(stage)) for stage in path]
    shapes = [((4, rows, cols), BF16), ((3, rows, cols), BF16),
              ((fans[1], rows // fans[1], cols), F32), ((fans[1] - 1, rows // fans[1], cols), F32)]
    for i in range(2, len(path)):
        later = tuple(fans[i + 1:])
        shapes += [((fans[i],) + later + TILE[part], F32), ((fans[i] - 1,) + later + TILE[part], F32)]
    return shapes


def scoped(f):
    def call(*args):
        with scope("_".join([f.__name__, *map(str, args)])):
            return f(*args)
    return call


def dot(a, b, dims):
    return lax.dot_general(a, b, (dims, ((), ())), preferred_element_type=F32)


def kernel(x_hbm, w1_hbm, w2_hbm, heads_hbm, lab_hbm, mask_hbm, sel_hbm,
           gin_hbm, gout_hbm, gram_out,
           x_ref, w1_ref, w2_ref, heads_ref, lab_ref, mask_ref, sel_ref,
           gin_ref, gout_ref, xt_ref, act_ref, pre_ref, cdf_ref, xsel_ref, dz_ref, err_ref, cnt_ref, gram_ref, *rest):
    rest = list(rest)
    bufs = {piece: [rest.pop(0) for _ in range(2 * len(path))] for piece, path in PATH.items()}
    in_sem, out_sem, rsem, ssem, cnt_ssem, cnt_rsem, gram_ssem, gram_rsem = rest
    me = lax.axis_index("data")
    core = lax.rem(me, 2)
    px = lax.rem(me // 2, 2)
    py = lax.rem(me // 4, 2)
    pz = me // 8
    zl, zh = lax.rem(pz, 2), pz // 2

    here = {"x": px, "y": py, "c": core, "zl": zl, "zh": zh}

    def peer(at):
        at = here | at
        return (owner(2 * at["zh"] + at["zl"], at["y"], at["x"], at["c"]),)

    def flip(v, d):
        return lax.rem(v + d, 2)

    def remote(src, dst, ssem, rsem, dev):
        return pltpu.make_async_remote_copy(src_ref=src, dst_ref=dst, send_sem=ssem, recv_sem=rsem,
                                            device_id=dev, device_id_type=pl.DeviceIdType.MESH)

    loads = {name: pltpu.make_async_copy(src, dst, in_sem.at[i]) for i, (name, src, dst) in enumerate((
        ("x", x_hbm, x_ref), ("w1", w1_hbm, w1_ref), ("mask", mask_hbm, mask_ref), ("w2", w2_hbm, w2_ref),
        ("heads", heads_hbm, heads_ref), ("lab", lab_hbm, lab_ref), ("sel", sel_hbm, sel_ref)))}
    for load in loads.values():
        load.start()

    others = []
    for z in (3 - pz, lax.rem(pz + 2, 4), pz + 1 - 2 * zl, pz):
        for dy, dx, dc in itertools.product((1, 0), repeat=3):
            others.append((owner(z, flip(py, dy), flip(px, dx), flip(core, dc)),))
    others.pop()

    barrier = pltpu.get_barrier_semaphore()
    for dev in others:
        pl.semaphore_signal(barrier, inc=1, device_id=dev, device_id_type=pl.DeviceIdType.MESH)

    def row_start(buf, ssem, rsem):
        for dev in others:
            remote(buf.at[me], buf.at[me], ssem, rsem, dev).start()

    def row_all(buf, ssem, rsem):
        rows = buf.at[pl.ds(0, DEVICES - 1)]
        return remote(rows, rows, ssem, rsem, others[0])

    lane = lax.broadcasted_iota(jnp.int32, (1, 128), 1)

    def lane_pick(row, k):
        return jnp.sum(jnp.where(lane == k, row, 0.0), axis=1, keepdims=True)

    def forward(i):
        cols = slice(i * 384, (i + 1) * 384)
        pre = dot(w1_ref[:, cols], xt_ref[...], ((0,), (0,)))
        cdf = 0.5 + 0.5 * jnp.tanh(pre * (GELU_C + (GELU_C * GELU_A) * (pre * pre)))
        act_ref[8 * i:8 * (i + 1)] = (pre * cdf).astype(BF16).reshape(8, CHUNKS, 16, TOK)
        pre_ref[cols, :] = pre
        cdf_ref[cols, :] = cdf

    with scope("xt"):
        loads["x"].wait()
        xt_ref[...] = jnp.transpose(x_ref[...])
    with scope("fwd"):
        loads["w1"].wait()
        forward(0)
        forward(1)
        loads["mask"].wait()
        counts = jnp.sum(mask_ref[...].astype(F32), axis=1, keepdims=True)
        cnt_ref[me] = jnp.where(lane == 0, counts[0:1], jnp.where(lane == 1, counts[1:2], 0.0))
    with scope("barrier"):
        pl.semaphore_wait(barrier, DEVICES - 1)
        row_start(cnt_ref, cnt_ssem, cnt_rsem)
    with scope("fwd2"):
        forward(2)
        forward(3)
    with scope("zt"):
        loads["w2"].wait()
        zt = dot(w2_ref[...], act_ref[...].reshape(HID, TOK), ((0,), (0,)))
        zt = (xt_ref[...].astype(F32) + zt).astype(BF16)

    with scope("cls"):
        loads["heads"].wait()
        loads["lab"].wait()
        pad = jnp.zeros((16 - CLS, DIM), BF16)
        heads = jnp.concatenate([heads_ref[:, 0, :], pad, heads_ref[:, 1, :], pad], axis=0)
        logits = dot(heads, zt, ((1,), (0,)))
        cls = lax.broadcasted_iota(jnp.int32, (16, TOK), 0)
        for t in range(TASKS):
            score = jnp.where(cls < CLS, logits[16 * t:16 * (t + 1)], -jnp.inf)
            ex = jnp.exp(score - jnp.max(score, axis=0, keepdims=True))
            prob = ex / jnp.sum(ex, axis=0, keepdims=True)
            onehot = jnp.where(lab_ref[t:t + 1, :] == cls, 1.0, 0.0)
            err_ref[t] = (mask_ref[t:t + 1, :].astype(F32) * (prob - onehot)).astype(BF16)
            head = heads[16 * t:16 * (t + 1)]
            dz_ref[:, t * DIM:(t + 1) * DIM] = dot(err_ref[t], head, ((0,), (0,))).astype(BF16)

    inv = []

    def wait_counts():
        with scope("cntwait"):
            row_all(cnt_ref, cnt_ssem, cnt_rsem).wait_recv()
            total = jnp.sum(cnt_ref[...], axis=0)
            inv.extend(1.0 / jnp.maximum(lane_pick(total, t), 1.0) for t in range(TASKS))

    @scoped
    def compute_b(k, *tasks):
        part = dot(act_ref[:, k].reshape(512, TOK), dz_ref[:, tasks[0] * DIM:(tasks[-1] + 1) * DIM], ((1,), (0,)))
        if not inv:
            wait_counts()
        for i, t in enumerate(tasks):
            scaled = (part[:, i * DIM:(i + 1) * DIM] * inv[t]).astype(BF16)
            send = bufs[1, k, t][0]
            for slot, first in enumerate(owners(PATH[1, k, t])):
                for n, j in enumerate(o for second in first for o in second):
                    send[slot, 16 * n:16 * (n + 1)] = scaled[16 * j:16 * (j + 1)]

    @scoped
    def compute_a(k, t):
        rows = slice(512 * k, 512 * (k + 1))
        back = dot(w2_ref[rows, :], dz_ref[:, t * DIM:(t + 1) * DIM], ((1,), (1,)))
        pre, cdf = pre_ref[rows, :], cdf_ref[rows, :]
        slope = cdf + (pre * cdf) * (1.0 - cdf) * (2.0 * GELU_C + (6.0 * GELU_C * GELU_A) * (pre * pre))
        dpre = (back * slope).astype(BF16)
        part = dot(xsel_ref[ORDER_OF[PATH[0, k, t]]], dpre, ((1,), (1,)))
        bufs[0, k, t][0][...] = (part * inv[t]).astype(BF16).reshape(4, 96, 512)

    def select_rows(r):
        xsel_ref[r] = dot(sel_ref[r], xt_ref[...], ((1,), (0,))).astype(BF16)

    def axes(piece, i):
        return (PATH[piece][0], "c") if i == 0 else axes_of(PATH[piece][i])

    def sent_on(piece, i):
        return 3 if i + 1 == len(PATH[piece]) else i

    def index_of(at, names):
        return sum(at[name] * 2 ** (len(names) - 1 - i) for i, name in enumerate(names))

    def send_stage(piece, i):
        send, recv = bufs[piece][2 * i:2 * i + 2]
        names = axes(piece, i)
        moves = list(itertools.product(range(2), repeat=len(names)))[1:]
        for p, move in reversed(list(enumerate(moves))):
            at = {name: flip(here[name], d) for name, d in zip(names, move)}
            remote(send.at[index_of(at, names)], recv.at[p], ssem.at[sent_on(piece, i)], rsem.at[NUMBER[piece], i],
                   peer(at)).start()

    def whole(ref, sem):
        return remote(ref, ref, sem, sem, others[0])

    @scoped
    def start(piece):
        send_stage(piece, 0)

    @scoped
    def advance(i, *pieces):
        for piece in pieces:
            advance_one(piece, i)

    def advance_one(piece, i):
        part, k, t = piece
        send, recv = bufs[piece][2 * i:2 * i + 2]
        whole(recv, rsem.at[NUMBER[piece], i]).wait_recv()
        terms = [send[index_of(here, axes(piece, i))].astype(F32)]
        terms += [recv[p].astype(F32) for p in range(recv.shape[0])]
        while len(terms) > 1:
            terms = [a + b for a, b in zip(terms[::2], terms[1::2])]
        tot = terms[0]
        if i + 1 < len(PATH[piece]):
            out = bufs[piece][2 * i + 2]
            if i == 1 and part == 0:
                count = tot.shape[0] // 12
                for q in range(count):
                    at = (q,) if out.shape[0] == count else (q // 2, q % 2)
                    top = tot[8 * q:8 * (q + 1)]
                    low = tot[8 * count + 4 * q:8 * count + 4 * (q + 1)]
                    out[at + (0,)] = top[:, :256]
                    out[at + (1,)] = top[:, 256:]
                    out[at + (2,)] = jnp.concatenate([low[:, :256], low[:, 256:]], axis=0)
            else:
                out[...] = tot.reshape(out.shape)
            send_stage(piece, i + 1)
        elif part == 0:
            for j in range(4):
                cols = slice(128 * (j % 2), 128 * (j % 2 + 1))
                gin_ref[t, pl.ds(4 * k + j, 8, stride=12), :] = tot[j // 2, :, cols]
                gin_ref[t, pl.ds(96 + 4 * k + j, 4, stride=12), :] = tot[2, 4 * (j // 2):4 * (j // 2 + 1), cols]
        else:
            for j in range(3):
                gout_ref[t, pl.ds(48 * k + j, 16, stride=3), :] = tot[:, 128 * j:128 * (j + 1)]

    compute_b(0, 0)
    start(Y[0])
    compute_b(0, 1)
    start(X[0])
    compute_b(1, 1)
    start(Z[1])
    compute_b(2, 0, 1)
    loads["sel"].wait()
    select_rows(0)
    start(Y[2])
    compute_a(2, 0)
    start(X[3])
    select_rows(1)
    compute_a(1, 1)
    start(Z[2])
    compute_a(2, 1)
    compute_b(1, 0)
    advance(0, Y[0], X[0])
    compute_a(0, 1)
    advance(0, Z[1])
    start(Y[1])
    start(X[1])
    start(Z[3])
    compute_a(0, 0)
    advance(0, Y[2])
    start(Y[3])
    compute_a(1, 0)
    advance(1, Y[0])
    start(X[2])
    start(Z[0])
    advance(0, Y[1], X[1])
    advance(1, X[0])
    advance(0, X[3])
    advance(1, Y[2])
    advance(0, Y[3], Z[3])
    advance(1, X[1])
    advance(0, X[2], Z[0])
    advance(1, X[3])
    advance(0, Z[2])
    advance(1, Y[1])
    advance(2, Y[2])
    advance(1, Y[3])
    advance(2, X[0], X[3])
    advance(1, X[2], Z[3], Z[1], Z[0])
    advance(2, Y[3], X[2], Y[0])
    advance(1, Z[2])
    advance(2, Z[3], Y[1], Z[1])
    advance(3, X[2], X[3])
    advance(2, Z[0])
    advance(3, Y[3])
    advance(2, X[1])
    advance(3, Y[2])
    advance(2, Z[2])

    stores = [pltpu.make_async_copy(src, dst, out_sem.at[i])
              for i, (src, dst) in enumerate(((gin_ref, gin_hbm), (gout_ref, gout_hbm)))]
    with scope("gram"):
        row = jnp.zeros((1, 128), F32)
        for q, (s, t) in enumerate(((0, 0), (0, 1), (1, 1))):
            prod = gin_ref[s] * gin_ref[t] + gout_ref[s] * gout_ref[t]
            one = jnp.sum(jnp.sum(prod, axis=0, keepdims=True), axis=1, keepdims=True)
            row = jnp.where(lane == q, one, row)
        gram_ref[me] = row
    with scope("gramx"):
        row_start(gram_ref, gram_ssem, gram_rsem)
        stores[0].start()
        stores[1].start()
        for i in range(4):
            sent = [b[2 * j + 1] for piece, b in bufs.items() for j in range(len(PATH[piece])) if sent_on(piece, j) == i]
            nbytes = sum(math.prod(ref.shape) * (2 if i == 0 else 4) for ref in sent)
            width = next(w for w in (1024, 512, 256) if nbytes // (4 * w) % 8 == 0)
            whole(pre_ref.at[pl.ds(0, nbytes // (4 * width)), pl.ds(0, width)], ssem.at[i]).wait_send()
        row_all(cnt_ref, cnt_ssem, cnt_rsem).wait_send()
        stores[0].wait()
        stores[1].wait()
        row_all(gram_ref, gram_ssem, gram_rsem).wait_recv()
    with scope("drain"):
        gram_out[...] = jnp.sum(gram_ref[...], axis=0)
        row_all(gram_ref, gram_ssem, gram_rsem).wait_send()


def combine(gram_ref, gin_hbm, gout_hbm, weights_ref, sum_in, sum_out, gin_ref, gout_ref, sem):
    loads = [pltpu.make_async_copy(src, dst, sem.at[i])
             for i, (src, dst) in enumerate(((gin_hbm, gin_ref), (gout_hbm, gout_ref)))]
    for load in loads:
        load.start()
    lane = lax.broadcasted_iota(jnp.int32, (1, 128), 1)
    m00, m01, m11 = [jnp.broadcast_to(jnp.sum(jnp.where(lane == q, gram_ref[...], 0.0), axis=1, keepdims=True), (1, 128))
                     for q in range(3)]
    scale = (m00 + m11) / 2.0
    w0 = jnp.full((1, 128), 0.5, F32)
    w1 = w0
    for _ in range(SOLVER_STEPS):
        r0 = w0 * jnp.exp(-(m00 * w0 + m01 * w1) / scale)
        r1 = w1 * jnp.exp(-(m01 * w0 + m11 * w1) / scale)
        norm = r0 + r1
        w0 = r0 / norm
        w1 = r1 / norm
    weights_ref[0] = w0[0, 0]
    weights_ref[1] = w1[0, 0]
    for load in loads:
        load.wait()
    sum_in[...] = w0 * gin_ref[0] + w1 * gin_ref[1]
    sum_out[...] = w0 * gout_ref[0] + w1 * gout_ref[1]


def solution(mesh):
    sel = select_matrices()

    def local_step(x_loc, w_in, w_out, task_heads, lab_loc, mask_loc):
        vmem = pl.BlockSpec(memory_space=pltpu.VMEM)
        hbm = pl.BlockSpec(memory_space=pl.ANY)
        dma = pltpu.SemaphoreType.DMA
        heads_t = jnp.transpose(task_heads, (2, 0, 1))
        args = (x_loc, w_in, w_out, heads_t, lab_loc, mask_loc, jnp.asarray(sel, BF16))
        piece = jax.ShapeDtypeStruct((144, 128), F32)
        outs = [jax.ShapeDtypeStruct((TASKS, 144, 128), F32)] * 2 + [jax.ShapeDtypeStruct((1, 128), F32)]
        scratch = [pltpu.VMEM(a.shape, a.dtype) for a in args] + [pltpu.VMEM(a.shape, a.dtype) for a in outs[:2]] + [
            pltpu.VMEM((DIM, TOK), BF16),
            pltpu.VMEM((32, CHUNKS, 16, TOK), BF16),
            pltpu.VMEM((HID, TOK), F32),
            pltpu.VMEM((HID, TOK), F32),
            pltpu.VMEM((len(ORDERS), DIM, TOK), BF16),
            pltpu.VMEM((TOK, TASKS * DIM), BF16),
            pltpu.VMEM((TASKS, 16, TOK), BF16),
            pltpu.VMEM((DEVICES, 1, 128), F32),
            pltpu.VMEM((DEVICES, 1, 128), F32)]
        scratch += [pltpu.VMEM(*shape) for piece, path in PATH.items() for shape in buffers(piece[0], path)]
        scratch += [dma((len(args),)), dma((3,)), dma((len(PATH), 4)), dma((4,)), dma, dma, dma, dma]
        gin, gout, gram = pl.pallas_call(
            kernel,
            out_shape=outs,
            in_specs=[hbm] * len(args),
            out_specs=[hbm, hbm, vmem],
            scratch_shapes=scratch,
            compiler_params=pltpu.CompilerParams(collective_id=0, has_side_effects=True,
                                                 vmem_limit_bytes=56547000),
            name="step",
        )(*args)
        weights, grad_in, grad_out = pl.pallas_call(
            combine,
            out_shape=[jax.ShapeDtypeStruct((TASKS,), F32), piece, piece],
            in_specs=[vmem, hbm, hbm],
            out_specs=[pl.BlockSpec(memory_space=pltpu.SMEM), vmem, vmem],
            scratch_shapes=[pltpu.VMEM(outs[0].shape, F32), pltpu.VMEM(outs[1].shape, F32), dma((2,))],
            compiler_params=pltpu.CompilerParams(vmem_limit_bytes=56547000),
            name="combine",
        )(gram, gin, gout)
        return weights, grad_in.reshape(-1), grad_out.reshape(-1)

    return jax.shard_map(local_step, mesh=mesh,
                         in_specs=(P("data", None), P(), P(), P(), P(None, "data"), P(None, "data")),
                         out_specs=(P(), P("data"), P("data")), check_vma=False)
```

```python
import contextlib
import itertools
import math

import jax
import jax.numpy as jnp
import numpy as np
from jax import lax
from jax.experimental import pallas as pl
from jax.experimental.pallas import tpu as pltpu
from jax.sharding import PartitionSpec as P

SOLVER_STEPS = 20
DEVICES = 32
DIM, HID, TOK, CLS = 384, 1536, 1024, 10
CHUNKS, TASKS = 3, 2
F32, BF16 = jnp.float32, jnp.bfloat16
GELU_C = 0.7978845608028654
GELU_A = 0.044715

ROUTES = {"x": ("x", "y", "zl", "zh"), "y": ("y", "x", "zl", "zh"), "z": ("zl", "xy", "zh"),
          "x3": ("x", "y", "z"), "y3": ("y", "x", "z"), "zh": ("zl", "zh", "xy"),
          "zyx": ("zl", "y", "x", "zh"), "zxy": ("zl", "x", "y", "zh")}
AXES = {"xy": ("y", "x"), "z": ("zl", "zh")}
X = ((1, 0, 1), (0, 0, 1), (0, 1, 0), (0, 2, 0))
Y = ((1, 0, 0), (1, 1, 0), (1, 2, 0), (1, 2, 1))
Z = ((0, 0, 0), (1, 1, 1), (0, 1, 1), (0, 2, 1))
CHOSEN = ("x3", "x3", "x", "x", "y3", "y3", "y", "y", "z", "zh", "z", "z")
PATH = {piece: ROUTES[name] for piece, name in zip(X + Y + Z, CHOSEN)}
NUMBER = {piece: i for i, piece in enumerate(PATH)}
COLS = (512, DIM)
PLANE = (96, 128)
TILE = ((3, 8, 256), (16, DIM))


def no_scope(name):
    return contextlib.nullcontext()


scope = no_scope


def owner(z, y, x, c):
    return 8 * z + 4 * y + 2 * x + c


def tiles(owners):
    return [12 * o + i for o in owners for i in range(8)] + [12 * o + i for o in owners for i in range(8, 12)]


def axes_of(stage):
    return AXES.get(stage, (stage,))


def owners(path):
    def points(axes):
        return [dict(zip(axes, bits)) for bits in itertools.product(range(2), repeat=len(axes))]

    def number(at):
        return owner(2 * at["zh"] + at["zl"], at["y"], at["x"], at["c"])

    rest = [axis for stage in path[2:] for axis in axes_of(stage)]
    return [[[number(p | q | r) for r in points(rest)] for q in points(axes_of(path[1]))] for p in points((path[0], "c"))]


def orders_of_rows():
    paths = list(dict.fromkeys(path for piece, path in PATH.items() if piece[0] == 0))
    orders = [tuple(r for first in owners(path) for second in first for r in tiles(second)) for path in paths]
    kinds = list(dict.fromkeys(orders))
    return kinds, {path: kinds.index(order) for path, order in zip(paths, orders)}


ORDERS, ORDER_OF = orders_of_rows()


def select_matrices():
    mat = np.zeros((len(ORDERS), DIM, DIM), np.float32)
    for m, order in zip(mat, ORDERS):
        m[np.arange(DIM), np.array(order)] = 1.0
    return mat


def buffers(part, path):
    rows, cols = PLANE[part], COLS[part]
    fans = [2 ** len(axes_of(stage)) for stage in path]
    shapes = [((4, rows, cols), BF16), ((3, rows, cols), BF16),
              ((fans[1], rows // fans[1], cols), F32), ((fans[1] - 1, rows // fans[1], cols), F32)]
    for i in range(2, len(path)):
        later = tuple(fans[i + 1:])
        shapes += [((fans[i],) + later + TILE[part], F32), ((fans[i] - 1,) + later + TILE[part], F32)]
    return shapes


def scoped(f):
    def call(*args):
        with scope("_".join([f.__name__, *map(str, args)])):
            return f(*args)
    return call


def dot(a, b, dims):
    return lax.dot_general(a, b, (dims, ((), ())), preferred_element_type=F32)


def kernel(x_hbm, w1_hbm, w2_hbm, heads_hbm, lab_hbm, mask_hbm, sel_hbm,
           gin_hbm, gout_hbm, gram_out,
           x_ref, w1_ref, w2_ref, heads_ref, lab_ref, mask_ref, sel_ref,
           gin_ref, gout_ref, xt_ref, act_ref, pre_ref, cdf_ref, xsel_ref, dz_ref, err_ref, cnt_ref, gram_ref, *rest):
    rest = list(rest)
    bufs = {piece: [rest.pop(0) for _ in range(2 * len(path))] for piece, path in PATH.items()}
    in_sem, out_sem, rsem, ssem, cnt_ssem, cnt_rsem, gram_ssem, gram_rsem = rest
    me = lax.axis_index("data")
    core = lax.rem(me, 2)
    px = lax.rem(me // 2, 2)
    py = lax.rem(me // 4, 2)
    pz = me // 8
    zl, zh = lax.rem(pz, 2), pz // 2

    here = {"x": px, "y": py, "c": core, "zl": zl, "zh": zh}

    def peer(at):
        at = here | at
        return (owner(2 * at["zh"] + at["zl"], at["y"], at["x"], at["c"]),)

    def flip(v, d):
        return lax.rem(v + d, 2)

    def remote(src, dst, ssem, rsem, dev):
        return pltpu.make_async_remote_copy(src_ref=src, dst_ref=dst, send_sem=ssem, recv_sem=rsem,
                                            device_id=dev, device_id_type=pl.DeviceIdType.MESH)

    loads = {name: pltpu.make_async_copy(src, dst, in_sem.at[i]) for i, (name, src, dst) in enumerate((
        ("x", x_hbm, x_ref), ("w1", w1_hbm, w1_ref), ("mask", mask_hbm, mask_ref), ("w2", w2_hbm, w2_ref),
        ("heads", heads_hbm, heads_ref), ("lab", lab_hbm, lab_ref), ("sel", sel_hbm, sel_ref)))}
    for load in loads.values():
        load.start()

    others = []
    for z in (3 - pz, lax.rem(pz + 2, 4), pz + 1 - 2 * zl, pz):
        for dy, dx, dc in itertools.product((1, 0), repeat=3):
            others.append((owner(z, flip(py, dy), flip(px, dx), flip(core, dc)),))
    others.pop()

    barrier = pltpu.get_barrier_semaphore()
    for dev in others:
        pl.semaphore_signal(barrier, inc=1, device_id=dev, device_id_type=pl.DeviceIdType.MESH)

    def row_start(buf, ssem, rsem):
        for dev in others:
            remote(buf.at[me], buf.at[me], ssem, rsem, dev).start()

    def row_all(buf, ssem, rsem):
        rows = buf.at[pl.ds(0, DEVICES - 1)]
        return remote(rows, rows, ssem, rsem, others[0])

    lane = lax.broadcasted_iota(jnp.int32, (1, 128), 1)

    def lane_pick(row, k):
        return jnp.sum(jnp.where(lane == k, row, 0.0), axis=1, keepdims=True)

    def forward(i):
        cols = slice(i * 384, (i + 1) * 384)
        pre = dot(w1_ref[:, cols], xt_ref[...], ((0,), (0,)))
        cdf = 0.5 + 0.5 * jnp.tanh(pre * (GELU_C + (GELU_C * GELU_A) * (pre * pre)))
        act_ref[8 * i:8 * (i + 1)] = (pre * cdf).astype(BF16).reshape(8, CHUNKS, 16, TOK)
        pre_ref[cols, :] = pre
        cdf_ref[cols, :] = cdf

    with scope("xt"):
        loads["x"].wait()
        xt_ref[...] = jnp.transpose(x_ref[...])
    with scope("fwd"):
        loads["w1"].wait()
        forward(0)
        forward(1)
        loads["mask"].wait()
        counts = jnp.sum(mask_ref[...].astype(F32), axis=1, keepdims=True)
        cnt_ref[me] = jnp.where(lane == 0, counts[0:1], jnp.where(lane == 1, counts[1:2], 0.0))
    with scope("barrier"):
        pl.semaphore_wait(barrier, DEVICES - 1)
        row_start(cnt_ref, cnt_ssem, cnt_rsem)
    with scope("fwd2"):
        forward(2)
        forward(3)
    with scope("zt"):
        loads["w2"].wait()
        zt = dot(w2_ref[...], act_ref[...].reshape(HID, TOK), ((0,), (0,)))
        zt = (xt_ref[...].astype(F32) + zt).astype(BF16)

    with scope("cls"):
        loads["heads"].wait()
        loads["lab"].wait()
        pad = jnp.zeros((16 - CLS, DIM), BF16)
        heads = jnp.concatenate([heads_ref[:, 0, :], pad, heads_ref[:, 1, :], pad], axis=0)
        logits = dot(heads, zt, ((1,), (0,)))
        cls = lax.broadcasted_iota(jnp.int32, (16, TOK), 0)

    def classes(t):
        score = jnp.where(cls < CLS, logits[16 * t:16 * (t + 1)], -jnp.inf)
        ex = jnp.exp(score - jnp.max(score, axis=0, keepdims=True))
        prob = ex / jnp.sum(ex, axis=0, keepdims=True)
        onehot = jnp.where(lab_ref[t:t + 1, :] == cls, 1.0, 0.0)
        err_ref[t] = (mask_ref[t:t + 1, :].astype(F32) * (prob - onehot)).astype(BF16)
        head = heads[16 * t:16 * (t + 1)]
        dz_ref[:, t * DIM:(t + 1) * DIM] = dot(err_ref[t], head, ((0,), (0,))).astype(BF16)

    classes(0)

    inv = []

    def wait_counts():
        with scope("cntwait"):
            row_all(cnt_ref, cnt_ssem, cnt_rsem).wait_recv()
            total = jnp.sum(cnt_ref[...], axis=0)
            inv.extend(1.0 / jnp.maximum(lane_pick(total, t), 1.0) for t in range(TASKS))

    @scoped
    def compute_b(k, *tasks):
        part = dot(act_ref[:, k].reshape(512, TOK), dz_ref[:, tasks[0] * DIM:(tasks[-1] + 1) * DIM], ((1,), (0,)))
        if not inv:
            wait_counts()
        for i, t in enumerate(tasks):
            scaled = (part[:, i * DIM:(i + 1) * DIM] * inv[t]).astype(BF16)
            send = bufs[1, k, t][0]
            for slot, first in enumerate(owners(PATH[1, k, t])):
                for n, j in enumerate(o for second in first for o in second):
                    send[slot, 16 * n:16 * (n + 1)] = scaled[16 * j:16 * (j + 1)]

    @scoped
    def compute_a(k, t):
        rows = slice(512 * k, 512 * (k + 1))
        back = dot(w2_ref[rows, :], dz_ref[:, t * DIM:(t + 1) * DIM], ((1,), (1,)))
        pre, cdf = pre_ref[rows, :], cdf_ref[rows, :]
        slope = cdf + (pre * cdf) * (1.0 - cdf) * (2.0 * GELU_C + (6.0 * GELU_C * GELU_A) * (pre * pre))
        dpre = (back * slope).astype(BF16)
        part = dot(xsel_ref[ORDER_OF[PATH[0, k, t]]], dpre, ((1,), (1,)))
        bufs[0, k, t][0][...] = (part * inv[t]).astype(BF16).reshape(4, 96, 512)

    def select_rows(r):
        xsel_ref[r] = dot(sel_ref[r], xt_ref[...], ((1,), (0,))).astype(BF16)

    def axes(piece, i):
        return (PATH[piece][0], "c") if i == 0 else axes_of(PATH[piece][i])

    def sent_on(piece, i):
        return 3 if i + 1 == len(PATH[piece]) else i

    def index_of(at, names):
        return sum(at[name] * 2 ** (len(names) - 1 - i) for i, name in enumerate(names))

    def send_stage(piece, i):
        send, recv = bufs[piece][2 * i:2 * i + 2]
        names = axes(piece, i)
        moves = list(itertools.product(range(2), repeat=len(names)))[1:]
        for p, move in reversed(list(enumerate(moves))):
            at = {name: flip(here[name], d) for name, d in zip(names, move)}
            remote(send.at[index_of(at, names)], recv.at[p], ssem.at[sent_on(piece, i)], rsem.at[NUMBER[piece], i],
                   peer(at)).start()

    def whole(ref, sem):
        return remote(ref, ref, sem, sem, others[0])

    @scoped
    def start(piece):
        send_stage(piece, 0)

    @scoped
    def advance(i, *pieces):
        for piece in pieces:
            advance_one(piece, i)

    def advance_one(piece, i):
        part, k, t = piece
        send, recv = bufs[piece][2 * i:2 * i + 2]
        whole(recv, rsem.at[NUMBER[piece], i]).wait_recv()
        terms = [send[index_of(here, axes(piece, i))].astype(F32)]
        terms += [recv[p].astype(F32) for p in range(recv.shape[0])]
        while len(terms) > 1:
            terms = [a + b for a, b in zip(terms[::2], terms[1::2])]
        tot = terms[0]
        if i + 1 < len(PATH[piece]):
            out = bufs[piece][2 * i + 2]
            if i == 1 and part == 0:
                count = tot.shape[0] // 12
                for q in range(count):
                    at = (q,) if out.shape[0] == count else (q // 2, q % 2)
                    top = tot[8 * q:8 * (q + 1)]
                    low = tot[8 * count + 4 * q:8 * count + 4 * (q + 1)]
                    out[at + (0,)] = top[:, :256]
                    out[at + (1,)] = top[:, 256:]
                    out[at + (2,)] = jnp.concatenate([low[:, :256], low[:, 256:]], axis=0)
            else:
                out[...] = tot.reshape(out.shape)
            send_stage(piece, i + 1)
        elif part == 0:
            for j in range(4):
                cols = slice(128 * (j % 2), 128 * (j % 2 + 1))
                gin_ref[t, pl.ds(4 * k + j, 8, stride=12), :] = tot[j // 2, :, cols]
                gin_ref[t, pl.ds(96 + 4 * k + j, 4, stride=12), :] = tot[2, 4 * (j // 2):4 * (j // 2 + 1), cols]
        else:
            for j in range(3):
                gout_ref[t, pl.ds(48 * k + j, 16, stride=3), :] = tot[:, 128 * j:128 * (j + 1)]

    compute_b(0, 0)
    start(Y[0])
    classes(1)
    compute_b(0, 1)
    start(X[0])
    compute_b(1, 1)
    start(Z[1])
    compute_b(2, 0, 1)
    loads["sel"].wait()
    select_rows(0)
    start(Y[2])
    compute_a(2, 0)
    start(X[3])
    select_rows(1)
    compute_a(1, 1)
    start(Z[2])
    compute_a(2, 1)
    compute_b(1, 0)
    advance(0, Y[0], X[0])
    compute_a(0, 1)
    advance(0, Z[1])
    start(Y[1])
    start(X[1])
    start(Z[3])
    compute_a(0, 0)
    advance(0, Y[2])
    start(Y[3])
    compute_a(1, 0)
    advance(1, Y[0])
    start(X[2])
    start(Z[0])
    advance(0, Y[1], X[1])
    advance(1, X[0])
    advance(0, X[3])
    advance(1, Y[2])
    advance(0, Y[3], Z[3])
    advance(1, X[1])
    advance(0, X[2], Z[0])
    advance(1, X[3])
    advance(0, Z[2])
    advance(1, Y[1])
    advance(2, Y[2])
    advance(1, Y[3])
    advance(2, X[0], X[3])
    advance(1, X[2], Z[3], Z[1], Z[0])
    advance(2, Y[3], X[2], Y[0])
    advance(1, Z[2])
    advance(2, Z[3], Y[1], Z[1])
    advance(3, X[2], X[3])
    advance(2, Z[0])
    advance(3, Y[3])
    advance(2, X[1])
    advance(3, Y[2])
    advance(2, Z[2])

    stores = [pltpu.make_async_copy(src, dst, out_sem.at[i])
              for i, (src, dst) in enumerate(((gin_ref, gin_hbm), (gout_ref, gout_hbm)))]
    with scope("gram"):
        row = jnp.zeros((1, 128), F32)
        for q, (s, t) in enumerate(((0, 0), (0, 1), (1, 1))):
            prod = gin_ref[s] * gin_ref[t] + gout_ref[s] * gout_ref[t]
            one = jnp.sum(jnp.sum(prod, axis=0, keepdims=True), axis=1, keepdims=True)
            row = jnp.where(lane == q, one, row)
        gram_ref[me] = row
    with scope("gramx"):
        row_start(gram_ref, gram_ssem, gram_rsem)
        stores[0].start()
        stores[1].start()
        for i in range(4):
            sent = [b[2 * j + 1] for piece, b in bufs.items() for j in range(len(PATH[piece])) if sent_on(piece, j) == i]
            nbytes = sum(math.prod(ref.shape) * (2 if i == 0 else 4) for ref in sent)
            width = next(w for w in (1024, 512, 256) if nbytes // (4 * w) % 8 == 0)
            whole(pre_ref.at[pl.ds(0, nbytes // (4 * width)), pl.ds(0, width)], ssem.at[i]).wait_send()
        row_all(cnt_ref, cnt_ssem, cnt_rsem).wait_send()
        stores[0].wait()
        stores[1].wait()
        row_all(gram_ref, gram_ssem, gram_rsem).wait_recv()
    with scope("drain"):
        gram_out[...] = jnp.sum(gram_ref[...], axis=0)
        row_all(gram_ref, gram_ssem, gram_rsem).wait_send()


def combine(gram_ref, gin_hbm, gout_hbm, weights_ref, sum_in, sum_out, gin_ref, gout_ref, sem):
    loads = [pltpu.make_async_copy(src, dst, sem.at[i])
             for i, (src, dst) in enumerate(((gin_hbm, gin_ref), (gout_hbm, gout_ref)))]
    for load in loads:
        load.start()
    lane = lax.broadcasted_iota(jnp.int32, (1, 128), 1)
    m00, m01, m11 = [jnp.broadcast_to(jnp.sum(jnp.where(lane == q, gram_ref[...], 0.0), axis=1, keepdims=True), (1, 128))
                     for q in range(3)]
    scale = (m00 + m11) / 2.0
    w0 = jnp.full((1, 128), 0.5, F32)
    w1 = w0
    for _ in range(SOLVER_STEPS):
        r0 = w0 * jnp.exp(-(m00 * w0 + m01 * w1) / scale)
        r1 = w1 * jnp.exp(-(m01 * w0 + m11 * w1) / scale)
        norm = r0 + r1
        w0 = r0 / norm
        w1 = r1 / norm
    weights_ref[0] = w0[0, 0]
    weights_ref[1] = w1[0, 0]
    for load in loads:
        load.wait()
    sum_in[...] = w0 * gin_ref[0] + w1 * gin_ref[1]
    sum_out[...] = w0 * gout_ref[0] + w1 * gout_ref[1]


def solution(mesh):
    sel = select_matrices()

    def local_step(x_loc, w_in, w_out, task_heads, lab_loc, mask_loc):
        vmem = pl.BlockSpec(memory_space=pltpu.VMEM)
        hbm = pl.BlockSpec(memory_space=pl.ANY)
        dma = pltpu.SemaphoreType.DMA
        heads_t = jnp.transpose(task_heads, (2, 0, 1))
        args = (x_loc, w_in, w_out, heads_t, lab_loc, mask_loc, jnp.asarray(sel, BF16))
        piece = jax.ShapeDtypeStruct((144, 128), F32)
        outs = [jax.ShapeDtypeStruct((TASKS, 144, 128), F32)] * 2 + [jax.ShapeDtypeStruct((1, 128), F32)]
        scratch = [pltpu.VMEM(a.shape, a.dtype) for a in args] + [pltpu.VMEM(a.shape, a.dtype) for a in outs[:2]] + [
            pltpu.VMEM((DIM, TOK), BF16),
            pltpu.VMEM((32, CHUNKS, 16, TOK), BF16),
            pltpu.VMEM((HID, TOK), F32),
            pltpu.VMEM((HID, TOK), F32),
            pltpu.VMEM((len(ORDERS), DIM, TOK), BF16),
            pltpu.VMEM((TOK, TASKS * DIM), BF16),
            pltpu.VMEM((TASKS, 16, TOK), BF16),
            pltpu.VMEM((DEVICES, 1, 128), F32),
            pltpu.VMEM((DEVICES, 1, 128), F32)]
        scratch += [pltpu.VMEM(*shape) for piece, path in PATH.items() for shape in buffers(piece[0], path)]
        scratch += [dma((len(args),)), dma((3,)), dma((len(PATH), 4)), dma((4,)), dma, dma, dma, dma]
        gin, gout, gram = pl.pallas_call(
            kernel,
            out_shape=outs,
            in_specs=[hbm] * len(args),
            out_specs=[hbm, hbm, vmem],
            scratch_shapes=scratch,
            compiler_params=pltpu.CompilerParams(collective_id=0, has_side_effects=True,
                                                 vmem_limit_bytes=56547000),
            name="step",
        )(*args)
        weights, grad_in, grad_out = pl.pallas_call(
            combine,
            out_shape=[jax.ShapeDtypeStruct((TASKS,), F32), piece, piece],
            in_specs=[vmem, hbm, hbm],
            out_specs=[pl.BlockSpec(memory_space=pltpu.SMEM), vmem, vmem],
            scratch_shapes=[pltpu.VMEM(outs[0].shape, F32), pltpu.VMEM(outs[1].shape, F32), dma((2,))],
            compiler_params=pltpu.CompilerParams(vmem_limit_bytes=56547000),
            name="combine",
        )(gram, gin, gout)
        return weights, grad_in.reshape(-1), grad_out.reshape(-1)

    return jax.shard_map(local_step, mesh=mesh,
                         in_specs=(P("data", None), P(), P(), P(), P(None, "data"), P(None, "data")),
                         out_specs=(P(), P("data"), P("data")), check_vma=False)
```
